32 devices in a mesh: grp: 2 (over y), row: 4 (over x, core), sub: 4 (over z).
Axes of the slice: x: 2, y: 2, z: 4, core: 2. Of those that a mesh axis runs over, the one named last changes fastest.
Arguments:
- residual_in: float32 [4, 2048, 2048], P('grp', ('row', 'sub')), parts along dimension 0, may hold values from -100 to 100
- direction: float32 [4, 2048, 2048], P('grp', ('row', 'sub')), parts along dimension 0, may hold values from -100 to 100
- spectrum: float32 [8192, 4096], P('grp', ('row', 'sub')), parts along dimension 0, may hold values from 0.0999 to 10.001, as said below
- noise_var: float32 [2], P('grp'), parts along dimension 0, may hold values from 0.5 to 2
Outputs:
- residual_out: float32 [4, 2048, 2048], P('grp', ('row', 'sub')), parts along dimension 0
- direction_out: float32 [4, 2048, 2048], P('grp', ('row', 'sub')), parts along dimension 0
- step_size: float32 [4], P('grp'), parts along dimension 0
The draws below stay inside these ranges and needn't reach their ends.
There are 2 independent parts, one for each index of `grp`. The reference program is written for one: setup_inputs(seed, part) draws one part's arguments, and reference() takes and returns one part's arrays. A program takes and returns all parts, laid end to end along the dimension named above; each array names one. Nothing has to cross between parts.
Inputs may be any that keep to these rules, and one draw needn't show every extreme that they name: spectrum[k, l] = spectrum[(4096 - k) % 4096, (4096 - l) % 4096] for all k, l.
All inputs are finite; a program needn't handle non-finite values.
Results may differ from the reference program's by a relative error of at most 0.00005.
Values sent between devices are 32-bit elements; how exact they have to be, the bound alone decides.
A program may use at most 128 MiB of HBM per device.

```python
import math
import jax
import jax.numpy as jnp
from jax import lax

GRID = 2048
EMBED = 4096
PROBES = 2


def field_values(key):
    subkeys = jax.random.split(key, 4)
    row_pos = jnp.arange(GRID, dtype=jnp.float32) / GRID
    row_log = 0.5 * row_pos + 0.5 * jax.random.uniform(subkeys[0], (GRID,))
    col_log = jax.random.uniform(subkeys[1], (GRID,))
    raw_vals = jax.random.normal(subkeys[3], (PROBES, GRID, GRID))
    values = raw_vals * jnp.power(10.0, row_log[:, None] + col_log[None, :] - 1.0)
    return jnp.clip(values, -100.0, 100.0).astype(jnp.float32)


def draw_residual_in(key, part):
    return field_values(jax.random.fold_in(key, 101))


def draw_direction(key, part):
    return field_values(jax.random.fold_in(key, 202))


def draw_spectrum(key, part):
    subkey = jax.random.fold_in(key, 303)
    raw_log = jax.random.uniform(subkey, (EMBED, EMBED), minval=-1.0, maxval=1.0)
    mirrored = jnp.roll(jnp.flip(raw_log, (0, 1)), 1, (0, 1))
    return jnp.power(10.0, 0.5 * (raw_log + mirrored)).astype(jnp.float32)


def setup_inputs(seed: int = 0, part: int = 0) -> dict:
    key_of = jax.random.split(jax.random.key(seed), 5)
    part_keys = jax.random.split(jax.random.fold_in(key_of[4], part), 5)
    return {
        "residual_in": draw_residual_in(jax.random.fold_in(jax.random.fold_in(key_of[4], part), 71), part),
        "direction": draw_direction(jax.random.fold_in(jax.random.fold_in(key_of[4], part), 71), part),
        "spectrum": draw_spectrum(jax.random.fold_in(jax.random.fold_in(key_of[4], part), 71), part),
        "noise_var": jnp.clip(jnp.exp(jax.random.uniform(part_keys[3], (1,), jnp.float32, math.log(0.5), math.log(2.0))), 0.5, 2.0),
    }


tiny_value = 1e-6


def reference(residual_in, direction, spectrum, noise_var):
    def one_probe(field_in):
        padded = jnp.pad(field_in, ((0, EMBED - GRID), (0, EMBED - GRID)))
        spectral = jnp.fft.fft2(padded)
        restored = jnp.fft.ifft2(spectral * spectrum)
        return jnp.real(restored)[:GRID, :GRID] + noise_var[0] * field_in

    image_out = lax.map(one_probe, direction)
    old_norm = jnp.sum(residual_in * residual_in, axis=(1, 2))
    curvature = jnp.sum(direction * image_out, axis=(1, 2))
    step_size = old_norm / curvature
    residual_out = residual_in - step_size[:, None, None] * image_out
    new_norm = jnp.sum(residual_out * residual_out, axis=(1, 2))
    direction_out = residual_out + (new_norm / (old_norm + tiny_value))[:, None, None] * direction
    return residual_out, direction_out, step_size
```

```python
import functools
import math

import jax
import jax.numpy as jnp
import numpy as np
from jax import lax
from jax.experimental import pallas as pl
from jax.experimental.pallas import tpu as pltpu
from jax.sharding import PartitionSpec as P

LANES = 128
TINY = 1e-06
CHUNKS = 4
PIECES = 4
MESH = pl.DeviceIdType.MESH
GRANT = 60 * 1024 * 1024


def unit(turns, modulus, orient):
    angle = orient * 2.0 * np.pi * (np.asarray(turns) % modulus) / modulus
    return np.cos(angle), np.sin(angle)


def halves(table):
    table = np.asarray(table, np.float32)
    hi = table.astype(jnp.bfloat16)
    lo = (table - hi.astype(np.float32)).astype(jnp.bfloat16)
    return jnp.asarray(np.stack([hi, lo]))


def complex_block(cos_part, sin_part):
    return np.stack(
        [np.stack([cos_part, sin_part], 1), np.stack([-sin_part, cos_part], 1)], 0
    )


def split(x):
    hi = x.astype(jnp.bfloat16)
    return hi, (x - hi.astype(jnp.float32)).astype(jnp.bfloat16)


def dot(a, b):
    return jnp.dot(a, b, preferred_element_type=jnp.float32)


def dot_right(x, table_ref):
    hi, lo = split(x)
    return dot(hi, table_ref[0]) + (dot(lo, table_ref[0]) + dot(hi, table_ref[1]))


def dot_left(table_ref, x):
    hi, lo = split(x)
    return dot(table_ref[0], hi) + (dot(table_ref[0], lo) + dot(table_ref[1], hi))


def turn(z, k, n, orient):
    k = k % n
    re, im = z
    if k == 0:
        return z
    if 2 * k == n:
        return -re, -im
    if 4 * k == n or 4 * k == 3 * n:
        sign = orient if 4 * k == n else -orient
        return (-im, re) if sign > 0 else (im, -re)
    c = math.cos(2 * math.pi * k / n)
    s = orient * math.sin(2 * math.pi * k / n)
    return re * c - im * s, re * s + im * c


def add(u, v):
    return u[0] + v[0], u[1] + v[1]


def sub(u, v):
    return u[0] - v[0], u[1] - v[1]


def butterflies(xs, orient):
    n = len(xs)
    if n == 1:
        return xs
    even = butterflies(xs[0::2], orient)
    odd = butterflies(xs[1::2], orient)
    odd = [turn(z, k, n, orient) for k, z in enumerate(odd)]
    return [add(e, o) for e, o in zip(even, odd)] + [sub(e, o) for e, o in zip(even, odd)]


def padded_forward(xs):
    n = len(xs)
    even = butterflies(xs, -1)
    odd = butterflies([turn(z, a, 2 * n, -1) for a, z in enumerate(xs)], -1)
    return [even[i // 2] if i % 2 == 0 else odd[i // 2] for i in range(2 * n)]


def cut_inverse(zs):
    n = len(zs) // 2
    even = butterflies(zs[0::2], 1)
    odd = butterflies(zs[1::2], 1)
    return [add(even[a], turn(odd[a], a, 2 * n, 1)) for a in range(n)]


def rotate(re, im, c, s):
    return re * c - im * s, re * s + im * c


def row_kernel(low, groups, dir_ref, table_ref, cos_ref, sin_ref, *rest):
    outs, work, turned = rest[:-2], rest[-2], rest[-1]
    half = low // 2
    rows = dir_ref.shape[1]
    for c in range(2):
        for a in range(half):
            turned[a, c] = dir_ref[c, :, a * LANES : (a + 1) * LANES].T

    def spread(t, carry):
        at = pl.ds(pl.multiple_of(t * 8, 8), 8)
        xs = [(turned[a, 0, at, :], turned[a, 1, at, :]) for a in range(half)]
        cos_rows, sin_rows = cos_ref[at, :], sin_ref[at, :]
        for m, (re, im) in enumerate(padded_forward(xs)):
            re, im = rotate(re, im, cos_rows[:, m : m + 1], sin_rows[:, m : m + 1])
            work[m, 0, at, :] = re
            work[m, 1, at, :] = im
        return carry

    lax.fori_loop(0, LANES // 8, spread, 0)
    per_chunk = low // len(outs)
    for i, out in enumerate(outs):

        def column(m, carry):
            got = dot_left(table_ref, work[i * per_chunk + m].reshape(2 * LANES, rows))
            size = 2 * LANES // groups
            for j in range(groups):
                out[j, m] = got[j * size : (j + 1) * size]
            return carry

        lax.fori_loop(0, per_chunk, column, 0)


def column_kernel(low, per, x_ref, w_ref, fwd_ref, inv_ref, cos_ref, sin_ref, out_ref, work):
    half = low // 2
    count = x_ref.shape[1]

    def spread(m, carry):
        xs = [(x_ref[a, m, :per], x_ref[a, m, per:]) for a in range(half)]
        for k, (re, im) in enumerate(padded_forward(xs)):
            re, im = rotate(re, im, cos_ref[k : k + 1, :], sin_ref[k : k + 1, :])
            work[k, m, :, :LANES] = re
            work[k, m, :, LANES:] = im
        return carry

    lax.fori_loop(0, count, spread, 0)

    def filtered(k, carry):
        spectral = dot_right(work[k].reshape(count * per, 2 * LANES), fwd_ref)
        weights = w_ref[k].reshape(count * per, LANES)
        spectral = spectral * jnp.concatenate([weights, weights], axis=1)
        got = dot_right(spectral, inv_ref)
        cos_row, sin_row = cos_ref[pl.ds(k, 1), :], sin_ref[pl.ds(k, 1), :]
        re, im = rotate(got[:, :LANES], got[:, LANES:], cos_row, -sin_row)
        work[k, :, :, :LANES] = re.reshape(count, per, LANES)
        work[k, :, :, LANES:] = im.reshape(count, per, LANES)
        return carry

    lax.fori_loop(0, low, filtered, 0)

    def gather(m, carry):
        zs = [(work[k, m, :, :LANES], work[k, m, :, LANES:]) for k in range(low)]
        for a, (re, im) in enumerate(cut_inverse(zs)):
            out_ref[a, m, :per] = re
            out_ref[a, m, per:] = im
        return carry

    lax.fori_loop(0, count, gather, 0)


def image_kernel(low, groups, chunks, *refs):
    ins = refs[:chunks]
    dir_ref, res_ref, noise_ref, table_ref, cos_ref, sin_ref = refs[chunks : chunks + 6]
    image_ref, sums_ref, work, applied = refs[chunks + 6 :]
    half = low // 2
    rows = dir_ref.shape[1]
    per_chunk = low // chunks
    for i, x_ref in enumerate(ins):

        def column(m, carry):
            parts = [x_ref[j, m] for j in range(groups)]
            got = dot_left(table_ref, parts[0] if groups == 1 else jnp.concatenate(parts, axis=0))
            work[i * per_chunk + m] = got.reshape(2, LANES, rows)
            return carry

        lax.fori_loop(0, per_chunk, column, 0)

    def gather(t, carry):
        at = pl.ds(pl.multiple_of(t * 8, 8), 8)
        cos_rows, sin_rows = cos_ref[at, :], sin_ref[at, :]
        zs = []
        for m in range(low):
            zs.append(
                rotate(work[m, 0, at, :], work[m, 1, at, :], cos_rows[:, m : m + 1], -sin_rows[:, m : m + 1])
            )
        for a, (re, im) in enumerate(cut_inverse(zs)):
            applied[a, 0, at, :] = re
            applied[a, 1, at, :] = im
        return carry

    lax.fori_loop(0, LANES // 8, gather, 0)
    noise = noise_ref[0]
    for c in range(2):
        totals = [jnp.zeros((rows, LANES), jnp.float32)] * 4
        for a in range(half):
            cols = slice(a * LANES, (a + 1) * LANES)
            d, r = dir_ref[c, :, cols], res_ref[c, :, cols]
            image = applied[a, c].T + noise * d
            image_ref[c, :, cols] = image
            for s, term in enumerate((r * r, d * image, r * image, image * image)):
                totals[s] = totals[s] + term
        for s in range(4):
            sums_ref[4 * c + s : 4 * c + s + 1, :] = jnp.sum(totals[s], axis=0, keepdims=True)


def update_kernel(n_row, n_sub, sums_ref, image_ref, dir_ref, res_ref, r_out, d_out, s_out, held, send_sem, recv_sem):
    n = n_row * n_sub
    me = lax.axis_index("row") * n_sub + lax.axis_index("sub")

    def place(o):
        peer = lax.rem(me + o, n)
        return {"row": peer // n_sub, "sub": lax.rem(peer, n_sub)}

    barrier = pltpu.get_barrier_semaphore()

    def greet(o, carry):
        pl.semaphore_signal(barrier, inc=1, device_id=place(o), device_id_type=MESH)
        return carry

    lax.fori_loop(1, n, greet, 0)
    pl.semaphore_wait(barrier, n - 1)

    def copy(o):
        return pltpu.make_async_remote_copy(
            src_ref=sums_ref,
            dst_ref=held.at[me],
            send_sem=send_sem.at[o],
            recv_sem=recv_sem.at[o],
            device_id=place(o),
            device_id_type=MESH,
        )

    def start(o, carry):
        copy(o).start()
        return carry

    lax.fori_loop(1, n, start, 0)
    held[me] = sums_ref[...]

    def finish(o, carry):
        copy(o).wait()
        return carry

    lax.fori_loop(1, n, finish, 0)
    total = jnp.sum(jnp.sum(held[...], axis=0), axis=1, keepdims=True)
    for c in range(2):
        old, curve, cross, square = [total[4 * c + s : 4 * c + s + 1] for s in range(4)]
        step = old / curve
        new = jnp.maximum(old - 2.0 * step * cross + step * step * square, 0.0)
        beta = new / (old + TINY)
        s_out[c : c + 1, :] = jnp.broadcast_to(step, (1, LANES))
        rows = min(8, res_ref.shape[1])

        def strip(t, carry):
            at = pl.ds(pl.multiple_of(t * rows, rows), rows)
            r = res_ref[c, at, :] - step * image_ref[c, at, :]
            r_out[c, at, :] = r
            d_out[c, at, :] = r + beta * dir_ref[c, at, :]
            return carry

        lax.fori_loop(0, res_ref.shape[1] // rows, strip, 0)


def params(**more):
    return pltpu.CompilerParams(vmem_limit_bytes=GRANT, **more)


def make_tables(embed, n, per):
    low, f32 = embed // LANES, jnp.float32
    slots, seconds = np.arange(LANES), np.arange(low)
    turn_cos, turn_sin = unit(slots[:, None] * seconds[None, :], embed, -1.0)
    wide_cos, wide_sin = jnp.asarray(turn_cos, f32), jnp.asarray(turn_sin, f32)
    tall_cos, tall_sin = jnp.asarray(turn_cos.T, f32), jnp.asarray(turn_sin.T, f32)
    fwd = complex_block(*unit(slots[:, None] * slots[None, :], LANES, -1.0))
    inv = complex_block(*unit(slots[:, None] * slots[None, :], LANES, 1.0))
    scale = 1.0 / (embed * embed)
    col_fwd = halves(fwd.reshape(2 * LANES, 2 * LANES))
    col_inv = halves(inv.reshape(2 * LANES, 2 * LANES) * scale)
    row_fwd = halves(
        fwd.reshape(2, LANES, 2, n, per).transpose(3, 2, 4, 0, 1).reshape(2 * LANES, 2 * LANES)
    )
    row_inv = halves(
        inv.reshape(2, n, per, 2, LANES).transpose(3, 4, 1, 0, 2).reshape(2 * LANES, 2 * LANES)
    )
    return row_fwd, row_inv, col_fwd, col_inv, wide_cos, wide_sin, tall_cos, tall_sin


def pair_body(n_row, n_sub, residual_in, direction, weights, noise_var):
    _, rows, grid_len = direction.shape
    embed = 2 * grid_len
    low, half = embed // LANES, grid_len // LANES
    n = n_row * n_sub
    per = LANES // n
    f32 = jnp.float32
    vmem = pl.BlockSpec(memory_space=pltpu.VMEM)
    chunks = CHUNKS
    per_chunk = low // chunks
    aligned = (2 * per) % 8 == 0
    groups = n if aligned else 1

    row_fwd, row_inv, col_fwd, col_inv, wide_cos, wide_sin, tall_cos, tall_sin = make_tables(embed, n, per)

    spread = pl.pallas_call(
        functools.partial(row_kernel, low, groups),
        out_shape=[jax.ShapeDtypeStruct((groups, per_chunk, 2 * LANES // groups, rows), f32)] * chunks,
        in_specs=[vmem] * 4,
        out_specs=[vmem] * chunks,
        scratch_shapes=[pltpu.VMEM((low, 2, LANES, rows), f32), pltpu.VMEM((half, 2, LANES, rows), f32)],
        compiler_params=params(),
        name="rows_out",
    )(direction, row_fwd, wide_cos, wide_sin)

    def swap(x):
        return lax.all_to_all(x, ("row", "sub"), split_axis=0, concat_axis=0, tiled=True)

    back = []
    for i, x in enumerate(spread):
        if not aligned:
            x = x.reshape(per_chunk, n, 2 * per, rows).transpose(1, 0, 2, 3)
        x = swap(x)
        if rows != LANES:
            x = x.reshape(half, LANES // rows, per_chunk, 2 * per, rows).transpose(0, 2, 3, 1, 4)
            x = x.reshape(half, per_chunk, 2 * per, LANES)
        x = pl.pallas_call(
            functools.partial(column_kernel, low, per),
            out_shape=jax.ShapeDtypeStruct((half, per_chunk, 2 * per, LANES), f32),
            in_specs=[vmem] * 6,
            out_specs=vmem,
            scratch_shapes=[pltpu.VMEM((low, per_chunk, per, 2 * LANES), f32)],
            compiler_params=params(),
            name=f"columns{i}",
        )(x, weights[:, i * per_chunk : (i + 1) * per_chunk], col_fwd, col_inv, tall_cos, tall_sin)
        if rows != LANES:
            x = x.reshape(half, per_chunk, 2 * per, LANES // rows, rows).transpose(0, 3, 1, 2, 4)
            x = x.reshape(n, per_chunk, 2 * per, rows)
        x = swap(x)
        if not aligned:
            x = x.transpose(1, 0, 2, 3).reshape(1, per_chunk, 2 * LANES, rows)
        back.append(x)

    image, sums = pl.pallas_call(
        functools.partial(image_kernel, low, groups, chunks),
        out_shape=[jax.ShapeDtypeStruct(direction.shape, f32), jax.ShapeDtypeStruct((8, LANES), f32)],
        in_specs=[vmem] * (chunks + 2) + [pl.BlockSpec(memory_space=pltpu.SMEM)] + [vmem] * 3,
        out_specs=[vmem] * 2,
        scratch_shapes=[pltpu.VMEM((low, 2, LANES, rows), f32), pltpu.VMEM((half, 2, LANES, rows), f32)],
        compiler_params=params(),
        name="rows_back",
    )(*back, direction, residual_in, noise_var, row_inv, wide_cos, wide_sin)

    residual_out, direction_out, steps = pl.pallas_call(
        functools.partial(update_kernel, n_row, n_sub),
        out_shape=[
            jax.ShapeDtypeStruct(direction.shape, f32),
            jax.ShapeDtypeStruct(direction.shape, f32),
            jax.ShapeDtypeStruct((2, LANES), f32),
        ],
        in_specs=[vmem] * 4,
        out_specs=[vmem] * 3,
        scratch_shapes=[
            pltpu.VMEM((n, 8, LANES), f32),
            pltpu.SemaphoreType.DMA((n,)),
            pltpu.SemaphoreType.DMA((n,)),
        ],
        compiler_params=params(collective_id=0, has_side_effects=True),
        name="update",
    )(sums, image, direction, residual_in)
    return residual_out, direction_out, steps[:, 0]


def odd_terms(d, n):
    q = n // 4
    zs = butterflies([turn((d[a], -d[a + q]), a, n, -1) for a in range(q)], -1)
    return {4 * j + 1: z for j, z in enumerate(zs)}


def real_forward(xs):
    n = len(xs)
    if n == 1:
        return {0: (xs[0], None)}
    if n == 2:
        return {0: (xs[0] + xs[1], None), 1: (xs[0] - xs[1], None)}
    h = n // 2
    out = {2 * k: z for k, z in real_forward([xs[a] + xs[a + h] for a in range(h)]).items()}
    out.update(odd_terms([xs[a] - xs[a + h] for a in range(h)], n))
    return out


def real_padded(xs):
    n = 2 * len(xs)
    out = {2 * k: z for k, z in real_forward(xs).items()}
    out.update(odd_terms(xs, n))
    return out


def odd_values(pairs, n):
    q = n // 4
    zs = [turn(z, a, n, 1) for a, z in enumerate(butterflies([pairs[4 * j + 1] for j in range(q)], 1))]
    return [z[0] for z in zs] + [-z[1] for z in zs]


def real_inverse(pairs, n):
    if n == 1:
        return [pairs[0][0]]
    if n == 2:
        return [pairs[0][0] + pairs[1][0], pairs[0][0] - pairs[1][0]]
    even = real_inverse({k // 2: z for k, z in pairs.items() if k % 2 == 0}, n // 2)
    odd = odd_values(pairs, n)
    return [e + o for e, o in zip(even, odd)] + [e - o for e, o in zip(even, odd)]


def real_cut(pairs, n):
    even = real_inverse({k // 2: z for k, z in pairs.items() if k % 2 == 0}, n // 2)
    return [e + o for e, o in zip(even, odd_values(pairs, n))]


def real_names(n):
    if n <= 2:
        return list(range(n))
    return [2 * k for k in real_names(n // 2)] + list(range(1, n, 4))


def loop(first, last, step):
    def run(i, carry):
        step(i)
        return carry

    lax.fori_loop(first, last, run, 0)


def half_kernel(
    low, chunks, pieces, n_row, n_sub,
    dir_ref, res_hbm, spec_hbm, noise_ref, row_fwd, row_inv, col_fwd, col_inv, tall_cos, tall_sin,
    r_out, d_out, s_out,
    res_ref, spec_ref, weights, work, cols, send, recv, back_send, back_recv,
    raw_in, img_send, img_in, x_send, x_recv, xb_send, xb_recv, held, sums_ref,
    load_sem, raw_ssem, raw_rsem, img_ssem, img_rsem, send_sem, recv_sem, back_ssem, back_rsem,
    x_ssem, x_rsem, xb_ssem, xb_rsem, sum_ssem, sum_rsem,
):
    n = n_row * n_sub
    hs = n_sub // 2
    g = n_row * hs
    half = low // 2
    count = low // chunks
    per = LANES // n
    size = 2 * per
    step_rows = LANES // pieces
    my_r, my_s = lax.axis_index("row"), lax.axis_index("sub")
    h = my_s // hs
    gi = my_r * hs + lax.rem(my_s, hs)
    me = my_r * n_sub + my_s
    mate_s = n_sub - 1 - my_s
    mate = {"row": my_r, "sub": mate_s}
    slabs = [me, my_r * n_sub + mate_s]
    lead = my_s == h * hs

    def place(o):
        peer = lax.rem(me + o, n)
        return {"row": peer // n_sub, "sub": lax.rem(peer, n_sub)}

    def ally(d, part):
        r, s = d // hs, part * hs + lax.rem(d, hs)
        return {"row": r, "sub": s}, [r * n_sub + s, r * n_sub + n_sub - 1 - s]

    def leader(e):
        return {"row": e, "sub": (1 - h) * hs}

    barrier = pltpu.get_barrier_semaphore()
    loop(
        1, n,
        lambda o: pl.semaphore_signal(barrier, inc=1, device_id=place(o), device_id_type=MESH),
    )
    load_res = pltpu.make_async_copy(res_hbm, res_ref, load_sem.at[0])
    load_spec = [
        pltpu.make_async_copy(spec_hbm.at[:, pl.ds(s * LANES, LANES)], spec_ref.at[s], load_sem.at[s + 1])
        for s in range(spec_ref.shape[0])
    ]

    def remote(src, dst, s_sem, r_sem, device):
        return pltpu.make_async_remote_copy(
            src_ref=src, dst_ref=dst, send_sem=s_sem, recv_sem=r_sem, device_id=device, device_id_type=MESH
        )

    def raw_copy(p):
        at = pl.ds(pl.multiple_of(p * step_rows, step_rows), step_rows)
        return remote(dir_ref.at[1 - h, at, :], raw_in.at[at, :], raw_ssem.at[p], raw_rsem.at[p], mate)

    def img_copy(p):
        at = pl.ds(pl.multiple_of(p * step_rows, step_rows), step_rows)
        return remote(img_send.at[at, :], img_in.at[at, :], img_ssem.at[p], img_rsem.at[p], mate)

    def ahead(i, b, o):
        p = lax.rem(gi + o, g)
        return remote(
            send.at[i, b, p], recv.at[i, slabs[b]], send_sem.at[i, b, o], recv_sem.at[i, b, o], ally(p, h)[0]
        )

    def home(i, b, o):
        p = lax.rem(gi + o, g)
        device, places = ally(p, h)
        return remote(
            back_send.at[i, places[b]], back_recv.at[i, b, gi], back_ssem.at[i, b, o], back_rsem.at[i, b, o], device
        )

    def x_ahead(e):
        return remote(x_send.at[e], x_recv.at[gi], x_ssem.at[e], x_rsem.at[gi], leader(e))

    def x_arrival(d):
        return remote(x_send.at[0], x_recv.at[d], x_ssem.at[0], x_rsem.at[d], mate)

    def x_home(d):
        return remote(xb_send.at[d], xb_recv.at[my_r], xb_ssem.at[d], xb_rsem.at[my_r], ally(d, 1 - h)[0])

    def x_back(e):
        return remote(xb_send.at[0], xb_recv.at[e], xb_ssem.at[0], xb_rsem.at[e], mate)

    pl.semaphore_wait(barrier, n - 1)
    loop(0, pieces, lambda p: raw_copy(p).start())
    for load in load_spec:
        load.start()
    load_res.start()

    def row_strip(read, t):
        at = pl.ds(pl.multiple_of(t * 8, 8), 8)
        found = real_padded([read(at, slice(a * LANES, (a + 1) * LANES)) for a in range(half)])
        for m in range(low):
            c, s = tall_cos[m : m + 1, :], tall_sin[m : m + 1, :]
            re, im = found[m] if m in found else found[low - m]
            if im is None:
                re, im = re * c, re * s
            elif m in found:
                re, im = rotate(re, im, c, s)
            else:
                re, im = re * c + im * s, re * s - im * c
            work[m, at, :LANES] = re
            work[m, at, LANES:] = im

    batch = min(4, count)

    def row_dots(x, table, at):
        hi, lo = split(x)
        return dot(hi, table[h, 0, :, at]) + (dot(lo, table[h, 0, :, at]) + dot(hi, table[h, 1, :, at]))

    def row_extras(b):
        got = row_dots(work[0], row_fwd, slice(LANES, 2 * LANES)).T
        for e in range(n_row):
            x_send[e, 2 * b : 2 * b + 2, :] = got[2 * e : 2 * e + 2]

    def send_chunk(i, b):
        def columns(t):
            m = t * batch
            x = work[pl.ds(i * count + m, batch)].reshape(batch * LANES, 2 * LANES)
            got = row_dots(x, row_fwd, slice(0, LANES))
            for k in range(batch):
                part = got[k * LANES : (k + 1) * LANES].T
                for d in range(g):
                    send[i, b, d, m + k] = part[d * size : (d + 1) * size]

        loop(0, count // batch, columns)
        recv[i, slabs[b]] = send[i, b, gi]
        loop(1, g, lambda o: ahead(i, b, o).start())

    loop(0, LANES // 8, lambda t: row_strip(lambda at, cs: dir_ref[h, at, cs], t))
    row_extras(0)
    loop(0, chunks, lambda i: send_chunk(i, 0))

    for load in load_spec:
        load.wait()

    def turn_spectrum(k):
        for s in range(spec_ref.shape[0]):
            part = spec_ref[s, pl.ds(k, LANES, stride=low), :]
            weights[k, s * LANES : (s + 1) * LANES, :] = part.T

    loop(0, low, turn_spectrum)

    def raw_piece(p):
        raw_copy(p).wait_recv()
        loop(
            p * (step_rows // 8), (p + 1) * (step_rows // 8),
            lambda t: row_strip(lambda at, cs: raw_in[at, cs], t),
        )

    loop(0, pieces, raw_piece)
    row_extras(1)
    loop(0, n_row, lambda e: x_ahead(e).start())
    loop(0, chunks, lambda i: send_chunk(i, 1))

    wide = 8

    def fix_in():
        def one(d):
            x_arrival(d).wait_recv()
            for b, place_in in enumerate(ally(d, 1 - h)[1]):
                re, im = x_recv[d, 2 * b : 2 * b + 1, :], x_recv[d, 2 * b + 1 : 2 * b + 2, :]
                recv[0, place_in, 0, 0:1, :] = recv[0, place_in, 0, 0:1, :] - im
                recv[0, place_in, 0, per : per + 1, :] = recv[0, place_in, 0, per : per + 1, :] + re

        loop(0, g, one)

    def fix_out():
        def one(d):
            for b, place_in in enumerate(ally(d, 1 - h)[1]):
                re = 0.5 * back_send[0, place_in, 0, 0:1, :]
                im = 0.5 * back_send[0, place_in, 0, per : per + 1, :]
                back_send[0, place_in, 0, 0:1, :] = re
                back_send[0, place_in, 0, per : per + 1, :] = im
                xb_send[d, 2 * b : 2 * b + 1, :] = im
                xb_send[d, 2 * b + 1 : 2 * b + 2, :] = -re
            x_home(d).start()

        loop(0, g, one)

    def column_chunk(i):
        for b in range(2):
            loop(1, g, lambda o: ahead(i, b, o).wait_recv())
        pl.when(jnp.logical_and(i == 0, lead))(fix_in)

        def spread(m):
            xs = [(recv[i, a, m, :per], recv[i, a, m, per:]) for a in range(half)]
            for k, (re, im) in enumerate(padded_forward(xs)):
                re, im = rotate(re, im, tall_cos[k : k + 1, :], tall_sin[k : k + 1, :])
                cols[k, m, :, :LANES] = re
                cols[k, m, :, LANES:] = im

        loop(0, count, spread)
        block = count * per

        def filtered(t):
            k = t * wide
            spectral = dot_right(cols[pl.ds(k, wide)].reshape(wide * block, 2 * LANES), col_fwd)
            scale = jnp.concatenate(
                [
                    weights[k + w, pl.ds(i * count + m, per, stride=low), :]
                    for w in range(wide)
                    for m in range(count)
                ],
                axis=0,
            )
            spectral = spectral * jnp.concatenate([scale, scale], axis=1)
            got = dot_right(spectral, col_inv)
            for w in range(wide):
                cos_row, sin_row = tall_cos[pl.ds(k + w, 1), :], tall_sin[pl.ds(k + w, 1), :]
                part = got[w * block : (w + 1) * block]
                re, im = rotate(part[:, :LANES], part[:, LANES:], cos_row, -sin_row)
                cols[k + w, :, :, :LANES] = re.reshape(count, per, LANES)
                cols[k + w, :, :, LANES:] = im.reshape(count, per, LANES)

        loop(0, low // wide, filtered)

        def gather(m):
            zs = [(cols[k, m, :, :LANES], cols[k, m, :, LANES:]) for k in range(low)]
            for a, (re, im) in enumerate(cut_inverse(zs)):
                back_send[i, a, m, :per] = re
                back_send[i, a, m, per:] = im

        loop(0, count, gather)
        pl.when(jnp.logical_and(i == 0, lead))(fix_out)
        for b in range(2):
            back_recv[i, b, gi] = back_send[i, slabs[b]]
        loop(1, g, lambda o: home(i, 1, o).start())

    loop(0, chunks, column_chunk)
    loop(0, chunks, lambda i: loop(1, g, lambda o: home(i, 0, o).start()))
    loop(0, n_row, lambda e: x_back(e).wait_recv())

    def take_chunk(i, b):
        loop(1, g, lambda o: home(i, b, o).wait_recv())

        def columns(t):
            m = t * batch
            parts = []
            for k in range(batch):
                parts.append(jnp.concatenate([back_recv[i, b, d, m + k] for d in range(g)], axis=0).T)
            got = row_dots(jnp.concatenate(parts, axis=0), row_inv, slice(None))
            work[pl.ds(i * count + m, batch)] = got.reshape(batch, LANES, 2 * LANES)

        loop(0, count // batch, columns)

    def take_extras(b):
        parts = [xb_recv[e, 2 * b : 2 * b + 2, :] for e in range(n_row)]
        parts.append(jnp.zeros((LANES - 2 * n_row, LANES), jnp.float32))
        x = jnp.concatenate(parts, axis=0).T
        hi, lo = split(x)
        first, second = row_inv[2 + h, 0], row_inv[2 + h, 1]
        work[0] = work[0] + (dot(hi, first) + (dot(lo, first) + dot(hi, second)))

    def back_strip(t):
        at = pl.ds(pl.multiple_of(t * 8, 8), 8)

        def entry(m):
            re, im = work[m, at, :LANES], work[m, at, LANES:]
            return rotate(re, im, tall_cos[m : m + 1, :], -tall_sin[m : m + 1, :])

        pairs = {}
        for m in real_names(low):
            re, im = entry(m)
            if m in (0, half):
                pairs[m] = (re, None)
            else:
                re_too, im_too = entry(low - m)
                pairs[m] = (re + re_too, im - im_too)
        return at, real_cut(pairs, low)

    loop(0, chunks, lambda i: take_chunk(i, 1))
    take_extras(1)

    def img_piece(p):
        def strip(t):
            at, xs = back_strip(t)
            for a, x in enumerate(xs):
                img_send[at, a * LANES : (a + 1) * LANES] = x

        loop(p * (step_rows // 8), (p + 1) * (step_rows // 8), strip)
        img_copy(p).start()

    loop(0, pieces, img_piece)
    loop(0, chunks, lambda i: take_chunk(i, 0))
    take_extras(0)
    load_res.wait()
    noise = noise_ref[0]

    def tally(c, at, a, applied, totals):
        cs = slice(a * LANES, (a + 1) * LANES)
        d, r = dir_ref[c, at, cs], res_ref[c, at, cs]
        image = applied + noise * d
        d_out[c, at, cs] = image
        terms = (r * r, d * image, r * image, image * image)
        return [total + term for total, term in zip(totals, terms)]

    def own_strip(t, totals):
        at, xs = back_strip(t)
        for a, x in enumerate(xs):
            totals = tally(h, at, a, x, totals)
        return totals

    def far_strip(t, totals):
        at = pl.ds(pl.multiple_of(t * 8, 8), 8)
        for a in range(half):
            totals = tally(1 - h, at, a, img_in[at, a * LANES : (a + 1) * LANES], totals)
        return totals

    zeros = [jnp.zeros((8, LANES), jnp.float32)] * 4

    def keep(c, totals):
        for s in range(4):
            sums_ref[c, s : s + 1, :] = jnp.sum(totals[s], axis=0, keepdims=True)

    sums_ref[...] = jnp.zeros_like(sums_ref)
    keep(h, lax.fori_loop(0, LANES // 8, own_strip, zeros))

    def far_piece(p, totals):
        img_copy(p).wait_recv()
        return lax.fori_loop(p * (step_rows // 8), (p + 1) * (step_rows // 8), far_strip, totals)

    keep(1 - h, lax.fori_loop(0, pieces, far_piece, zeros))

    def share(o):
        return remote(sums_ref, held.at[me], sum_ssem.at[o], sum_rsem.at[o], place(o))

    held[me] = sums_ref[...]
    loop(1, n, lambda o: share(o).start())

    def drain(i):
        for b in range(2):
            loop(1, g, lambda o: ahead(i, b, o).wait_send())
            loop(1, g, lambda o: home(i, b, o).wait_send())

    loop(0, chunks, drain)
    loop(0, n_row, lambda e: x_ahead(e).wait_send())
    pl.when(lead)(lambda: loop(0, g, lambda d: x_home(d).wait_send()))
    loop(0, pieces, lambda p: raw_copy(p).wait_send())
    loop(0, pieces, lambda p: img_copy(p).wait_send())
    loop(1, n, lambda o: share(o).wait())
    total = jnp.sum(held[...], axis=0)
    for c in range(2):
        line = jnp.sum(total[c], axis=1, keepdims=True)
        old, curve, cross, square = [line[s : s + 1] for s in range(4)]
        step = old / curve
        new = jnp.maximum(old - 2.0 * step * cross + step * step * square, 0.0)
        beta = new / (old + TINY)
        s_out[c : c + 1, :] = jnp.broadcast_to(step, (1, LANES))

        def strip(t):
            at = pl.ds(pl.multiple_of(t * 8, 8), 8)
            r = res_ref[c, at, :] - step * d_out[c, at, :]
            r_out[c, at, :] = r
            d_out[c, at, :] = r + beta * dir_ref[c, at, :]

        loop(0, LANES // 8, strip)


def half_tables(embed, n_row, n_sub):
    low, n, hs = embed // LANES, n_row * n_sub, n_sub // 2
    per = LANES // n
    slots = np.arange(LANES)
    scale = 2.0 / (embed * embed)
    fwd_all, inv_all, inv_extra = [], [], []
    for part in range(2):
        own = [r * n_sub + part * hs + s for r in range(n_row) for s in range(hs)]
        freqs = np.stack([per * j + np.arange(per) for j in own])
        extra = np.array([per * (r * n_sub + (1 - part) * hs) for r in range(n_row)])[:, None]

        def forward(q):
            block = complex_block(*unit(slots[:, None] * q.reshape(-1)[None, :], LANES, -1.0))
            block = block.reshape(2, LANES, 2, *q.shape).transpose(0, 1, 3, 2, 4).reshape(2 * LANES, -1)
            return np.pad(block, ((0, 0), (0, LANES - block.shape[1])))

        def inverse(q):
            block = complex_block(*unit(q.reshape(-1)[:, None] * slots[None, :], LANES, 1.0))
            block = block.reshape(2, *q.shape, 2 * LANES).transpose(1, 0, 2, 3).reshape(-1, 2 * LANES)
            return np.pad(block * scale, ((0, LANES - block.shape[0]), (0, 0)))

        fwd_all.append(halves(np.concatenate([forward(freqs), forward(extra)], axis=1)))
        inv_all.append(halves(inverse(freqs)))
        inv_extra.append(halves(inverse(extra)))
    return jnp.stack(fwd_all), jnp.stack(inv_all + inv_extra)


def half_body(n_row, n_sub, residual_in, direction, spectrum, noise_var):
    _, rows, grid_len = direction.shape
    embed = 2 * grid_len
    low = embed // LANES
    n = n_row * n_sub
    g = n // 2
    per = LANES // n
    f32 = jnp.float32
    vmem = pl.BlockSpec(memory_space=pltpu.VMEM)
    away = pl.BlockSpec(memory_space=pl.ANY)
    chunks, pieces = CHUNKS, PIECES
    count = low // chunks
    lanes = spectrum.shape[1]
    row_fwd, row_inv = half_tables(embed, n_row, n_sub)
    _, _, col_fwd, col_inv, _, _, tall_cos, tall_sin = make_tables(embed, n, per)
    col_inv = halves(complex_block(*unit(np.arange(LANES)[:, None] * np.arange(LANES)[None, :], LANES, 1.0)).reshape(2 * LANES, 2 * LANES))
    tile = (count, 2 * per, LANES)
    dma = pltpu.SemaphoreType.DMA
    residual_out, direction_out, steps = pl.pallas_call(
        functools.partial(half_kernel, low, chunks, pieces, n_row, n_sub),
        out_shape=[
            jax.ShapeDtypeStruct(direction.shape, f32),
            jax.ShapeDtypeStruct(direction.shape, f32),
            jax.ShapeDtypeStruct((2, LANES), f32),
        ],
        in_specs=[vmem, away, away, pl.BlockSpec(memory_space=pltpu.SMEM)] + [vmem] * 6,
        out_specs=[vmem] * 3,
        scratch_shapes=[
            pltpu.VMEM(direction.shape, f32),
            pltpu.VMEM((lanes // LANES, embed, LANES), f32),
            pltpu.VMEM((low, lanes, LANES), f32),
            pltpu.VMEM((low, rows, 2 * LANES), f32),
            pltpu.VMEM((low, count, per, 2 * LANES), f32),
            pltpu.VMEM((chunks, 2, g, *tile), f32),
            pltpu.VMEM((chunks, n, *tile), f32),
            pltpu.VMEM((chunks, n, *tile), f32),
            pltpu.VMEM((chunks, 2, g, *tile), f32),
            pltpu.VMEM((rows, grid_len), f32),
            pltpu.VMEM((rows, grid_len), f32),
            pltpu.VMEM((rows, grid_len), f32),
            pltpu.VMEM((n_row, 8, LANES), f32),
            pltpu.VMEM((g, 8, LANES), f32),
            pltpu.VMEM((g, 8, LANES), f32),
            pltpu.VMEM((n_row, 8, LANES), f32),
            pltpu.VMEM((n, 2, 8, LANES), f32),
            pltpu.VMEM((2, 8, LANES), f32),
            dma((1 + lanes // LANES,)),
            dma((pieces,)), dma((pieces,)), dma((pieces,)), dma((pieces,)),
            dma((chunks, 2, g)), dma((chunks, 2, g)), dma((chunks, 2, g)), dma((chunks, 2, g)),
            dma((n_row,)), dma((g,)), dma((g,)), dma((n_row,)),
            dma((n,)), dma((n,)),
        ],
        compiler_params=params(collective_id=1, has_side_effects=True),
        name="cg_step",
    )(direction, residual_in, spectrum, noise_var, row_fwd, row_inv, col_fwd, col_inv, tall_cos, tall_sin)
    return residual_out, direction_out, steps[:, 0]


def solution(mesh):
    n_row, n_sub = mesh.shape["row"], mesh.shape["sub"]

    def body(residual_in, direction, spectrum, noise_var):
        embed = spectrum.shape[0]
        low = embed // LANES
        per = LANES // (n_row * n_sub)
        whole = direction.shape[1] == LANES and direction.shape[2] == LANES * n_row * n_sub
        if whole and per % 8 == 0 and n_sub % 2 == 0:
            return half_body(n_row, n_sub, residual_in, direction, spectrum, noise_var)
        weights = spectrum.reshape(LANES, low, per, low).transpose(1, 3, 2, 0)
        return pair_body(n_row, n_sub, residual_in, direction, weights, noise_var)

    placed = P("grp", ("row", "sub"), None)
    return jax.shard_map(
        body,
        mesh=mesh,
        in_specs=(placed, placed, P("grp", ("row", "sub")), P("grp")),
        out_specs=(placed, placed, P("grp")),
        check_vma=False,
    )
```

```python
import functools
import math

import jax
import jax.numpy as jnp
import numpy as np
from jax import lax
from jax.experimental import pallas as pl
from jax.experimental.pallas import tpu as pltpu
from jax.sharding import PartitionSpec as P

LANES = 128
TINY = 1e-06
CHUNKS = 4
PIECES = 4
HALF_GRANT = 48 * 1024 * 1024
MESH = pl.DeviceIdType.MESH
GRANT = 60 * 1024 * 1024


def unit(turns, modulus, orient):
    angle = orient * 2.0 * np.pi * (np.asarray(turns) % modulus) / modulus
    return np.cos(angle), np.sin(angle)


def halves(table):
    table = np.asarray(table, np.float32)
    hi = table.astype(jnp.bfloat16)
    lo = (table - hi.astype(np.float32)).astype(jnp.bfloat16)
    return jnp.asarray(np.stack([hi, lo]))


def complex_block(cos_part, sin_part):
    return np.stack(
        [np.stack([cos_part, sin_part], 1), np.stack([-sin_part, cos_part], 1)], 0
    )


def split(x):
    hi = x.astype(jnp.bfloat16)
    return hi, (x - hi.astype(jnp.float32)).astype(jnp.bfloat16)


def dot(a, b):
    return jnp.dot(a, b, preferred_element_type=jnp.float32)


def dot_right(x, table_ref):
    hi, lo = split(x)
    return dot(hi, table_ref[0]) + (dot(lo, table_ref[0]) + dot(hi, table_ref[1]))


def dot_left(table_ref, x):
    hi, lo = split(x)
    return dot(table_ref[0], hi) + (dot(table_ref[0], lo) + dot(table_ref[1], hi))


def turn(z, k, n, orient):
    k = k % n
    re, im = z
    if k == 0:
        return z
    if 2 * k == n:
        return -re, -im
    if 4 * k == n or 4 * k == 3 * n:
        sign = orient if 4 * k == n else -orient
        return (-im, re) if sign > 0 else (im, -re)
    c = math.cos(2 * math.pi * k / n)
    s = orient * math.sin(2 * math.pi * k / n)
    return re * c - im * s, re * s + im * c


def add(u, v):
    return u[0] + v[0], u[1] + v[1]


def sub(u, v):
    return u[0] - v[0], u[1] - v[1]


def butterflies(xs, orient):
    n = len(xs)
    if n == 1:
        return xs
    even = butterflies(xs[0::2], orient)
    odd = butterflies(xs[1::2], orient)
    odd = [turn(z, k, n, orient) for k, z in enumerate(odd)]
    return [add(e, o) for e, o in zip(even, odd)] + [sub(e, o) for e, o in zip(even, odd)]


def padded_forward(xs):
    n = len(xs)
    even = butterflies(xs, -1)
    odd = butterflies([turn(z, a, 2 * n, -1) for a, z in enumerate(xs)], -1)
    return [even[i // 2] if i % 2 == 0 else odd[i // 2] for i in range(2 * n)]


def cut_inverse(zs):
    n = len(zs) // 2
    even = butterflies(zs[0::2], 1)
    odd = butterflies(zs[1::2], 1)
    return [add(even[a], turn(odd[a], a, 2 * n, 1)) for a in range(n)]


def rotate(re, im, c, s):
    return re * c - im * s, re * s + im * c


def row_kernel(low, groups, dir_ref, table_ref, cos_ref, sin_ref, *rest):
    outs, work, turned = rest[:-2], rest[-2], rest[-1]
    half = low // 2
    rows = dir_ref.shape[1]
    for c in range(2):
        for a in range(half):
            turned[a, c] = dir_ref[c, :, a * LANES : (a + 1) * LANES].T

    def spread(t, carry):
        at = pl.ds(pl.multiple_of(t * 8, 8), 8)
        xs = [(turned[a, 0, at, :], turned[a, 1, at, :]) for a in range(half)]
        cos_rows, sin_rows = cos_ref[at, :], sin_ref[at, :]
        for m, (re, im) in enumerate(padded_forward(xs)):
            re, im = rotate(re, im, cos_rows[:, m : m + 1], sin_rows[:, m : m + 1])
            work[m, 0, at, :] = re
            work[m, 1, at, :] = im
        return carry

    lax.fori_loop(0, LANES // 8, spread, 0)
    per_chunk = low // len(outs)
    for i, out in enumerate(outs):

        def column(m, carry):
            got = dot_left(table_ref, work[i * per_chunk + m].reshape(2 * LANES, rows))
            size = 2 * LANES // groups
            for j in range(groups):
                out[j, m] = got[j * size : (j + 1) * size]
            return carry

        lax.fori_loop(0, per_chunk, column, 0)


def column_kernel(low, per, x_ref, w_ref, fwd_ref, inv_ref, cos_ref, sin_ref, out_ref, work):
    half = low // 2
    count = x_ref.shape[1]

    def spread(m, carry):
        xs = [(x_ref[a, m, :per], x_ref[a, m, per:]) for a in range(half)]
        for k, (re, im) in enumerate(padded_forward(xs)):
            re, im = rotate(re, im, cos_ref[k : k + 1, :], sin_ref[k : k + 1, :])
            work[k, m, :, :LANES] = re
            work[k, m, :, LANES:] = im
        return carry

    lax.fori_loop(0, count, spread, 0)

    def filtered(k, carry):
        spectral = dot_right(work[k].reshape(count * per, 2 * LANES), fwd_ref)
        weights = w_ref[k].reshape(count * per, LANES)
        spectral = spectral * jnp.concatenate([weights, weights], axis=1)
        got = dot_right(spectral, inv_ref)
        cos_row, sin_row = cos_ref[pl.ds(k, 1), :], sin_ref[pl.ds(k, 1), :]
        re, im = rotate(got[:, :LANES], got[:, LANES:], cos_row, -sin_row)
        work[k, :, :, :LANES] = re.reshape(count, per, LANES)
        work[k, :, :, LANES:] = im.reshape(count, per, LANES)
        return carry

    lax.fori_loop(0, low, filtered, 0)

    def gather(m, carry):
        zs = [(work[k, m, :, :LANES], work[k, m, :, LANES:]) for k in range(low)]
        for a, (re, im) in enumerate(cut_inverse(zs)):
            out_ref[a, m, :per] = re
            out_ref[a, m, per:] = im
        return carry

    lax.fori_loop(0, count, gather, 0)


def image_kernel(low, groups, chunks, *refs):
    ins = refs[:chunks]
    dir_ref, res_ref, noise_ref, table_ref, cos_ref, sin_ref = refs[chunks : chunks + 6]
    image_ref, sums_ref, work, applied = refs[chunks + 6 :]
    half = low // 2
    rows = dir_ref.shape[1]
    per_chunk = low // chunks
    for i, x_ref in enumerate(ins):

        def column(m, carry):
            parts = [x_ref[j, m] for j in range(groups)]
            got = dot_left(table_ref, parts[0] if groups == 1 else jnp.concatenate(parts, axis=0))
            work[i * per_chunk + m] = got.reshape(2, LANES, rows)
            return carry

        lax.fori_loop(0, per_chunk, column, 0)

    def gather(t, carry):
        at = pl.ds(pl.multiple_of(t * 8, 8), 8)
        cos_rows, sin_rows = cos_ref[at, :], sin_ref[at, :]
        zs = []
        for m in range(low):
            zs.append(
                rotate(work[m, 0, at, :], work[m, 1, at, :], cos_rows[:, m : m + 1], -sin_rows[:, m : m + 1])
            )
        for a, (re, im) in enumerate(cut_inverse(zs)):
            applied[a, 0, at, :] = re
            applied[a, 1, at, :] = im
        return carry

    lax.fori_loop(0, LANES // 8, gather, 0)
    noise = noise_ref[0]
    for c in range(2):
        totals = [jnp.zeros((rows, LANES), jnp.float32)] * 4
        for a in range(half):
            cols = slice(a * LANES, (a + 1) * LANES)
            d, r = dir_ref[c, :, cols], res_ref[c, :, cols]
            image = applied[a, c].T + noise * d
            image_ref[c, :, cols] = image
            for s, term in enumerate((r * r, d * image, r * image, image * image)):
                totals[s] = totals[s] + term
        for s in range(4):
            sums_ref[4 * c + s : 4 * c + s + 1, :] = jnp.sum(totals[s], axis=0, keepdims=True)


def update_kernel(n_row, n_sub, sums_ref, image_ref, dir_ref, res_ref, r_out, d_out, s_out, held, send_sem, recv_sem):
    n = n_row * n_sub
    me = lax.axis_index("row") * n_sub + lax.axis_index("sub")

    def place(o):
        peer = lax.rem(me + o, n)
        return {"row": peer // n_sub, "sub": lax.rem(peer, n_sub)}

    barrier = pltpu.get_barrier_semaphore()

    def greet(o, carry):
        pl.semaphore_signal(barrier, inc=1, device_id=place(o), device_id_type=MESH)
        return carry

    lax.fori_loop(1, n, greet, 0)
    pl.semaphore_wait(barrier, n - 1)

    def copy(o):
        return pltpu.make_async_remote_copy(
            src_ref=sums_ref,
            dst_ref=held.at[me],
            send_sem=send_sem.at[o],
            recv_sem=recv_sem.at[o],
            device_id=place(o),
            device_id_type=MESH,
        )

    def start(o, carry):
        copy(o).start()
        return carry

    lax.fori_loop(1, n, start, 0)
    held[me] = sums_ref[...]

    def finish(o, carry):
        copy(o).wait()
        return carry

    lax.fori_loop(1, n, finish, 0)
    total = jnp.sum(jnp.sum(held[...], axis=0), axis=1, keepdims=True)
    for c in range(2):
        old, curve, cross, square = [total[4 * c + s : 4 * c + s + 1] for s in range(4)]
        step = old / curve
        new = jnp.maximum(old - 2.0 * step * cross + step * step * square, 0.0)
        beta = new / (old + TINY)
        s_out[c : c + 1, :] = jnp.broadcast_to(step, (1, LANES))
        rows = min(8, res_ref.shape[1])

        def strip(t, carry):
            at = pl.ds(pl.multiple_of(t * rows, rows), rows)
            r = res_ref[c, at, :] - step * image_ref[c, at, :]
            r_out[c, at, :] = r
            d_out[c, at, :] = r + beta * dir_ref[c, at, :]
            return carry

        lax.fori_loop(0, res_ref.shape[1] // rows, strip, 0)


def params(**more):
    return pltpu.CompilerParams(vmem_limit_bytes=GRANT, **more)


def make_tables(embed, n, per):
    low, f32 = embed // LANES, jnp.float32
    slots, seconds = np.arange(LANES), np.arange(low)
    turn_cos, turn_sin = unit(slots[:, None] * seconds[None, :], embed, -1.0)
    wide_cos, wide_sin = jnp.asarray(turn_cos, f32), jnp.asarray(turn_sin, f32)
    tall_cos, tall_sin = jnp.asarray(turn_cos.T, f32), jnp.asarray(turn_sin.T, f32)
    fwd = complex_block(*unit(slots[:, None] * slots[None, :], LANES, -1.0))
    inv = complex_block(*unit(slots[:, None] * slots[None, :], LANES, 1.0))
    scale = 1.0 / (embed * embed)
    col_fwd = halves(fwd.reshape(2 * LANES, 2 * LANES))
    col_inv = halves(inv.reshape(2 * LANES, 2 * LANES) * scale)
    row_fwd = halves(
        fwd.reshape(2, LANES, 2, n, per).transpose(3, 2, 4, 0, 1).reshape(2 * LANES, 2 * LANES)
    )
    row_inv = halves(
        inv.reshape(2, n, per, 2, LANES).transpose(3, 4, 1, 0, 2).reshape(2 * LANES, 2 * LANES)
    )
    return row_fwd, row_inv, col_fwd, col_inv, wide_cos, wide_sin, tall_cos, tall_sin


def pair_body(n_row, n_sub, residual_in, direction, weights, noise_var):
    _, rows, grid_len = direction.shape
    embed = 2 * grid_len
    low, half = embed // LANES, grid_len // LANES
    n = n_row * n_sub
    per = LANES // n
    f32 = jnp.float32
    vmem = pl.BlockSpec(memory_space=pltpu.VMEM)
    chunks = CHUNKS
    per_chunk = low // chunks
    aligned = (2 * per) % 8 == 0
    groups = n if aligned else 1

    row_fwd, row_inv, col_fwd, col_inv, wide_cos, wide_sin, tall_cos, tall_sin = make_tables(embed, n, per)

    spread = pl.pallas_call(
        functools.partial(row_kernel, low, groups),
        out_shape=[jax.ShapeDtypeStruct((groups, per_chunk, 2 * LANES // groups, rows), f32)] * chunks,
        in_specs=[vmem] * 4,
        out_specs=[vmem] * chunks,
        scratch_shapes=[pltpu.VMEM((low, 2, LANES, rows), f32), pltpu.VMEM((half, 2, LANES, rows), f32)],
        compiler_params=params(),
        name="rows_out",
    )(direction, row_fwd, wide_cos, wide_sin)

    def swap(x):
        return lax.all_to_all(x, ("row", "sub"), split_axis=0, concat_axis=0, tiled=True)

    back = []
    for i, x in enumerate(spread):
        if not aligned:
            x = x.reshape(per_chunk, n, 2 * per, rows).transpose(1, 0, 2, 3)
        x = swap(x)
        if rows != LANES:
            x = x.reshape(half, LANES // rows, per_chunk, 2 * per, rows).transpose(0, 2, 3, 1, 4)
            x = x.reshape(half, per_chunk, 2 * per, LANES)
        x = pl.pallas_call(
            functools.partial(column_kernel, low, per),
            out_shape=jax.ShapeDtypeStruct((half, per_chunk, 2 * per, LANES), f32),
            in_specs=[vmem] * 6,
            out_specs=vmem,
            scratch_shapes=[pltpu.VMEM((low, per_chunk, per, 2 * LANES), f32)],
            compiler_params=params(),
            name=f"columns{i}",
        )(x, weights[:, i * per_chunk : (i + 1) * per_chunk], col_fwd, col_inv, tall_cos, tall_sin)
        if rows != LANES:
            x = x.reshape(half, per_chunk, 2 * per, LANES // rows, rows).transpose(0, 3, 1, 2, 4)
            x = x.reshape(n, per_chunk, 2 * per, rows)
        x = swap(x)
        if not aligned:
            x = x.transpose(1, 0, 2, 3).reshape(1, per_chunk, 2 * LANES, rows)
        back.append(x)

    image, sums = pl.pallas_call(
        functools.partial(image_kernel, low, groups, chunks),
        out_shape=[jax.ShapeDtypeStruct(direction.shape, f32), jax.ShapeDtypeStruct((8, LANES), f32)],
        in_specs=[vmem] * (chunks + 2) + [pl.BlockSpec(memory_space=pltpu.SMEM)] + [vmem] * 3,
        out_specs=[vmem] * 2,
        scratch_shapes=[pltpu.VMEM((low, 2, LANES, rows), f32), pltpu.VMEM((half, 2, LANES, rows), f32)],
        compiler_params=params(),
        name="rows_back",
    )(*back, direction, residual_in, noise_var, row_inv, wide_cos, wide_sin)

    residual_out, direction_out, steps = pl.pallas_call(
        functools.partial(update_kernel, n_row, n_sub),
        out_shape=[
            jax.ShapeDtypeStruct(direction.shape, f32),
            jax.ShapeDtypeStruct(direction.shape, f32),
            jax.ShapeDtypeStruct((2, LANES), f32),
        ],
        in_specs=[vmem] * 4,
        out_specs=[vmem] * 3,
        scratch_shapes=[
            pltpu.VMEM((n, 8, LANES), f32),
            pltpu.SemaphoreType.DMA((n,)),
            pltpu.SemaphoreType.DMA((n,)),
        ],
        compiler_params=params(collective_id=0, has_side_effects=True),
        name="update",
    )(sums, image, direction, residual_in)
    return residual_out, direction_out, steps[:, 0]


def odd_terms(d, n):
    q = n // 4
    zs = butterflies([turn((d[a], -d[a + q]), a, n, -1) for a in range(q)], -1)
    return {4 * j + 1: z for j, z in enumerate(zs)}


def real_forward(xs):
    n = len(xs)
    if n == 1:
        return {0: (xs[0], None)}
    if n == 2:
        return {0: (xs[0] + xs[1], None), 1: (xs[0] - xs[1], None)}
    h = n // 2
    out = {2 * k: z for k, z in real_forward([xs[a] + xs[a + h] for a in range(h)]).items()}
    out.update(odd_terms([xs[a] - xs[a + h] for a in range(h)], n))
    return out


def real_padded(xs):
    n = 2 * len(xs)
    out = {2 * k: z for k, z in real_forward(xs).items()}
    out.update(odd_terms(xs, n))
    return out


def odd_values(pairs, n):
    q = n // 4
    zs = [turn(z, a, n, 1) for a, z in enumerate(butterflies([pairs[4 * j + 1] for j in range(q)], 1))]
    return [z[0] for z in zs] + [-z[1] for z in zs]


def real_inverse(pairs, n):
    if n == 1:
        return [pairs[0][0]]
    if n == 2:
        return [pairs[0][0] + pairs[1][0], pairs[0][0] - pairs[1][0]]
    even = real_inverse({k // 2: z for k, z in pairs.items() if k % 2 == 0}, n // 2)
    odd = odd_values(pairs, n)
    return [e + o for e, o in zip(even, odd)] + [e - o for e, o in zip(even, odd)]


def real_cut(pairs, n):
    even = real_inverse({k // 2: z for k, z in pairs.items() if k % 2 == 0}, n // 2)
    return [e + o for e, o in zip(even, odd_values(pairs, n))]


def real_names(n):
    if n <= 2:
        return list(range(n))
    return [2 * k for k in real_names(n // 2)] + list(range(1, n, 4))


def loop(first, last, step):
    def run(i, carry):
        step(i)
        return carry

    lax.fori_loop(first, last, run, 0)


def half_kernel(
    low, chunks, pieces, n_row, n_sub,
    dir_hbm, res_hbm, spec_hbm, noise_ref, row_fwd_hbm, row_inv_hbm, col_fwd_hbm, col_inv_hbm, tall_cos, tall_sin,
    image_ref, dir_ref, res_ref, coef_ref,
    spec_ref, row_fwd, row_inv, col_fwd, col_inv,
    weights, work, cols, send, recv, back_send, back_recv,
    raw_in, img_send, img_in, x_send, x_recv, xb_send, xb_recv, held, sums_ref,
    load_sem, raw_ssem, raw_rsem, img_ssem, img_rsem, send_sem, recv_sem, back_ssem, back_rsem,
    x_ssem, x_rsem, xb_ssem, xb_rsem, sum_ssem, sum_rsem,
):
    n = n_row * n_sub
    hs = n_sub // 2
    g = n_row * hs
    half = low // 2
    count = low // chunks
    per = LANES // n
    size = 2 * per
    step_rows = LANES // pieces
    my_r, my_s = lax.axis_index("row"), lax.axis_index("sub")
    h = my_s // hs
    gi = my_r * hs + lax.rem(my_s, hs)
    me = my_r * n_sub + my_s
    mate_s = n_sub - 1 - my_s
    mate = {"row": my_r, "sub": mate_s}
    slabs = [me, my_r * n_sub + mate_s]
    lead = my_s == h * hs

    def place(o):
        peer = lax.rem(me + o, n)
        return {"row": peer // n_sub, "sub": lax.rem(peer, n_sub)}

    def ally(d, part):
        r, s = d // hs, part * hs + lax.rem(d, hs)
        return {"row": r, "sub": s}, [r * n_sub + s, r * n_sub + n_sub - 1 - s]

    def leader(e):
        return {"row": e, "sub": (1 - h) * hs}

    barrier = pltpu.get_barrier_semaphore()
    loop(
        1, n,
        lambda o: pl.semaphore_signal(barrier, inc=1, device_id=place(o), device_id_type=MESH),
    )

    def load(src, dst, slot):
        return pltpu.make_async_copy(src, dst, load_sem.at[slot])

    load_dir = [load(dir_hbm.at[c], dir_ref.at[c], s) for s, c in enumerate((h, 1 - h))]
    load_fwd = load(row_fwd_hbm, row_fwd, 2)
    load_rest = [
        load(src, dst, 3 + s)
        for s, (src, dst) in enumerate(
            ((row_inv_hbm, row_inv), (col_fwd_hbm, col_fwd), (col_inv_hbm, col_inv), (res_hbm, res_ref))
        )
    ]
    load_spec = [
        load(spec_hbm.at[:, pl.ds(s * LANES, LANES)], spec_ref.at[s], 7 + s) for s in range(spec_ref.shape[0])
    ]
    load_dir[0].start()
    load_fwd.start()
    for one in load_spec:
        one.start()
    for one in load_rest:
        one.start()
    load_dir[1].start()

    def remote(src, dst, s_sem, r_sem, device):
        return pltpu.make_async_remote_copy(
            src_ref=src, dst_ref=dst, send_sem=s_sem, recv_sem=r_sem, device_id=device, device_id_type=MESH
        )

    def raw_copy(p):
        at = pl.ds(pl.multiple_of(p * step_rows, step_rows), step_rows)
        return remote(dir_hbm.at[1 - h, at, :], raw_in.at[at, :], raw_ssem.at[p], raw_rsem.at[p], mate)

    def img_copy(p):
        at = pl.ds(pl.multiple_of(p * step_rows, step_rows), step_rows)
        return remote(img_send.at[at, :], img_in.at[at, :], img_ssem.at[p], img_rsem.at[p], mate)

    def ahead(i, b, o):
        p = lax.rem(gi + o, g)
        return remote(
            send.at[i, b, p], recv.at[i, slabs[b]], send_sem.at[i, b, o], recv_sem.at[i, b, o], ally(p, h)[0]
        )

    def home(i, b, o):
        p = lax.rem(gi + o, g)
        device, places = ally(p, h)
        return remote(
            back_send.at[i, places[b]], back_recv.at[i, b, gi], back_ssem.at[i, b, o], back_rsem.at[i, b, o], device
        )

    def x_ahead(e):
        return remote(x_send.at[e], x_recv.at[gi], x_ssem.at[e], x_rsem.at[gi], leader(e))

    def x_arrival(d):
        return remote(x_send.at[0], x_recv.at[d], x_ssem.at[0], x_rsem.at[d], mate)

    def x_home(d):
        return remote(xb_send.at[d], xb_recv.at[my_r], xb_ssem.at[d], xb_rsem.at[my_r], ally(d, 1 - h)[0])

    def x_back(e):
        return remote(xb_send.at[0], xb_recv.at[e], xb_ssem.at[0], xb_rsem.at[e], mate)

    pl.semaphore_wait(barrier, n - 1)
    loop(0, pieces, lambda p: raw_copy(p).start())

    def row_strip(read, t):
        at = pl.ds(pl.multiple_of(t * 8, 8), 8)
        found = real_padded([read(at, slice(a * LANES, (a + 1) * LANES)) for a in range(half)])
        for m in range(low):
            c, s = tall_cos[m : m + 1, :], tall_sin[m : m + 1, :]
            re, im = found[m] if m in found else found[low - m]
            if im is None:
                re, im = re * c, re * s
            elif m in found:
                re, im = rotate(re, im, c, s)
            else:
                re, im = re * c + im * s, re * s - im * c
            work[m, at, :LANES] = re
            work[m, at, LANES:] = im

    batch = min(4, count)

    def row_dots(x, table, at):
        hi, lo = split(x)
        return dot(hi, table[h, 0, :, at]) + (dot(lo, table[h, 0, :, at]) + dot(hi, table[h, 1, :, at]))

    def row_extras(b):
        got = row_dots(work[0], row_fwd, slice(LANES, 2 * LANES)).T
        for e in range(n_row):
            x_send[e, 2 * b : 2 * b + 2, :] = got[2 * e : 2 * e + 2]

    def send_chunk(i, b):
        def columns(t):
            m = t * batch
            x = work[pl.ds(i * count + m, batch)].reshape(batch * LANES, 2 * LANES)
            got = row_dots(x, row_fwd, slice(0, LANES))
            for k in range(batch):
                part = got[k * LANES : (k + 1) * LANES].T
                for d in range(g):
                    send[i, b, d, m + k] = part[d * size : (d + 1) * size]

        loop(0, count // batch, columns)
        recv[i, slabs[b]] = send[i, b, gi]
        loop(1, g, lambda o: ahead(i, b, o).start())

    load_dir[0].wait()
    load_fwd.wait()
    loop(0, LANES // 8, lambda t: row_strip(lambda at, cs: dir_ref[h, at, cs], t))
    row_extras(0)
    loop(0, chunks, lambda i: send_chunk(i, 0))

    for one in load_spec:
        one.wait()

    def turn_spectrum(k):
        for s in range(spec_ref.shape[0]):
            part = spec_ref[s, pl.ds(k, LANES, stride=low), :]
            weights[k, s * LANES : (s + 1) * LANES, :] = part.T

    loop(0, low, turn_spectrum)
    for one in load_rest:
        one.wait()
    load_dir[1].wait()

    def raw_piece(p):
        raw_copy(p).wait_recv()
        loop(
            p * (step_rows // 8), (p + 1) * (step_rows // 8),
            lambda t: row_strip(lambda at, cs: raw_in[at, cs], t),
        )

    loop(0, pieces, raw_piece)
    row_extras(1)
    loop(0, n_row, lambda e: x_ahead(e).start())
    loop(0, chunks, lambda i: send_chunk(i, 1))

    wide = 8

    def fix_in():
        def one(d):
            x_arrival(d).wait_recv()
            for b, place_in in enumerate(ally(d, 1 - h)[1]):
                re, im = x_recv[d, 2 * b : 2 * b + 1, :], x_recv[d, 2 * b + 1 : 2 * b + 2, :]
                recv[0, place_in, 0, 0:1, :] = recv[0, place_in, 0, 0:1, :] - im
                recv[0, place_in, 0, per : per + 1, :] = recv[0, place_in, 0, per : per + 1, :] + re

        loop(0, g, one)

    def fix_out():
        def one(d):
            for b, place_in in enumerate(ally(d, 1 - h)[1]):
                re = 0.5 * back_send[0, place_in, 0, 0:1, :]
                im = 0.5 * back_send[0, place_in, 0, per : per + 1, :]
                back_send[0, place_in, 0, 0:1, :] = re
                back_send[0, place_in, 0, per : per + 1, :] = im
                xb_send[d, 2 * b : 2 * b + 1, :] = im
                xb_send[d, 2 * b + 1 : 2 * b + 2, :] = -re
            x_home(d).start()

        loop(0, g, one)

    def column_chunk(i):
        for b in range(2):
            loop(1, g, lambda o: ahead(i, b, o).wait_recv())
        pl.when(jnp.logical_and(i == 0, lead))(fix_in)

        def spread(m):
            xs = [(recv[i, a, m, :per], recv[i, a, m, per:]) for a in range(half)]
            for k, (re, im) in enumerate(padded_forward(xs)):
                re, im = rotate(re, im, tall_cos[k : k + 1, :], tall_sin[k : k + 1, :])
                cols[k, m, :, :LANES] = re
                cols[k, m, :, LANES:] = im

        loop(0, count, spread)
        block = count * per

        def filtered(t):
            k = t * wide
            spectral = dot_right(cols[pl.ds(k, wide)].reshape(wide * block, 2 * LANES), col_fwd)
            scale = jnp.concatenate(
                [
                    weights[k + w, pl.ds(i * count + m, per, stride=low), :]
                    for w in range(wide)
                    for m in range(count)
                ],
                axis=0,
            )
            spectral = spectral * jnp.concatenate([scale, scale], axis=1)
            got = dot_right(spectral, col_inv)
            for w in range(wide):
                cos_row, sin_row = tall_cos[pl.ds(k + w, 1), :], tall_sin[pl.ds(k + w, 1), :]
                part = got[w * block : (w + 1) * block]
                re, im = rotate(part[:, :LANES], part[:, LANES:], cos_row, -sin_row)
                cols[k + w, :, :, :LANES] = re.reshape(count, per, LANES)
                cols[k + w, :, :, LANES:] = im.reshape(count, per, LANES)

        loop(0, low // wide, filtered)

        def gather(m):
            zs = [(cols[k, m, :, :LANES], cols[k, m, :, LANES:]) for k in range(low)]
            for a, (re, im) in enumerate(cut_inverse(zs)):
                back_send[i, a, m, :per] = re
                back_send[i, a, m, per:] = im

        loop(0, count, gather)
        pl.when(jnp.logical_and(i == 0, lead))(fix_out)
        for b in range(2):
            back_recv[i, b, gi] = back_send[i, slabs[b]]
        loop(1, g, lambda o: home(i, 1, o).start())

    loop(0, chunks, column_chunk)
    loop(0, chunks, lambda i: loop(1, g, lambda o: home(i, 0, o).start()))
    loop(0, n_row, lambda e: x_back(e).wait_recv())

    def take_chunk(i, b):
        loop(1, g, lambda o: home(i, b, o).wait_recv())

        def columns(t):
            m = t * batch
            parts = []
            for k in range(batch):
                parts.append(jnp.concatenate([back_recv[i, b, d, m + k] for d in range(g)], axis=0).T)
            got = row_dots(jnp.concatenate(parts, axis=0), row_inv, slice(None))
            work[pl.ds(i * count + m, batch)] = got.reshape(batch, LANES, 2 * LANES)

        loop(0, count // batch, columns)

    def take_extras(b):
        parts = [xb_recv[e, 2 * b : 2 * b + 2, :] for e in range(n_row)]
        parts.append(jnp.zeros((LANES - 2 * n_row, LANES), jnp.float32))
        x = jnp.concatenate(parts, axis=0).T
        hi, lo = split(x)
        first, second = row_inv[2 + h, 0], row_inv[2 + h, 1]
        work[0] = work[0] + (dot(hi, first) + (dot(lo, first) + dot(hi, second)))

    def back_strip(t):
        at = pl.ds(pl.multiple_of(t * 8, 8), 8)

        def entry(m):
            re, im = work[m, at, :LANES], work[m, at, LANES:]
            return rotate(re, im, tall_cos[m : m + 1, :], -tall_sin[m : m + 1, :])

        pairs = {}
        for m in real_names(low):
            re, im = entry(m)
            if m in (0, half):
                pairs[m] = (re, None)
            else:
                re_too, im_too = entry(low - m)
                pairs[m] = (re + re_too, im - im_too)
        return at, real_cut(pairs, low)

    loop(0, chunks, lambda i: take_chunk(i, 1))
    take_extras(1)

    def img_piece(p):
        def strip(t):
            at, xs = back_strip(t)
            for a, x in enumerate(xs):
                img_send[at, a * LANES : (a + 1) * LANES] = x

        loop(p * (step_rows // 8), (p + 1) * (step_rows // 8), strip)
        img_copy(p).start()

    loop(0, pieces, img_piece)
    loop(0, chunks, lambda i: take_chunk(i, 0))
    take_extras(0)
    noise = noise_ref[0]

    def tally(c, at, a, applied, totals):
        cs = slice(a * LANES, (a + 1) * LANES)
        d, r = dir_ref[c, at, cs], res_ref[c, at, cs]
        image = applied + noise * d
        image_ref[c, at, cs] = image
        terms = (r * r, d * image, r * image, image * image)
        return [total + term for total, term in zip(totals, terms)]

    def own_strip(t, totals):
        at, xs = back_strip(t)
        for a, x in enumerate(xs):
            totals = tally(h, at, a, x, totals)
        return totals

    def far_strip(t, totals):
        at = pl.ds(pl.multiple_of(t * 8, 8), 8)
        for a in range(half):
            totals = tally(1 - h, at, a, img_in[at, a * LANES : (a + 1) * LANES], totals)
        return totals

    zeros = [jnp.zeros((8, LANES), jnp.float32)] * 4

    def keep(c, totals):
        for s in range(4):
            sums_ref[c, s : s + 1, :] = jnp.sum(totals[s], axis=0, keepdims=True)

    sums_ref[...] = jnp.zeros_like(sums_ref)
    keep(h, lax.fori_loop(0, LANES // 8, own_strip, zeros))

    def far_piece(p, totals):
        img_copy(p).wait_recv()
        return lax.fori_loop(p * (step_rows // 8), (p + 1) * (step_rows // 8), far_strip, totals)

    keep(1 - h, lax.fori_loop(0, pieces, far_piece, zeros))

    def share(o):
        return remote(sums_ref, held.at[me], sum_ssem.at[o], sum_rsem.at[o], place(o))

    held[me] = sums_ref[...]
    loop(1, n, lambda o: share(o).start())

    def drain(i):
        for b in range(2):
            loop(1, g, lambda o: ahead(i, b, o).wait_send())
            loop(1, g, lambda o: home(i, b, o).wait_send())

    loop(0, chunks, drain)
    loop(0, n_row, lambda e: x_ahead(e).wait_send())
    pl.when(lead)(lambda: loop(0, g, lambda d: x_home(d).wait_send()))
    loop(0, pieces, lambda p: raw_copy(p).wait_send())
    loop(0, pieces, lambda p: img_copy(p).wait_send())
    loop(1, n, lambda o: share(o).wait())
    total = jnp.sum(held[...], axis=0)
    for c in range(2):
        line = jnp.sum(total[c], axis=1, keepdims=True)
        old, curve, cross, square = [line[s : s + 1] for s in range(4)]
        step = old / curve
        new = jnp.maximum(old - 2.0 * step * cross + step * step * square, 0.0)
        beta = new / (old + TINY)
        coef_ref[c : c + 1, :] = jnp.broadcast_to(step, (1, LANES))
        coef_ref[2 + c : 3 + c, :] = jnp.broadcast_to(beta, (1, LANES))


def finish_kernel(parts, image_ref, dir_ref, res_ref, coef_ref, r_hbm, d_hbm, s_out, r_ref, d_ref, out_sem):
    probes, rows = image_ref.shape[:2]
    strip_rows = rows // parts

    def stores(k):
        at = pl.ds(pl.multiple_of(lax.rem(k, parts) * strip_rows, strip_rows), strip_rows)
        return [
            pltpu.make_async_copy(src.at[k // parts, at, :], dst.at[k // parts, at, :], out_sem.at[s, k])
            for s, (src, dst) in enumerate(((r_ref, r_hbm), (d_ref, d_hbm)))
        ]

    for c in range(probes):
        s_out[c] = coef_ref[c, 0]

    def work(k):
        c = k // parts
        step, beta = coef_ref[pl.ds(c, 1), 0:1], coef_ref[pl.ds(c + 2, 1), 0:1]

        def strip(t):
            at = pl.ds(pl.multiple_of(lax.rem(k, parts) * strip_rows + t * 8, 8), 8)
            r = res_ref[c, at, :] - step * image_ref[c, at, :]
            r_ref[c, at, :] = r
            d_ref[c, at, :] = r + beta * dir_ref[c, at, :]

        loop(0, strip_rows // 8, strip)
        for one in stores(k):
            one.start()

    def drain(k):
        for one in stores(k):
            one.wait()

    loop(0, probes * parts, work)
    loop(0, probes * parts, drain)


def half_tables(embed, n_row, n_sub):
    low, n, hs = embed // LANES, n_row * n_sub, n_sub // 2
    per = LANES // n
    slots = np.arange(LANES)
    scale = 2.0 / (embed * embed)
    fwd_all, inv_all, inv_extra = [], [], []
    for part in range(2):
        own = [r * n_sub + part * hs + s for r in range(n_row) for s in range(hs)]
        freqs = np.stack([per * j + np.arange(per) for j in own])
        extra = np.array([per * (r * n_sub + (1 - part) * hs) for r in range(n_row)])[:, None]

        def forward(q):
            block = complex_block(*unit(slots[:, None] * q.reshape(-1)[None, :], LANES, -1.0))
            block = block.reshape(2, LANES, 2, *q.shape).transpose(0, 1, 3, 2, 4).reshape(2 * LANES, -1)
            return np.pad(block, ((0, 0), (0, LANES - block.shape[1])))

        def inverse(q):
            block = complex_block(*unit(q.reshape(-1)[:, None] * slots[None, :], LANES, 1.0))
            block = block.reshape(2, *q.shape, 2 * LANES).transpose(1, 0, 2, 3).reshape(-1, 2 * LANES)
            return np.pad(block * scale, ((0, LANES - block.shape[0]), (0, 0)))

        fwd_all.append(halves(np.concatenate([forward(freqs), forward(extra)], axis=1)))
        inv_all.append(halves(inverse(freqs)))
        inv_extra.append(halves(inverse(extra)))
    return jnp.stack(fwd_all), jnp.stack(inv_all + inv_extra)


def half_body(n_row, n_sub, residual_in, direction, spectrum, noise_var):
    _, rows, grid_len = direction.shape
    embed = 2 * grid_len
    low = embed // LANES
    n = n_row * n_sub
    g = n // 2
    per = LANES // n
    f32 = jnp.float32
    vmem = pl.BlockSpec(memory_space=pltpu.VMEM)
    away = pl.BlockSpec(memory_space=pl.ANY)
    chunks, pieces = CHUNKS, PIECES
    count = low // chunks
    lanes = spectrum.shape[1]
    row_fwd, row_inv = half_tables(embed, n_row, n_sub)
    _, _, col_fwd, col_inv, _, _, tall_cos, tall_sin = make_tables(embed, n, per)
    col_inv = halves(complex_block(*unit(np.arange(LANES)[:, None] * np.arange(LANES)[None, :], LANES, 1.0)).reshape(2 * LANES, 2 * LANES))
    tile = (count, 2 * per, LANES)
    dma = pltpu.SemaphoreType.DMA
    whole = pltpu.VMEM(direction.shape, f32)
    kept = pltpu.VMEM(direction.shape, f32)
    image, mine, rest, coef = pl.pallas_call(
        functools.partial(half_kernel, low, chunks, pieces, n_row, n_sub),
        out_shape=[kept, kept, kept, pltpu.VMEM((4, LANES), f32)],
        in_specs=[away, away, away, pl.BlockSpec(memory_space=pltpu.SMEM)] + [away] * 4 + [vmem] * 2,
        out_specs=[vmem] * 4,
        scratch_shapes=[
            pltpu.VMEM((lanes // LANES, embed, LANES), f32),
            *[pltpu.VMEM(table.shape, table.dtype) for table in (row_fwd, row_inv, col_fwd, col_inv)],
            pltpu.VMEM((low, lanes, LANES), f32),
            pltpu.VMEM((low, rows, 2 * LANES), f32),
            pltpu.VMEM((low, count, per, 2 * LANES), f32),
            pltpu.VMEM((chunks, 2, g, *tile), f32),
            pltpu.VMEM((chunks, n, *tile), f32),
            pltpu.VMEM((chunks, n, *tile), f32),
            pltpu.VMEM((chunks, 2, g, *tile), f32),
            pltpu.VMEM((rows, grid_len), f32),
            pltpu.VMEM((rows, grid_len), f32),
            pltpu.VMEM((rows, grid_len), f32),
            pltpu.VMEM((n_row, 8, LANES), f32),
            pltpu.VMEM((g, 8, LANES), f32),
            pltpu.VMEM((g, 8, LANES), f32),
            pltpu.VMEM((n_row, 8, LANES), f32),
            pltpu.VMEM((n, 2, 8, LANES), f32),
            pltpu.VMEM((2, 8, LANES), f32),
            dma((7 + lanes // LANES,)),
            dma((pieces,)), dma((pieces,)), dma((pieces,)), dma((pieces,)),
            dma((chunks, 2, g)), dma((chunks, 2, g)), dma((chunks, 2, g)), dma((chunks, 2, g)),
            dma((n_row,)), dma((g,)), dma((g,)), dma((n_row,)),
            dma((n,)), dma((n,)),
        ],
        compiler_params=pltpu.CompilerParams(
            vmem_limit_bytes=HALF_GRANT, collective_id=1, has_side_effects=True
        ),
        name="cg_step",
    )(direction, residual_in, spectrum, noise_var, row_fwd, row_inv, col_fwd, col_inv, tall_cos, tall_sin)
    parts = PIECES
    residual_out, direction_out, steps = pl.pallas_call(
        functools.partial(finish_kernel, parts),
        out_shape=[
            jax.ShapeDtypeStruct(direction.shape, f32),
            jax.ShapeDtypeStruct(direction.shape, f32),
            jax.ShapeDtypeStruct((2,), f32),
        ],
        in_specs=[vmem] * 4,
        out_specs=[away, away, pl.BlockSpec(memory_space=pltpu.SMEM)],
        scratch_shapes=[whole, whole, dma((2, 2 * parts))],
        compiler_params=pltpu.CompilerParams(vmem_limit_bytes=8 * 1024 * 1024),
        name="finish",
    )(*[pltpu.with_memory_space_constraint(x, pltpu.VMEM) for x in (image, mine, rest, coef)])
    return residual_out, direction_out, steps


def solution(mesh):
    n_row, n_sub = mesh.shape["row"], mesh.shape["sub"]

    def body(residual_in, direction, spectrum, noise_var):
        embed = spectrum.shape[0]
        low = embed // LANES
        per = LANES // (n_row * n_sub)
        whole = direction.shape[1] == LANES and direction.shape[2] == LANES * n_row * n_sub
        if whole and per % 8 == 0 and n_sub % 2 == 0:
            return half_body(n_row, n_sub, residual_in, direction, spectrum, noise_var)
        weights = spectrum.reshape(LANES, low, per, low).transpose(1, 3, 2, 0)
        return pair_body(n_row, n_sub, residual_in, direction, weights, noise_var)

    placed = P("grp", ("row", "sub"), None)
    return jax.shard_map(
        body,
        mesh=mesh,
        in_specs=(placed, placed, P("grp", ("row", "sub")), P("grp")),
        out_specs=(placed, placed, P("grp")),
        check_vma=False,
    )
```

```python
import functools
import math

import jax
import jax.numpy as jnp
import numpy as np
from jax import lax
from jax.experimental import pallas as pl
from jax.experimental.pallas import tpu as pltpu
from jax.sharding import PartitionSpec as P

LANES = 128
TINY = 1e-06
CHUNKS = 8
PIECES = 4
HALF_GRANT = 54 * 1024 * 1024
MESH = pl.DeviceIdType.MESH
GRANT = 60 * 1024 * 1024


def unit(turns, modulus, orient):
    angle = orient * 2.0 * np.pi * (np.asarray(turns) % modulus) / modulus
    return np.cos(angle), np.sin(angle)


def halves(table):
    table = np.asarray(table, np.float32)
    hi = table.astype(jnp.bfloat16)
    lo = (table - hi.astype(np.float32)).astype(jnp.bfloat16)
    return jnp.asarray(np.stack([hi, lo]))


def complex_block(cos_part, sin_part):
    return np.stack(
        [np.stack([cos_part, sin_part], 1), np.stack([-sin_part, cos_part], 1)], 0
    )


def split(x):
    hi = x.astype(jnp.bfloat16)
    return hi, (x - hi.astype(jnp.float32)).astype(jnp.bfloat16)


def dot(a, b):
    return jnp.dot(a, b, preferred_element_type=jnp.float32)


def dot_right(x, table_ref):
    hi, lo = split(x)
    return dot(hi, table_ref[0]) + (dot(lo, table_ref[0]) + dot(hi, table_ref[1]))


def dot_left(table_ref, x):
    hi, lo = split(x)
    return dot(table_ref[0], hi) + (dot(table_ref[0], lo) + dot(table_ref[1], hi))


def turn(z, k, n, orient):
    k = k % n
    re, im = z
    if k == 0:
        return z
    if 2 * k == n:
        return -re, -im
    if 4 * k == n or 4 * k == 3 * n:
        sign = orient if 4 * k == n else -orient
        return (-im, re) if sign > 0 else (im, -re)
    c = math.cos(2 * math.pi * k / n)
    s = orient * math.sin(2 * math.pi * k / n)
    return re * c - im * s, re * s + im * c


def add(u, v):
    return u[0] + v[0], u[1] + v[1]


def sub(u, v):
    return u[0] - v[0], u[1] - v[1]


def butterflies(xs, orient):
    n = len(xs)
    if n == 1:
        return xs
    even = butterflies(xs[0::2], orient)
    odd = butterflies(xs[1::2], orient)
    odd = [turn(z, k, n, orient) for k, z in enumerate(odd)]
    return [add(e, o) for e, o in zip(even, odd)] + [sub(e, o) for e, o in zip(even, odd)]


def padded_forward(xs):
    n = len(xs)
    even = butterflies(xs, -1)
    odd = butterflies([turn(z, a, 2 * n, -1) for a, z in enumerate(xs)], -1)
    return [even[i // 2] if i % 2 == 0 else odd[i // 2] for i in range(2 * n)]


def cut_inverse(zs):
    n = len(zs) // 2
    even = butterflies(zs[0::2], 1)
    odd = butterflies(zs[1::2], 1)
    return [add(even[a], turn(odd[a], a, 2 * n, 1)) for a in range(n)]


def rotate(re, im, c, s):
    return re * c - im * s, re * s + im * c


def row_kernel(low, groups, dir_ref, table_ref, cos_ref, sin_ref, *rest):
    outs, work, turned = rest[:-2], rest[-2], rest[-1]
    half = low // 2
    rows = dir_ref.shape[1]
    for c in range(2):
        for a in range(half):
            turned[a, c] = dir_ref[c, :, a * LANES : (a + 1) * LANES].T

    def spread(t, carry):
        at = pl.ds(pl.multiple_of(t * 8, 8), 8)
        xs = [(turned[a, 0, at, :], turned[a, 1, at, :]) for a in range(half)]
        cos_rows, sin_rows = cos_ref[at, :], sin_ref[at, :]
        for m, (re, im) in enumerate(padded_forward(xs)):
            re, im = rotate(re, im, cos_rows[:, m : m + 1], sin_rows[:, m : m + 1])
            work[m, 0, at, :] = re
            work[m, 1, at, :] = im
        return carry

    lax.fori_loop(0, LANES // 8, spread, 0)
    per_chunk = low // len(outs)
    for i, out in enumerate(outs):

        def column(m, carry):
            got = dot_left(table_ref, work[i * per_chunk + m].reshape(2 * LANES, rows))
            size = 2 * LANES // groups
            for j in range(groups):
                out[j, m] = got[j * size : (j + 1) * size]
            return carry

        lax.fori_loop(0, per_chunk, column, 0)


def column_kernel(low, per, x_ref, w_ref, fwd_ref, inv_ref, cos_ref, sin_ref, out_ref, work):
    half = low // 2
    count = x_ref.shape[1]

    def spread(m, carry):
        xs = [(x_ref[a, m, :per], x_ref[a, m, per:]) for a in range(half)]
        for k, (re, im) in enumerate(padded_forward(xs)):
            re, im = rotate(re, im, cos_ref[k : k + 1, :], sin_ref[k : k + 1, :])
            work[k, m, :, :LANES] = re
            work[k, m, :, LANES:] = im
        return carry

    lax.fori_loop(0, count, spread, 0)

    def filtered(k, carry):
        spectral = dot_right(work[k].reshape(count * per, 2 * LANES), fwd_ref)
        weights = w_ref[k].reshape(count * per, LANES)
        spectral = spectral * jnp.concatenate([weights, weights], axis=1)
        got = dot_right(spectral, inv_ref)
        cos_row, sin_row = cos_ref[pl.ds(k, 1), :], sin_ref[pl.ds(k, 1), :]
        re, im = rotate(got[:, :LANES], got[:, LANES:], cos_row, -sin_row)
        work[k, :, :, :LANES] = re.reshape(count, per, LANES)
        work[k, :, :, LANES:] = im.reshape(count, per, LANES)
        return carry

    lax.fori_loop(0, low, filtered, 0)

    def gather(m, carry):
        zs = [(work[k, m, :, :LANES], work[k, m, :, LANES:]) for k in range(low)]
        for a, (re, im) in enumerate(cut_inverse(zs)):
            out_ref[a, m, :per] = re
            out_ref[a, m, per:] = im
        return carry

    lax.fori_loop(0, count, gather, 0)


def image_kernel(low, groups, chunks, *refs):
    ins = refs[:chunks]
    dir_ref, res_ref, noise_ref, table_ref, cos_ref, sin_ref = refs[chunks : chunks + 6]
    image_ref, sums_ref, work, applied = refs[chunks + 6 :]
    half = low // 2
    rows = dir_ref.shape[1]
    per_chunk = low // chunks
    for i, x_ref in enumerate(ins):

        def column(m, carry):
            parts = [x_ref[j, m] for j in range(groups)]
            got = dot_left(table_ref, parts[0] if groups == 1 else jnp.concatenate(parts, axis=0))
            work[i * per_chunk + m] = got.reshape(2, LANES, rows)
            return carry

        lax.fori_loop(0, per_chunk, column, 0)

    def gather(t, carry):
        at = pl.ds(pl.multiple_of(t * 8, 8), 8)
        cos_rows, sin_rows = cos_ref[at, :], sin_ref[at, :]
        zs = []
        for m in range(low):
            zs.append(
                rotate(work[m, 0, at, :], work[m, 1, at, :], cos_rows[:, m : m + 1], -sin_rows[:, m : m + 1])
            )
        for a, (re, im) in enumerate(cut_inverse(zs)):
            applied[a, 0, at, :] = re
            applied[a, 1, at, :] = im
        return carry

    lax.fori_loop(0, LANES // 8, gather, 0)
    noise = noise_ref[0]
    for c in range(2):
        totals = [jnp.zeros((rows, LANES), jnp.float32)] * 4
        for a in range(half):
            cols = slice(a * LANES, (a + 1) * LANES)
            d, r = dir_ref[c, :, cols], res_ref[c, :, cols]
            image = applied[a, c].T + noise * d
            image_ref[c, :, cols] = image
            for s, term in enumerate((r * r, d * image, r * image, image * image)):
                totals[s] = totals[s] + term
        for s in range(4):
            sums_ref[4 * c + s : 4 * c + s + 1, :] = jnp.sum(totals[s], axis=0, keepdims=True)


def update_kernel(n_row, n_sub, sums_ref, image_ref, dir_ref, res_ref, r_out, d_out, s_out, held, send_sem, recv_sem):
    n = n_row * n_sub
    me = lax.axis_index("row") * n_sub + lax.axis_index("sub")

    def place(o):
        peer = lax.rem(me + o, n)
        return {"row": peer // n_sub, "sub": lax.rem(peer, n_sub)}

    barrier = pltpu.get_barrier_semaphore()

    def greet(o, carry):
        pl.semaphore_signal(barrier, inc=1, device_id=place(o), device_id_type=MESH)
        return carry

    lax.fori_loop(1, n, greet, 0)
    pl.semaphore_wait(barrier, n - 1)

    def copy(o):
        return pltpu.make_async_remote_copy(
            src_ref=sums_ref,
            dst_ref=held.at[me],
            send_sem=send_sem.at[o],
            recv_sem=recv_sem.at[o],
            device_id=place(o),
            device_id_type=MESH,
        )

    def start(o, carry):
        copy(o).start()
        return carry

    lax.fori_loop(1, n, start, 0)
    held[me] = sums_ref[...]

    def finish(o, carry):
        copy(o).wait()
        return carry

    lax.fori_loop(1, n, finish, 0)
    total = jnp.sum(jnp.sum(held[...], axis=0), axis=1, keepdims=True)
    for c in range(2):
        old, curve, cross, square = [total[4 * c + s : 4 * c + s + 1] for s in range(4)]
        step = old / curve
        new = jnp.maximum(old - 2.0 * step * cross + step * step * square, 0.0)
        beta = new / (old + TINY)
        s_out[c : c + 1, :] = jnp.broadcast_to(step, (1, LANES))
        rows = min(8, res_ref.shape[1])

        def strip(t, carry):
            at = pl.ds(pl.multiple_of(t * rows, rows), rows)
            r = res_ref[c, at, :] - step * image_ref[c, at, :]
            r_out[c, at, :] = r
            d_out[c, at, :] = r + beta * dir_ref[c, at, :]
            return carry

        lax.fori_loop(0, res_ref.shape[1] // rows, strip, 0)


def params(**more):
    return pltpu.CompilerParams(vmem_limit_bytes=GRANT, **more)


def make_tables(embed, n, per):
    low, f32 = embed // LANES, jnp.float32
    slots, seconds = np.arange(LANES), np.arange(low)
    turn_cos, turn_sin = unit(slots[:, None] * seconds[None, :], embed, -1.0)
    wide_cos, wide_sin = jnp.asarray(turn_cos, f32), jnp.asarray(turn_sin, f32)
    tall_cos, tall_sin = jnp.asarray(turn_cos.T, f32), jnp.asarray(turn_sin.T, f32)
    fwd = complex_block(*unit(slots[:, None] * slots[None, :], LANES, -1.0))
    inv = complex_block(*unit(slots[:, None] * slots[None, :], LANES, 1.0))
    scale = 1.0 / (embed * embed)
    col_fwd = halves(fwd.reshape(2 * LANES, 2 * LANES))
    col_inv = halves(inv.reshape(2 * LANES, 2 * LANES) * scale)
    row_fwd = halves(
        fwd.reshape(2, LANES, 2, n, per).transpose(3, 2, 4, 0, 1).reshape(2 * LANES, 2 * LANES)
    )
    row_inv = halves(
        inv.reshape(2, n, per, 2, LANES).transpose(3, 4, 1, 0, 2).reshape(2 * LANES, 2 * LANES)
    )
    return row_fwd, row_inv, col_fwd, col_inv, wide_cos, wide_sin, tall_cos, tall_sin


def pair_body(n_row, n_sub, residual_in, direction, weights, noise_var):
    _, rows, grid_len = direction.shape
    embed = 2 * grid_len
    low, half = embed // LANES, grid_len // LANES
    n = n_row * n_sub
    per = LANES // n
    f32 = jnp.float32
    vmem = pl.BlockSpec(memory_space=pltpu.VMEM)
    chunks = CHUNKS
    per_chunk = low // chunks
    aligned = (2 * per) % 8 == 0
    groups = n if aligned else 1

    row_fwd, row_inv, col_fwd, col_inv, wide_cos, wide_sin, tall_cos, tall_sin = make_tables(embed, n, per)

    spread = pl.pallas_call(
        functools.partial(row_kernel, low, groups),
        out_shape=[jax.ShapeDtypeStruct((groups, per_chunk, 2 * LANES // groups, rows), f32)] * chunks,
        in_specs=[vmem] * 4,
        out_specs=[vmem] * chunks,
        scratch_shapes=[pltpu.VMEM((low, 2, LANES, rows), f32), pltpu.VMEM((half, 2, LANES, rows), f32)],
        compiler_params=params(),
        name="rows_out",
    )(direction, row_fwd, wide_cos, wide_sin)

    def swap(x):
        return lax.all_to_all(x, ("row", "sub"), split_axis=0, concat_axis=0, tiled=True)

    back = []
    for i, x in enumerate(spread):
        if not aligned:
            x = x.reshape(per_chunk, n, 2 * per, rows).transpose(1, 0, 2, 3)
        x = swap(x)
        if rows != LANES:
            x = x.reshape(half, LANES // rows, per_chunk, 2 * per, rows).transpose(0, 2, 3, 1, 4)
            x = x.reshape(half, per_chunk, 2 * per, LANES)
        x = pl.pallas_call(
            functools.partial(column_kernel, low, per),
            out_shape=jax.ShapeDtypeStruct((half, per_chunk, 2 * per, LANES), f32),
            in_specs=[vmem] * 6,
            out_specs=vmem,
            scratch_shapes=[pltpu.VMEM((low, per_chunk, per, 2 * LANES), f32)],
            compiler_params=params(),
            name=f"columns{i}",
        )(x, weights[:, i * per_chunk : (i + 1) * per_chunk], col_fwd, col_inv, tall_cos, tall_sin)
        if rows != LANES:
            x = x.reshape(half, per_chunk, 2 * per, LANES // rows, rows).transpose(0, 3, 1, 2, 4)
            x = x.reshape(n, per_chunk, 2 * per, rows)
        x = swap(x)
        if not aligned:
            x = x.transpose(1, 0, 2, 3).reshape(1, per_chunk, 2 * LANES, rows)
        back.append(x)

    image, sums = pl.pallas_call(
        functools.partial(image_kernel, low, groups, chunks),
        out_shape=[jax.ShapeDtypeStruct(direction.shape, f32), jax.ShapeDtypeStruct((8, LANES), f32)],
        in_specs=[vmem] * (chunks + 2) + [pl.BlockSpec(memory_space=pltpu.SMEM)] + [vmem] * 3,
        out_specs=[vmem] * 2,
        scratch_shapes=[pltpu.VMEM((low, 2, LANES, rows), f32), pltpu.VMEM((half, 2, LANES, rows), f32)],
        compiler_params=params(),
        name="rows_back",
    )(*back, direction, residual_in, noise_var, row_inv, wide_cos, wide_sin)

    residual_out, direction_out, steps = pl.pallas_call(
        functools.partial(update_kernel, n_row, n_sub),
        out_shape=[
            jax.ShapeDtypeStruct(direction.shape, f32),
            jax.ShapeDtypeStruct(direction.shape, f32),
            jax.ShapeDtypeStruct((2, LANES), f32),
        ],
        in_specs=[vmem] * 4,
        out_specs=[vmem] * 3,
        scratch_shapes=[
            pltpu.VMEM((n, 8, LANES), f32),
            pltpu.SemaphoreType.DMA((n,)),
            pltpu.SemaphoreType.DMA((n,)),
        ],
        compiler_params=params(collective_id=0, has_side_effects=True),
        name="update",
    )(sums, image, direction, residual_in)
    return residual_out, direction_out, steps[:, 0]


def odd_terms(d, n):
    q = n // 4
    zs = butterflies([turn((d[a], -d[a + q]), a, n, -1) for a in range(q)], -1)
    return {4 * j + 1: z for j, z in enumerate(zs)}


def real_forward(xs):
    n = len(xs)
    if n == 1:
        return {0: (xs[0], None)}
    if n == 2:
        return {0: (xs[0] + xs[1], None), 1: (xs[0] - xs[1], None)}
    h = n // 2
    out = {2 * k: z for k, z in real_forward([xs[a] + xs[a + h] for a in range(h)]).items()}
    out.update(odd_terms([xs[a] - xs[a + h] for a in range(h)], n))
    return out


def real_padded(xs):
    n = 2 * len(xs)
    out = {2 * k: z for k, z in real_forward(xs).items()}
    out.update(odd_terms(xs, n))
    return out


def odd_values(pairs, n):
    q = n // 4
    zs = [turn(z, a, n, 1) for a, z in enumerate(butterflies([pairs[4 * j + 1] for j in range(q)], 1))]
    return [z[0] for z in zs] + [-z[1] for z in zs]


def real_inverse(pairs, n):
    if n == 1:
        return [pairs[0][0]]
    if n == 2:
        return [pairs[0][0] + pairs[1][0], pairs[0][0] - pairs[1][0]]
    even = real_inverse({k // 2: z for k, z in pairs.items() if k % 2 == 0}, n // 2)
    odd = odd_values(pairs, n)
    return [e + o for e, o in zip(even, odd)] + [e - o for e, o in zip(even, odd)]


def real_cut(pairs, n):
    even = real_inverse({k // 2: z for k, z in pairs.items() if k % 2 == 0}, n // 2)
    return [e + o for e, o in zip(even, odd_values(pairs, n))]


def real_names(n):
    if n <= 2:
        return list(range(n))
    return [2 * k for k in real_names(n // 2)] + list(range(1, n, 4))


def loop(first, last, step):
    def run(i, carry):
        step(i)
        return carry

    lax.fori_loop(first, last, run, 0)


def half_kernel(
    low, chunks, pieces, n_row, n_sub,
    dir_hbm, res_hbm, spec_hbm, noise_ref, row_fwd_hbm, row_inv_hbm, col_fwd_hbm, col_inv_hbm, tall_cos, tall_sin,
    image_ref, dir_ref, res_ref, coef_ref,
    spec_ref, row_fwd, row_inv, col_fwd, col_inv,
    weights, work, cols, send, recv, back_send, back_recv,
    raw_in, img_send, img_in, x_send, x_recv, xb_send, xb_recv, held, sums_ref,
    load_sem, raw_ssem, raw_rsem, img_ssem, img_rsem, send_sem, recv_sem, back_ssem, back_rsem,
    x_sem, sum_sem,
):
    n = n_row * n_sub
    hs = n_sub // 2
    g = n_row * hs
    held_rows = 3
    half = low // 2
    count = low // chunks
    per = LANES // n
    size = 2 * per
    step_rows = LANES // pieces
    my_r, my_s = lax.axis_index("row"), lax.axis_index("sub")
    h = my_s // hs
    gi = my_r * hs + lax.rem(my_s, hs)
    me = my_r * n_sub + my_s

    def subs(part, own):
        return [own, (n_sub - 1) * (1 - part), hs - part]

    slabs = [my_r * n_sub + one for one in subs(h, my_s)]
    inner = my_s == hs - 1 + h
    tier = lax.rem(my_s + h, 2)
    across = {"row": my_r, "sub": hs - h}
    lead = my_s == h * hs

    def place(o):
        peer = lax.rem(me + o, n)
        return {"row": peer // n_sub, "sub": lax.rem(peer, n_sub)}

    def ally(d, part):
        r, s = d // hs, part * hs + lax.rem(d, hs)
        return {"row": r, "sub": s}, [r * n_sub + one for one in subs(part, s)]

    def others(step):
        loop(1, g, lambda o: step(lax.rem(gi + o, g)))

    def inner_others(step):
        def one(r):
            p = r * hs + 1 - h
            pl.when(p != gi)(lambda: step(p))

        loop(0, n_row, one)

    def leader(e):
        return {"row": e, "sub": (1 - h) * hs}

    barrier = pltpu.get_barrier_semaphore()
    loop(
        1, n,
        lambda o: pl.semaphore_signal(barrier, inc=1, device_id=place(o), device_id_type=MESH),
    )

    def load(src, dst, slot):
        return pltpu.make_async_copy(src, dst, load_sem.at[slot])

    load_dir = [load(dir_hbm.at[c], dir_ref.at[c], s) for s, c in enumerate((h, 1 - h))]
    load_fwd = load(row_fwd_hbm, row_fwd, 2)
    load_rest = [
        load(src, dst, 3 + s)
        for s, (src, dst) in enumerate(
            ((row_inv_hbm, row_inv), (col_fwd_hbm, col_fwd), (col_inv_hbm, col_inv), (res_hbm, res_ref))
        )
    ]
    load_spec = [
        load(spec_hbm.at[:, pl.ds(s * LANES, LANES)], spec_ref.at[s], 7 + s) for s in range(spec_ref.shape[0])
    ]
    load_dir[0].start()
    load_fwd.start()
    for one in load_spec:
        one.start()
    for one in load_rest:
        one.start()
    load_dir[1].start()

    def remote(src, dst, s_sem, r_sem, device):
        return pltpu.make_async_remote_copy(
            src_ref=src, dst_ref=dst, send_sem=s_sem, recv_sem=r_sem, device_id=device, device_id_type=MESH
        )

    def strip_of(p):
        return pl.ds(pl.multiple_of(p * step_rows, step_rows), step_rows)

    def raw_copy(p):
        at = strip_of(p)
        return remote(dir_hbm.at[1 - h, at, :], raw_in.at[tier, at, :], raw_ssem.at[0], raw_rsem.at[tier, p], across)

    def raw_arrival(b, p):
        at = strip_of(p)
        return remote(
            dir_hbm.at[1 - h, at, :], raw_in.at[b - 1, at, :], raw_ssem.at[0], raw_rsem.at[b - 1, p], across
        )

    def img_copy(b, p):
        at = strip_of(p)
        device = {"row": my_r, "sub": subs(h, my_s)[b]}
        return remote(img_send.at[b - 1, at, :], img_in.at[at, :], img_ssem.at[0], img_rsem.at[p], device)

    def img_arrival(p):
        at = strip_of(p)
        return remote(img_send.at[0, at, :], img_in.at[at, :], img_ssem.at[0], img_rsem.at[p], across)

    def ahead(i, b, p):
        return remote(
            send.at[i, b, p], recv.at[i, slabs[b]], send_sem.at[i], recv_sem.at[i], ally(p, h)[0]
        )

    def gather_in(i, tiles):
        return remote(recv.at[i, pl.ds(0, tiles)], recv.at[i, pl.ds(0, tiles)], send_sem.at[i], recv_sem.at[i], across)

    def gone(i, held):
        ref = send.at[i, pl.ds(0, held), pl.ds(0, g - 1)]
        return remote(ref, ref, send_sem.at[i], recv_sem.at[i], across)

    def back_gone(i, tiles):
        ref = back_send.at[i, pl.ds(0, tiles)]
        return remote(ref, ref, back_ssem.at[i], back_rsem.at[i, 0], across)

    def home(i, b, p):
        device, places = ally(p, h)
        return remote(
            back_send.at[i, places[b]], back_recv.at[i, b, gi], back_ssem.at[i], back_rsem.at[i, b], device
        )

    def back_arrival(i, b):
        ref = back_recv.at[i, b, pl.ds(0, g - 1)]
        return remote(ref, ref, back_ssem.at[i], back_rsem.at[i, b], across)

    def either(step):
        pl.when(inner)(lambda: step(True))
        pl.when(jnp.logical_not(inner))(lambda: step(False))

    alien = (held_rows - 1) * n_row + g - 1

    def x_ahead(e):
        return remote(x_send.at[e], x_recv.at[gi], x_sem.at[0], x_sem.at[1], leader(e))

    def x_home(d):
        return remote(xb_send.at[d], xb_recv.at[my_r], x_sem.at[2], x_sem.at[3], ally(d, 1 - h)[0])

    def x_all(ref, k):
        return remote(ref, ref, x_sem.at[k], x_sem.at[k], across)

    pl.semaphore_wait(barrier, n - 1)
    loop(0, pieces, lambda p: raw_copy(p).start())

    def row_strip(read, t):
        at = pl.ds(pl.multiple_of(t * 8, 8), 8)
        found = real_padded([read(at, slice(a * LANES, (a + 1) * LANES)) for a in range(half)])
        for m in range(low):
            c, s = tall_cos[m : m + 1, :], tall_sin[m : m + 1, :]
            re, im = found[m] if m in found else found[low - m]
            if im is None:
                re, im = re * c, re * s
            elif m in found:
                re, im = rotate(re, im, c, s)
            else:
                re, im = re * c + im * s, re * s - im * c
            work[m, at, :LANES] = re
            work[m, at, LANES:] = im

    batch = min(4, count)

    def row_dots(x, table, at):
        hi, lo = split(x)
        return dot(hi, table[h, 0, :, at]) + (dot(lo, table[h, 0, :, at]) + dot(hi, table[h, 1, :, at]))

    def row_extras(b):
        got = row_dots(work[0], row_fwd, slice(LANES, 2 * LANES)).T
        for e in range(n_row):
            x_send[e, 2 * b : 2 * b + 2, :] = got[2 * e : 2 * e + 2]

    def send_chunk(i, b):
        def columns(t):
            m = t * batch
            x = work[pl.ds(i * count + m, batch)].reshape(batch * LANES, 2 * LANES)
            got = row_dots(x, row_fwd, slice(0, LANES))
            for k in range(batch):
                part = got[k * LANES : (k + 1) * LANES].T
                for d in range(g):
                    send[i, b, d, m + k] = part[d * size : (d + 1) * size]

        loop(0, count // batch, columns)
        recv[i, slabs[b]] = send[i, b, gi]
        others(lambda p: ahead(i, b, p).start())

    load_dir[0].wait()
    load_fwd.wait()
    loop(0, LANES // 8, lambda t: row_strip(lambda at, cs: dir_ref[h, at, cs], t))
    row_extras(0)
    loop(0, chunks, lambda i: send_chunk(i, 0))

    def send_extras():
        loop(0, n_row, lambda e: x_ahead(e).start())

    pl.when(jnp.logical_not(inner))(send_extras)

    for one in load_spec:
        one.wait()

    def turn_spectrum(k):
        for s in range(spec_ref.shape[0]):
            part = spec_ref[s, pl.ds(k, LANES, stride=low), :]
            weights[k, s * LANES : (s + 1) * LANES, :] = part.T

    loop(0, low, turn_spectrum)
    for one in load_rest:
        one.wait()
    load_dir[1].wait()

    def far_rows():
        for b in range(1, held_rows):

            def raw_piece(p):
                raw_arrival(b, p).wait_recv()
                loop(
                    p * (step_rows // 8), (p + 1) * (step_rows // 8),
                    lambda t: row_strip(lambda at, cs: raw_in[b - 1, at, cs], t),
                )

            loop(0, pieces, raw_piece)
            row_extras(b)
            loop(0, chunks, lambda i: send_chunk(i, b))
        send_extras()

    pl.when(inner)(far_rows)

    wide = 16

    def foreign(d, step):
        places = ally(d, 1 - h)[1]
        step(0, places[0])

        def rest():
            for b in range(1, held_rows):
                step(b, places[b])

        pl.when(lax.rem(d, hs) == h)(rest)

    def fix_in():
        def one(d):
            def add_in(b, place_in):
                re, im = x_recv[d, 2 * b : 2 * b + 1, :], x_recv[d, 2 * b + 1 : 2 * b + 2, :]
                recv[0, place_in, 0, 0:1, :] = recv[0, place_in, 0, 0:1, :] - im
                recv[0, place_in, 0, per : per + 1, :] = recv[0, place_in, 0, per : per + 1, :] + re

            foreign(d, add_in)

        x_all(x_recv, 1).wait_recv()
        loop(0, g, one)

    def fix_out():
        def one(d):
            def take_out(b, place_in):
                re = 0.5 * back_send[0, place_in, 0, 0:1, :]
                im = 0.5 * back_send[0, place_in, 0, per : per + 1, :]
                back_send[0, place_in, 0, 0:1, :] = re
                back_send[0, place_in, 0, per : per + 1, :] = im
                xb_send[d, 2 * b : 2 * b + 1, :] = im
                xb_send[d, 2 * b + 1 : 2 * b + 2, :] = -re

            foreign(d, take_out)
            x_home(d).start()

        loop(0, g, one)

    def column_chunk(i):
        either(lambda near: gather_in(i, alien - (held_rows - 1 if near else 0)).wait_recv())
        pl.when(jnp.logical_and(i == 0, lead))(fix_in)

        def spread(m):
            xs = [(recv[i, a, m, :per], recv[i, a, m, per:]) for a in range(half)]
            for k, (re, im) in enumerate(padded_forward(xs)):
                re, im = rotate(re, im, tall_cos[k : k + 1, :], tall_sin[k : k + 1, :])
                cols[k, m, :, :LANES] = re
                cols[k, m, :, LANES:] = im

        loop(0, count, spread)
        block = count * per

        def filtered(t):
            k = t * wide
            spectral = dot_right(cols[pl.ds(k, wide)].reshape(wide * block, 2 * LANES), col_fwd)
            scale = jnp.concatenate(
                [
                    weights[k + w, pl.ds(i * count + m, per, stride=low), :]
                    for w in range(wide)
                    for m in range(count)
                ],
                axis=0,
            )
            spectral = spectral * jnp.concatenate([scale, scale], axis=1)
            got = dot_right(spectral, col_inv)
            for w in range(wide):
                cos_row, sin_row = tall_cos[pl.ds(k + w, 1), :], tall_sin[pl.ds(k + w, 1), :]
                part = got[w * block : (w + 1) * block]
                re, im = rotate(part[:, :LANES], part[:, LANES:], cos_row, -sin_row)
                cols[k + w, :, :, :LANES] = re.reshape(count, per, LANES)
                cols[k + w, :, :, LANES:] = im.reshape(count, per, LANES)

        loop(0, low // wide, filtered)

        def gather(m):
            zs = [(cols[k, m, :, :LANES], cols[k, m, :, LANES:]) for k in range(low)]
            for a, (re, im) in enumerate(cut_inverse(zs)):
                back_send[i, a, m, :per] = re
                back_send[i, a, m, per:] = im

        loop(0, count, gather)
        pl.when(jnp.logical_and(i == 0, lead))(fix_out)
        for b in range(held_rows):
            back_recv[i, b, gi] = back_send[i, slabs[b]]

        def first(p):
            near = lax.rem(p + h, hs) == 1
            pl.when(near)(lambda: home(i, 1, p).start())
            pl.when(jnp.logical_not(near))(lambda: home(i, 0, p).start())

        others(first)

    loop(0, chunks, column_chunk)
    for b in (2, 0):
        loop(0, chunks, lambda i: inner_others(lambda p: home(i, b, p).start()))
    x_all(xb_recv, 3).wait_recv()

    def take_chunk(i, b):
        back_arrival(i, b).wait_recv()

        def columns(t):
            m = t * batch
            parts = []
            for k in range(batch):
                parts.append(jnp.concatenate([back_recv[i, b, d, m + k] for d in range(g)], axis=0).T)
            got = row_dots(jnp.concatenate(parts, axis=0), row_inv, slice(None))
            work[pl.ds(i * count + m, batch)] = got.reshape(batch, LANES, 2 * LANES)

        loop(0, count // batch, columns)

    def take_extras(b):
        parts = [xb_recv[e, 2 * b : 2 * b + 2, :] for e in range(n_row)]
        parts.append(jnp.zeros((LANES - 2 * n_row, LANES), jnp.float32))
        x = jnp.concatenate(parts, axis=0).T
        hi, lo = split(x)
        first, second = row_inv[2 + h, 0], row_inv[2 + h, 1]
        work[0] = work[0] + (dot(hi, first) + (dot(lo, first) + dot(hi, second)))

    def back_strip(t):
        at = pl.ds(pl.multiple_of(t * 8, 8), 8)

        def entry(m):
            re, im = work[m, at, :LANES], work[m, at, LANES:]
            return rotate(re, im, tall_cos[m : m + 1, :], -tall_sin[m : m + 1, :])

        pairs = {}
        for m in real_names(low):
            re, im = entry(m)
            if m in (0, half):
                pairs[m] = (re, None)
            else:
                re_too, im_too = entry(low - m)
                pairs[m] = (re + re_too, im - im_too)
        return at, real_cut(pairs, low)

    def far_back():
        for b in range(1, held_rows):
            loop(0, chunks, lambda i: take_chunk(i, b))
            take_extras(b)

            def img_piece(p):
                def strip(t):
                    at, xs = back_strip(t)
                    for a, x in enumerate(xs):
                        img_send[b - 1, at, a * LANES : (a + 1) * LANES] = x

                loop(p * (step_rows // 8), (p + 1) * (step_rows // 8), strip)
                img_copy(b, p).start()

            loop(0, pieces, img_piece)

    pl.when(inner)(far_back)
    loop(0, chunks, lambda i: take_chunk(i, 0))
    take_extras(0)
    noise = noise_ref[0]

    def tally(c, at, a, applied, totals):
        cs = slice(a * LANES, (a + 1) * LANES)
        d, r = dir_ref[c, at, cs], res_ref[c, at, cs]
        image = applied + noise * d
        image_ref[c, at, cs] = image
        terms = (r * r, d * image, r * image, image * image)
        return [total + term for total, term in zip(totals, terms)]

    def own_strip(t, totals):
        at, xs = back_strip(t)
        for a, x in enumerate(xs):
            totals = tally(h, at, a, x, totals)
        return totals

    def far_strip(t, totals):
        at = pl.ds(pl.multiple_of(t * 8, 8), 8)
        for a in range(half):
            totals = tally(1 - h, at, a, img_in[at, a * LANES : (a + 1) * LANES], totals)
        return totals

    zeros = [jnp.zeros((8, LANES), jnp.float32)] * 4

    def keep(c, totals):
        for s in range(4):
            sums_ref[c, s : s + 1, :] = jnp.sum(totals[s], axis=0, keepdims=True)

    sums_ref[...] = jnp.zeros_like(sums_ref)
    keep(h, lax.fori_loop(0, LANES // 8, own_strip, zeros))

    def far_piece(p, totals):
        img_arrival(p).wait_recv()
        return lax.fori_loop(p * (step_rows // 8), (p + 1) * (step_rows // 8), far_strip, totals)

    keep(1 - h, lax.fori_loop(0, pieces, far_piece, zeros))

    def share(o):
        return remote(sums_ref, held.at[me], sum_sem.at[0], sum_sem.at[1], place(o))

    held[me] = sums_ref[...]
    loop(1, n, lambda o: share(o).start())

    def drain(near):
        def one(i):
            gone(i, held_rows if near else 1).wait_send()
            back_gone(i, alien - (held_rows - 1 if near else 0)).wait_send()

        loop(0, chunks, one)

    either(drain)
    x_all(x_send, 0).wait_send()
    pl.when(lead)(lambda: x_all(xb_send, 2).wait_send())
    remote(img_in, img_in, raw_ssem.at[0], raw_ssem.at[0], across).wait_send()

    pl.when(inner)(lambda: remote(img_send, img_send, img_ssem.at[0], img_ssem.at[0], across).wait_send())
    all_sums = held.at[pl.ds(0, n - 1)]
    remote(all_sums, all_sums, sum_sem.at[0], sum_sem.at[1], across).wait()
    total = jnp.sum(held[...], axis=0)
    for c in range(2):
        line = jnp.sum(total[c], axis=1, keepdims=True)
        old, curve, cross, square = [line[s : s + 1] for s in range(4)]
        step = old / curve
        new = jnp.maximum(old - 2.0 * step * cross + step * step * square, 0.0)
        beta = new / (old + TINY)
        coef_ref[c : c + 1, :] = jnp.broadcast_to(step, (1, LANES))
        coef_ref[2 + c : 3 + c, :] = jnp.broadcast_to(beta, (1, LANES))


def finish_kernel(parts, image_ref, dir_ref, res_ref, coef_ref, r_hbm, d_hbm, s_out, r_ref, d_ref, out_sem):
    probes, rows = image_ref.shape[:2]
    strip_rows = rows // parts

    def stores(k):
        at = pl.ds(pl.multiple_of(lax.rem(k, parts) * strip_rows, strip_rows), strip_rows)
        return [
            pltpu.make_async_copy(src.at[k // parts, at, :], dst.at[k // parts, at, :], out_sem.at[s])
            for s, (src, dst) in enumerate(((r_ref, r_hbm), (d_ref, d_hbm)))
        ]

    for c in range(probes):
        s_out[c] = coef_ref[c, 0]

    def work(k):
        c = k // parts
        step, beta = coef_ref[pl.ds(c, 1), 0:1], coef_ref[pl.ds(c + 2, 1), 0:1]

        def strip(t):
            at = pl.ds(pl.multiple_of(lax.rem(k, parts) * strip_rows + t * 8, 8), 8)
            r = res_ref[c, at, :] - step * image_ref[c, at, :]
            r_ref[c, at, :] = r
            d_ref[c, at, :] = r + beta * dir_ref[c, at, :]

        loop(0, strip_rows // 8, strip)
        for one in stores(k):
            one.start()

    loop(0, probes * parts, work)
    pltpu.make_async_copy(r_ref, r_hbm, out_sem.at[0]).wait()
    pltpu.make_async_copy(d_ref, d_hbm, out_sem.at[1]).wait()


def half_tables(embed, n_row, n_sub):
    low, n, hs = embed // LANES, n_row * n_sub, n_sub // 2
    per = LANES // n
    slots = np.arange(LANES)
    scale = 2.0 / (embed * embed)
    fwd_all, inv_all, inv_extra = [], [], []
    for part in range(2):
        own = [r * n_sub + part * hs + s for r in range(n_row) for s in range(hs)]
        freqs = np.stack([per * j + np.arange(per) for j in own])
        extra = np.array([per * (r * n_sub + (1 - part) * hs) for r in range(n_row)])[:, None]

        def forward(q):
            block = complex_block(*unit(slots[:, None] * q.reshape(-1)[None, :], LANES, -1.0))
            block = block.reshape(2, LANES, 2, *q.shape).transpose(0, 1, 3, 2, 4).reshape(2 * LANES, -1)
            return np.pad(block, ((0, 0), (0, LANES - block.shape[1])))

        def inverse(q):
            block = complex_block(*unit(q.reshape(-1)[:, None] * slots[None, :], LANES, 1.0))
            block = block.reshape(2, *q.shape, 2 * LANES).transpose(1, 0, 2, 3).reshape(-1, 2 * LANES)
            return np.pad(block * scale, ((0, LANES - block.shape[0]), (0, 0)))

        fwd_all.append(halves(np.concatenate([forward(freqs), forward(extra)], axis=1)))
        inv_all.append(halves(inverse(freqs)))
        inv_extra.append(halves(inverse(extra)))
    return jnp.stack(fwd_all), jnp.stack(inv_all + inv_extra)


def half_body(n_row, n_sub, residual_in, direction, spectrum, noise_var):
    _, rows, grid_len = direction.shape
    embed = 2 * grid_len
    low = embed // LANES
    n = n_row * n_sub
    g = n // 2
    per = LANES // n
    f32 = jnp.float32
    vmem = pl.BlockSpec(memory_space=pltpu.VMEM)
    away = pl.BlockSpec(memory_space=pl.ANY)
    chunks, pieces = CHUNKS, PIECES
    count = low // chunks
    lanes = spectrum.shape[1]
    row_fwd, row_inv = half_tables(embed, n_row, n_sub)
    _, _, col_fwd, col_inv, _, _, tall_cos, tall_sin = make_tables(embed, n, per)
    col_inv = halves(complex_block(*unit(np.arange(LANES)[:, None] * np.arange(LANES)[None, :], LANES, 1.0)).reshape(2 * LANES, 2 * LANES))
    tile = (count, 2 * per, LANES)
    dma = pltpu.SemaphoreType.DMA
    whole = pltpu.VMEM(direction.shape, f32)
    kept = pltpu.VMEM(direction.shape, f32)
    image, mine, rest, coef = pl.pallas_call(
        functools.partial(half_kernel, low, chunks, pieces, n_row, n_sub),
        out_shape=[kept, kept, kept, pltpu.VMEM((4, LANES), f32)],
        in_specs=[away, away, away, pl.BlockSpec(memory_space=pltpu.SMEM)] + [away] * 4 + [vmem] * 2,
        out_specs=[vmem] * 4,
        scratch_shapes=[
            pltpu.VMEM((lanes // LANES, embed, LANES), f32),
            *[pltpu.VMEM(table.shape, table.dtype) for table in (row_fwd, row_inv, col_fwd, col_inv)],
            pltpu.VMEM((low, lanes, LANES), f32),
            pltpu.VMEM((low, rows, 2 * LANES), f32),
            pltpu.VMEM((low, count, per, 2 * LANES), f32),
            pltpu.VMEM((chunks, 3, g, *tile), f32),
            pltpu.VMEM((chunks, n, *tile), f32),
            pltpu.VMEM((chunks, n, *tile), f32),
            pltpu.VMEM((chunks, 3, g, *tile), f32),
            pltpu.VMEM((2, rows, grid_len), f32),
            pltpu.VMEM((2, rows, grid_len), f32),
            pltpu.VMEM((rows, grid_len), f32),
            pltpu.VMEM((n_row, 8, LANES), f32),
            pltpu.VMEM((g, 8, LANES), f32),
            pltpu.VMEM((g, 8, LANES), f32),
            pltpu.VMEM((n_row, 8, LANES), f32),
            pltpu.VMEM((n, 2, 8, LANES), f32),
            pltpu.VMEM((2, 8, LANES), f32),
            dma((7 + lanes // LANES,)),
            dma((1,)), dma((2, pieces)), dma((1,)), dma((pieces,)),
            dma((chunks,)), dma((chunks,)), dma((chunks,)), dma((chunks, 3)),
            dma((4,)), dma((2,)),
        ],
        compiler_params=pltpu.CompilerParams(
            vmem_limit_bytes=HALF_GRANT, collective_id=1, has_side_effects=True
        ),
        name="cg_step",
    )(direction, residual_in, spectrum, noise_var, row_fwd, row_inv, col_fwd, col_inv, tall_cos, tall_sin)
    parts = PIECES
    residual_out, direction_out, steps = pl.pallas_call(
        functools.partial(finish_kernel, parts),
        out_shape=[
            jax.ShapeDtypeStruct(direction.shape, f32),
            jax.ShapeDtypeStruct(direction.shape, f32),
            jax.ShapeDtypeStruct((2,), f32),
        ],
        in_specs=[vmem] * 4,
        out_specs=[away, away, pl.BlockSpec(memory_space=pltpu.SMEM)],
        scratch_shapes=[whole, whole, dma((2,))],
        compiler_params=pltpu.CompilerParams(vmem_limit_bytes=8 * 1024 * 1024),
        name="finish",
    )(*[pltpu.with_memory_space_constraint(x, pltpu.VMEM) for x in (image, mine, rest, coef)])
    return residual_out, direction_out, steps


def solution(mesh):
    n_row, n_sub = mesh.shape["row"], mesh.shape["sub"]

    def body(residual_in, direction, spectrum, noise_var):
        embed = spectrum.shape[0]
        low = embed // LANES
        per = LANES // (n_row * n_sub)
        whole = direction.shape[1] == LANES and direction.shape[2] == LANES * n_row * n_sub
        if whole and per % 8 == 0 and n_sub == 4:
            return half_body(n_row, n_sub, residual_in, direction, spectrum, noise_var)
        weights = spectrum.reshape(LANES, low, per, low).transpose(1, 3, 2, 0)
        return pair_body(n_row, n_sub, residual_in, direction, weights, noise_var)

    placed = P("grp", ("row", "sub"), None)
    return jax.shard_map(
        body,
        mesh=mesh,
        in_specs=(placed, placed, P("grp", ("row", "sub")), P("grp")),
        out_specs=(placed, placed, P("grp")),
        check_vma=False,
    )
```

```python
import functools
import math

import jax
import jax.numpy as jnp
import numpy as np
from jax import lax
from jax.experimental import pallas as pl
from jax.experimental.pallas import tpu as pltpu
from jax.sharding import PartitionSpec as P

LANES = 128
TINY = 1e-06
CHUNKS = 8
PIECES = 4
HALF_GRANT = 54 * 1024 * 1024
MESH = pl.DeviceIdType.MESH
GRANT = 60 * 1024 * 1024


def unit(turns, modulus, orient):
    angle = orient * 2.0 * np.pi * (np.asarray(turns) % modulus) / modulus
    return np.cos(angle), np.sin(angle)


def halves(table):
    table = np.asarray(table, np.float32)
    hi = table.astype(jnp.bfloat16)
    lo = (table - hi.astype(np.float32)).astype(jnp.bfloat16)
    return jnp.asarray(np.stack([hi, lo]))


def complex_block(cos_part, sin_part):
    return np.stack(
        [np.stack([cos_part, sin_part], 1), np.stack([-sin_part, cos_part], 1)], 0
    )


def split(x):
    hi = x.astype(jnp.bfloat16)
    return hi, (x - hi.astype(jnp.float32)).astype(jnp.bfloat16)


def dot(a, b):
    return jnp.dot(a, b, preferred_element_type=jnp.float32)


def dot_right(x, table_ref):
    hi, lo = split(x)
    return dot(hi, table_ref[0]) + (dot(lo, table_ref[0]) + dot(hi, table_ref[1]))


def dot_left(table_ref, x):
    hi, lo = split(x)
    return dot(table_ref[0], hi) + (dot(table_ref[0], lo) + dot(table_ref[1], hi))


def turn(z, k, n, orient):
    k = k % n
    re, im = z
    if k == 0:
        return z
    if 2 * k == n:
        return -re, -im
    if 4 * k == n or 4 * k == 3 * n:
        sign = orient if 4 * k == n else -orient
        return (-im, re) if sign > 0 else (im, -re)
    c = math.cos(2 * math.pi * k / n)
    s = orient * math.sin(2 * math.pi * k / n)
    return re * c - im * s, re * s + im * c


def add(u, v):
    return u[0] + v[0], u[1] + v[1]


def sub(u, v):
    return u[0] - v[0], u[1] - v[1]


def butterflies(xs, orient):
    n = len(xs)
    if n == 1:
        return xs
    even = butterflies(xs[0::2], orient)
    odd = butterflies(xs[1::2], orient)
    odd = [turn(z, k, n, orient) for k, z in enumerate(odd)]
    return [add(e, o) for e, o in zip(even, odd)] + [sub(e, o) for e, o in zip(even, odd)]


def padded_forward(xs):
    n = len(xs)
    even = butterflies(xs, -1)
    odd = butterflies([turn(z, a, 2 * n, -1) for a, z in enumerate(xs)], -1)
    return [even[i // 2] if i % 2 == 0 else odd[i // 2] for i in range(2 * n)]


def cut_inverse(zs):
    n = len(zs) // 2
    even = butterflies(zs[0::2], 1)
    odd = butterflies(zs[1::2], 1)
    return [add(even[a], turn(odd[a], a, 2 * n, 1)) for a in range(n)]


def rotate(re, im, c, s):
    return re * c - im * s, re * s + im * c


def row_kernel(low, groups, dir_ref, table_ref, cos_ref, sin_ref, *rest):
    outs, work, turned = rest[:-2], rest[-2], rest[-1]
    half = low // 2
    rows = dir_ref.shape[1]
    for c in range(2):
        for a in range(half):
            turned[a, c] = dir_ref[c, :, a * LANES : (a + 1) * LANES].T

    def spread(t, carry):
        at = pl.ds(pl.multiple_of(t * 8, 8), 8)
        xs = [(turned[a, 0, at, :], turned[a, 1, at, :]) for a in range(half)]
        cos_rows, sin_rows = cos_ref[at, :], sin_ref[at, :]
        for m, (re, im) in enumerate(padded_forward(xs)):
            re, im = rotate(re, im, cos_rows[:, m : m + 1], sin_rows[:, m : m + 1])
            work[m, 0, at, :] = re
            work[m, 1, at, :] = im
        return carry

    lax.fori_loop(0, LANES // 8, spread, 0)
    per_chunk = low // len(outs)
    for i, out in enumerate(outs):

        def column(m, carry):
            got = dot_left(table_ref, work[i * per_chunk + m].reshape(2 * LANES, rows))
            size = 2 * LANES // groups
            for j in range(groups):
                out[j, m] = got[j * size : (j + 1) * size]
            return carry

        lax.fori_loop(0, per_chunk, column, 0)


def column_kernel(low, per, x_ref, w_ref, fwd_ref, inv_ref, cos_ref, sin_ref, out_ref, work):
    half = low // 2
    count = x_ref.shape[1]

    def spread(m, carry):
        xs = [(x_ref[a, m, :per], x_ref[a, m, per:]) for a in range(half)]
        for k, (re, im) in enumerate(padded_forward(xs)):
            re, im = rotate(re, im, cos_ref[k : k + 1, :], sin_ref[k : k + 1, :])
            work[k, m, :, :LANES] = re
            work[k, m, :, LANES:] = im
        return carry

    lax.fori_loop(0, count, spread, 0)

    def filtered(k, carry):
        spectral = dot_right(work[k].reshape(count * per, 2 * LANES), fwd_ref)
        weights = w_ref[k].reshape(count * per, LANES)
        spectral = spectral * jnp.concatenate([weights, weights], axis=1)
        got = dot_right(spectral, inv_ref)
        cos_row, sin_row = cos_ref[pl.ds(k, 1), :], sin_ref[pl.ds(k, 1), :]
        re, im = rotate(got[:, :LANES], got[:, LANES:], cos_row, -sin_row)
        work[k, :, :, :LANES] = re.reshape(count, per, LANES)
        work[k, :, :, LANES:] = im.reshape(count, per, LANES)
        return carry

    lax.fori_loop(0, low, filtered, 0)

    def gather(m, carry):
        zs = [(work[k, m, :, :LANES], work[k, m, :, LANES:]) for k in range(low)]
        for a, (re, im) in enumerate(cut_inverse(zs)):
            out_ref[a, m, :per] = re
            out_ref[a, m, per:] = im
        return carry

    lax.fori_loop(0, count, gather, 0)


def image_kernel(low, groups, chunks, *refs):
    ins = refs[:chunks]
    dir_ref, res_ref, noise_ref, table_ref, cos_ref, sin_ref = refs[chunks : chunks + 6]
    image_ref, sums_ref, work, applied = refs[chunks + 6 :]
    half = low // 2
    rows = dir_ref.shape[1]
    per_chunk = low // chunks
    for i, x_ref in enumerate(ins):

        def column(m, carry):
            parts = [x_ref[j, m] for j in range(groups)]
            got = dot_left(table_ref, parts[0] if groups == 1 else jnp.concatenate(parts, axis=0))
            work[i * per_chunk + m] = got.reshape(2, LANES, rows)
            return carry

        lax.fori_loop(0, per_chunk, column, 0)

    def gather(t, carry):
        at = pl.ds(pl.multiple_of(t * 8, 8), 8)
        cos_rows, sin_rows = cos_ref[at, :], sin_ref[at, :]
        zs = []
        for m in range(low):
            zs.append(
                rotate(work[m, 0, at, :], work[m, 1, at, :], cos_rows[:, m : m + 1], -sin_rows[:, m : m + 1])
            )
        for a, (re, im) in enumerate(cut_inverse(zs)):
            applied[a, 0, at, :] = re
            applied[a, 1, at, :] = im
        return carry

    lax.fori_loop(0, LANES // 8, gather, 0)
    noise = noise_ref[0]
    for c in range(2):
        totals = [jnp.zeros((rows, LANES), jnp.float32)] * 4
        for a in range(half):
            cols = slice(a * LANES, (a + 1) * LANES)
            d, r = dir_ref[c, :, cols], res_ref[c, :, cols]
            image = applied[a, c].T + noise * d
            image_ref[c, :, cols] = image
            for s, term in enumerate((r * r, d * image, r * image, image * image)):
                totals[s] = totals[s] + term
        for s in range(4):
            sums_ref[4 * c + s : 4 * c + s + 1, :] = jnp.sum(totals[s], axis=0, keepdims=True)


def update_kernel(n_row, n_sub, sums_ref, image_ref, dir_ref, res_ref, r_out, d_out, s_out, held, send_sem, recv_sem):
    n = n_row * n_sub
    me = lax.axis_index("row") * n_sub + lax.axis_index("sub")

    def place(o):
        peer = lax.rem(me + o, n)
        return {"row": peer // n_sub, "sub": lax.rem(peer, n_sub)}

    barrier = pltpu.get_barrier_semaphore()

    def greet(o, carry):
        pl.semaphore_signal(barrier, inc=1, device_id=place(o), device_id_type=MESH)
        return carry

    lax.fori_loop(1, n, greet, 0)
    pl.semaphore_wait(barrier, n - 1)

    def copy(o):
        return pltpu.make_async_remote_copy(
            src_ref=sums_ref,
            dst_ref=held.at[me],
            send_sem=send_sem.at[o],
            recv_sem=recv_sem.at[o],
            device_id=place(o),
            device_id_type=MESH,
        )

    def start(o, carry):
        copy(o).start()
        return carry

    lax.fori_loop(1, n, start, 0)
    held[me] = sums_ref[...]

    def finish(o, carry):
        copy(o).wait()
        return carry

    lax.fori_loop(1, n, finish, 0)
    total = jnp.sum(jnp.sum(held[...], axis=0), axis=1, keepdims=True)
    for c in range(2):
        old, curve, cross, square = [total[4 * c + s : 4 * c + s + 1] for s in range(4)]
        step = old / curve
        new = jnp.maximum(old - 2.0 * step * cross + step * step * square, 0.0)
        beta = new / (old + TINY)
        s_out[c : c + 1, :] = jnp.broadcast_to(step, (1, LANES))
        rows = min(8, res_ref.shape[1])

        def strip(t, carry):
            at = pl.ds(pl.multiple_of(t * rows, rows), rows)
            r = res_ref[c, at, :] - step * image_ref[c, at, :]
            r_out[c, at, :] = r
            d_out[c, at, :] = r + beta * dir_ref[c, at, :]
            return carry

        lax.fori_loop(0, res_ref.shape[1] // rows, strip, 0)


def params(**more):
    return pltpu.CompilerParams(vmem_limit_bytes=GRANT, **more)


def make_tables(embed, n, per):
    low, f32 = embed // LANES, jnp.float32
    slots, seconds = np.arange(LANES), np.arange(low)
    turn_cos, turn_sin = unit(slots[:, None] * seconds[None, :], embed, -1.0)
    wide_cos, wide_sin = jnp.asarray(turn_cos, f32), jnp.asarray(turn_sin, f32)
    tall_cos, tall_sin = jnp.asarray(turn_cos.T, f32), jnp.asarray(turn_sin.T, f32)
    fwd = complex_block(*unit(slots[:, None] * slots[None, :], LANES, -1.0))
    inv = complex_block(*unit(slots[:, None] * slots[None, :], LANES, 1.0))
    scale = 1.0 / (embed * embed)
    col_fwd = halves(fwd.reshape(2 * LANES, 2 * LANES))
    col_inv = halves(inv.reshape(2 * LANES, 2 * LANES) * scale)
    row_fwd = halves(
        fwd.reshape(2, LANES, 2, n, per).transpose(3, 2, 4, 0, 1).reshape(2 * LANES, 2 * LANES)
    )
    row_inv = halves(
        inv.reshape(2, n, per, 2, LANES).transpose(3, 4, 1, 0, 2).reshape(2 * LANES, 2 * LANES)
    )
    return row_fwd, row_inv, col_fwd, col_inv, wide_cos, wide_sin, tall_cos, tall_sin


def pair_body(n_row, n_sub, residual_in, direction, weights, noise_var):
    _, rows, grid_len = direction.shape
    embed = 2 * grid_len
    low, half = embed // LANES, grid_len // LANES
    n = n_row * n_sub
    per = LANES // n
    f32 = jnp.float32
    vmem = pl.BlockSpec(memory_space=pltpu.VMEM)
    chunks = CHUNKS
    per_chunk = low // chunks
    aligned = (2 * per) % 8 == 0
    groups = n if aligned else 1

    row_fwd, row_inv, col_fwd, col_inv, wide_cos, wide_sin, tall_cos, tall_sin = make_tables(embed, n, per)

    spread = pl.pallas_call(
        functools.partial(row_kernel, low, groups),
        out_shape=[jax.ShapeDtypeStruct((groups, per_chunk, 2 * LANES // groups, rows), f32)] * chunks,
        in_specs=[vmem] * 4,
        out_specs=[vmem] * chunks,
        scratch_shapes=[pltpu.VMEM((low, 2, LANES, rows), f32), pltpu.VMEM((half, 2, LANES, rows), f32)],
        compiler_params=params(),
        name="rows_out",
    )(direction, row_fwd, wide_cos, wide_sin)

    def swap(x):
        return lax.all_to_all(x, ("row", "sub"), split_axis=0, concat_axis=0, tiled=True)

    back = []
    for i, x in enumerate(spread):
        if not aligned:
            x = x.reshape(per_chunk, n, 2 * per, rows).transpose(1, 0, 2, 3)
        x = swap(x)
        if rows != LANES:
            x = x.reshape(half, LANES // rows, per_chunk, 2 * per, rows).transpose(0, 2, 3, 1, 4)
            x = x.reshape(half, per_chunk, 2 * per, LANES)
        x = pl.pallas_call(
            functools.partial(column_kernel, low, per),
            out_shape=jax.ShapeDtypeStruct((half, per_chunk, 2 * per, LANES), f32),
            in_specs=[vmem] * 6,
            out_specs=vmem,
            scratch_shapes=[pltpu.VMEM((low, per_chunk, per, 2 * LANES), f32)],
            compiler_params=params(),
            name=f"columns{i}",
        )(x, weights[:, i * per_chunk : (i + 1) * per_chunk], col_fwd, col_inv, tall_cos, tall_sin)
        if rows != LANES:
            x = x.reshape(half, per_chunk, 2 * per, LANES // rows, rows).transpose(0, 3, 1, 2, 4)
            x = x.reshape(n, per_chunk, 2 * per, rows)
        x = swap(x)
        if not aligned:
            x = x.transpose(1, 0, 2, 3).reshape(1, per_chunk, 2 * LANES, rows)
        back.append(x)

    image, sums = pl.pallas_call(
        functools.partial(image_kernel, low, groups, chunks),
        out_shape=[jax.ShapeDtypeStruct(direction.shape, f32), jax.ShapeDtypeStruct((8, LANES), f32)],
        in_specs=[vmem] * (chunks + 2) + [pl.BlockSpec(memory_space=pltpu.SMEM)] + [vmem] * 3,
        out_specs=[vmem] * 2,
        scratch_shapes=[pltpu.VMEM((low, 2, LANES, rows), f32), pltpu.VMEM((half, 2, LANES, rows), f32)],
        compiler_params=params(),
        name="rows_back",
    )(*back, direction, residual_in, noise_var, row_inv, wide_cos, wide_sin)

    residual_out, direction_out, steps = pl.pallas_call(
        functools.partial(update_kernel, n_row, n_sub),
        out_shape=[
            jax.ShapeDtypeStruct(direction.shape, f32),
            jax.ShapeDtypeStruct(direction.shape, f32),
            jax.ShapeDtypeStruct((2, LANES), f32),
        ],
        in_specs=[vmem] * 4,
        out_specs=[vmem] * 3,
        scratch_shapes=[
            pltpu.VMEM((n, 8, LANES), f32),
            pltpu.SemaphoreType.DMA((n,)),
            pltpu.SemaphoreType.DMA((n,)),
        ],
        compiler_params=params(collective_id=0, has_side_effects=True),
        name="update",
    )(sums, image, direction, residual_in)
    return residual_out, direction_out, steps[:, 0]


def odd_terms(d, n):
    q = n // 4
    zs = butterflies([turn((d[a], -d[a + q]), a, n, -1) for a in range(q)], -1)
    return {4 * j + 1: z for j, z in enumerate(zs)}


def real_forward(xs):
    n = len(xs)
    if n == 1:
        return {0: (xs[0], None)}
    if n == 2:
        return {0: (xs[0] + xs[1], None), 1: (xs[0] - xs[1], None)}
    h = n // 2
    out = {2 * k: z for k, z in real_forward([xs[a] + xs[a + h] for a in range(h)]).items()}
    out.update(odd_terms([xs[a] - xs[a + h] for a in range(h)], n))
    return out


def real_padded(xs):
    n = 2 * len(xs)
    out = {2 * k: z for k, z in real_forward(xs).items()}
    out.update(odd_terms(xs, n))
    return out


def odd_values(pairs, n):
    q = n // 4
    zs = [turn(z, a, n, 1) for a, z in enumerate(butterflies([pairs[4 * j + 1] for j in range(q)], 1))]
    return [z[0] for z in zs] + [-z[1] for z in zs]


def real_inverse(pairs, n):
    if n == 1:
        return [pairs[0][0]]
    if n == 2:
        return [pairs[0][0] + pairs[1][0], pairs[0][0] - pairs[1][0]]
    even = real_inverse({k // 2: z for k, z in pairs.items() if k % 2 == 0}, n // 2)
    odd = odd_values(pairs, n)
    return [e + o for e, o in zip(even, odd)] + [e - o for e, o in zip(even, odd)]


def real_cut(pairs, n):
    even = real_inverse({k // 2: z for k, z in pairs.items() if k % 2 == 0}, n // 2)
    return [e + o for e, o in zip(even, odd_values(pairs, n))]


def real_names(n):
    if n <= 2:
        return list(range(n))
    return [2 * k for k in real_names(n // 2)] + list(range(1, n, 4))


def loop(first, last, step):
    def run(i, carry):
        step(i)
        return carry

    lax.fori_loop(first, last, run, 0)


def half_kernel(
    low, chunks, pieces, n_row, n_sub,
    dir_hbm, res_hbm, spec_hbm, noise_ref, row_fwd_hbm, row_inv_hbm, col_fwd_hbm, col_inv_hbm, tall_cos, tall_sin,
    image_ref, dir_ref, res_ref, coef_ref,
    spec_ref, row_fwd, row_inv, col_fwd, col_inv,
    weights, work, cols, send, recv, back_send, back_recv,
    raw_in, img_send, img_in, x_send, x_recv, xb_send, xb_recv, held, sums_ref,
    load_sem, raw_ssem, raw_rsem, img_ssem, img_rsem, send_sem, recv_sem, back_ssem, back_rsem,
    x_sem, sum_sem,
):
    n = n_row * n_sub
    hs = n_sub // 2
    g = n_row * hs
    held_rows = 3
    half = low // 2
    count = low // chunks
    per = LANES // n
    size = 2 * per
    step_rows = LANES // pieces
    my_r, my_s = lax.axis_index("row"), lax.axis_index("sub")
    h = my_s // hs
    gi = my_r * hs + lax.rem(my_s, hs)
    me = my_r * n_sub + my_s

    def subs(part, own):
        return [own, (n_sub - 1) * (1 - part), hs - part]

    slabs = [my_r * n_sub + one for one in subs(h, my_s)]
    inner = my_s == hs - 1 + h
    tier = lax.rem(my_s + h, 2)
    across = {"row": my_r, "sub": hs - h}
    lead = my_s == h * hs

    def place(o):
        peer = lax.rem(me + o, n)
        return {"row": peer // n_sub, "sub": lax.rem(peer, n_sub)}

    def ally(d, part):
        r, s = d // hs, part * hs + lax.rem(d, hs)
        return {"row": r, "sub": s}, [r * n_sub + one for one in subs(part, s)]

    def others(step):
        loop(1, g, lambda o: step(lax.rem(gi + o, g)))

    def inner_others(step):
        def one(r):
            p = r * hs + 1 - h
            pl.when(p != gi)(lambda: step(p))

        loop(0, n_row, one)

    def leader(e):
        return {"row": e, "sub": (1 - h) * hs}

    barrier = pltpu.get_barrier_semaphore()
    loop(
        1, n,
        lambda o: pl.semaphore_signal(barrier, inc=1, device_id=place(o), device_id_type=MESH),
    )

    def load(src, dst, slot):
        return pltpu.make_async_copy(src, dst, load_sem.at[slot])

    load_dir = [load(dir_hbm.at[c], dir_ref.at[c], s) for s, c in enumerate((h, 1 - h))]
    load_fwd = load(row_fwd_hbm, row_fwd, 2)
    load_rest = [
        load(src, dst, 3 + s)
        for s, (src, dst) in enumerate(
            ((row_inv_hbm, row_inv), (col_fwd_hbm, col_fwd), (col_inv_hbm, col_inv), (res_hbm, res_ref))
        )
    ]
    load_spec = [
        load(spec_hbm.at[:, pl.ds(s * LANES, LANES)], spec_ref.at[s], 7 + s) for s in range(spec_ref.shape[0])
    ]
    load_dir[0].start()
    load_fwd.start()
    for one in load_spec:
        one.start()
    for one in load_rest:
        one.start()
    load_dir[1].start()

    def remote(src, dst, s_sem, r_sem, device):
        return pltpu.make_async_remote_copy(
            src_ref=src, dst_ref=dst, send_sem=s_sem, recv_sem=r_sem, device_id=device, device_id_type=MESH
        )

    def strip_of(p):
        return pl.ds(pl.multiple_of(p * step_rows, step_rows), step_rows)

    def raw_copy(p):
        at = strip_of(p)
        return remote(dir_hbm.at[1 - h, at, :], raw_in.at[tier, at, :], raw_ssem.at[0], raw_rsem.at[tier, p], across)

    def raw_arrival(b, p):
        at = strip_of(p)
        return remote(
            dir_hbm.at[1 - h, at, :], raw_in.at[b - 1, at, :], raw_ssem.at[0], raw_rsem.at[b - 1, p], across
        )

    def img_copy(b, p):
        at = strip_of(p)
        device = {"row": my_r, "sub": subs(h, my_s)[b]}
        return remote(img_send.at[b - 1, at, :], img_in.at[at, :], img_ssem.at[0], img_rsem.at[p], device)

    def img_arrival(p):
        at = strip_of(p)
        return remote(img_send.at[0, at, :], img_in.at[at, :], img_ssem.at[0], img_rsem.at[p], across)

    def ahead(i, b, p):
        return remote(
            send.at[i, b, p], recv.at[i, slabs[b]], send_sem.at[i], recv_sem.at[i], ally(p, h)[0]
        )

    def gather_in(i, tiles):
        return remote(recv.at[i, pl.ds(0, tiles)], recv.at[i, pl.ds(0, tiles)], send_sem.at[i], recv_sem.at[i], across)

    def gone(i, held):
        ref = send.at[i, pl.ds(0, held), pl.ds(0, g - 1)]
        return remote(ref, ref, send_sem.at[i], recv_sem.at[i], across)

    def back_gone(i, tiles):
        ref = back_send.at[i, pl.ds(0, tiles)]
        return remote(ref, ref, back_ssem.at[i], back_rsem.at[i, 0], across)

    def home(i, b, p):
        device, places = ally(p, h)
        return remote(
            back_send.at[i, places[b]], back_recv.at[i, b, gi], back_ssem.at[i], back_rsem.at[i, b], device
        )

    def back_arrival(i, b):
        ref = back_recv.at[i, b, pl.ds(0, g - 1)]
        return remote(ref, ref, back_ssem.at[i], back_rsem.at[i, b], across)

    def either(step):
        pl.when(inner)(lambda: step(True))
        pl.when(jnp.logical_not(inner))(lambda: step(False))

    alien = (held_rows - 1) * n_row + g - 1

    def x_ahead(e):
        return remote(x_send.at[e], x_recv.at[gi], x_sem.at[0], x_sem.at[1], leader(e))

    def x_home(d):
        return remote(xb_send.at[d], xb_recv.at[my_r], x_sem.at[2], x_sem.at[3], ally(d, 1 - h)[0])

    def x_all(ref, k):
        return remote(ref, ref, x_sem.at[k], x_sem.at[k], across)

    pl.semaphore_wait(barrier, n - 1)
    loop(0, pieces, lambda p: raw_copy(p).start())

    def row_strip(read, t):
        at = pl.ds(pl.multiple_of(t * 8, 8), 8)
        found = real_padded([read(at, slice(a * LANES, (a + 1) * LANES)) for a in range(half)])
        for m in range(low):
            c, s = tall_cos[m : m + 1, :], tall_sin[m : m + 1, :]
            re, im = found[m] if m in found else found[low - m]
            if im is None:
                re, im = re * c, re * s
            elif m in found:
                re, im = rotate(re, im, c, s)
            else:
                re, im = re * c + im * s, re * s - im * c
            work[m, at, :LANES] = re
            work[m, at, LANES:] = im

    batch = min(4, count)

    def row_dots(x, table, at):
        hi, lo = split(x)
        return dot(hi, table[h, 0, :, at]) + (dot(lo, table[h, 0, :, at]) + dot(hi, table[h, 1, :, at]))

    def row_extras(b):
        got = row_dots(work[0], row_fwd, slice(LANES, 2 * LANES)).T
        for e in range(n_row):
            x_send[e, 2 * b : 2 * b + 2, :] = got[2 * e : 2 * e + 2]

    def send_chunk(i, b):
        def columns(t):
            m = t * batch
            x = work[pl.ds(i * count + m, batch)].reshape(batch * LANES, 2 * LANES)
            got = row_dots(x, row_fwd, slice(0, LANES))
            for k in range(batch):
                part = got[k * LANES : (k + 1) * LANES].T
                for d in range(g):
                    send[i, b, d, m + k] = part[d * size : (d + 1) * size]

        loop(0, count // batch, columns)
        recv[i, slabs[b]] = send[i, b, gi]
        others(lambda p: ahead(i, b, p).start())

    load_dir[0].wait()
    load_fwd.wait()
    loop(0, LANES // 8, lambda t: row_strip(lambda at, cs: dir_ref[h, at, cs], t))
    row_extras(0)
    loop(0, chunks, lambda i: send_chunk(i, 0))

    def send_extras():
        loop(0, n_row, lambda e: x_ahead(e).start())

    pl.when(jnp.logical_not(inner))(send_extras)

    for one in load_spec:
        one.wait()

    def turn_spectrum(k):
        for s in range(spec_ref.shape[0]):
            part = spec_ref[s, pl.ds(k, LANES, stride=low), :]
            turned = part.T
            for q in range(LANES // low):
                at = pl.ds(s * (LANES // low) + q, low, stride=per)
                weights[k, at, :] = turned[q * low : (q + 1) * low]

    loop(0, low, turn_spectrum)
    for one in load_rest:
        one.wait()
    load_dir[1].wait()

    def far_rows():
        for b in range(1, held_rows):

            def raw_piece(p):
                raw_arrival(b, p).wait_recv()
                loop(
                    p * (step_rows // 8), (p + 1) * (step_rows // 8),
                    lambda t: row_strip(lambda at, cs: raw_in[b - 1, at, cs], t),
                )

            loop(0, pieces, raw_piece)
            row_extras(b)
            loop(0, chunks, lambda i: send_chunk(i, b))
        send_extras()

    pl.when(inner)(far_rows)

    wide, twin = 16, 1

    def foreign(d, step):
        places = ally(d, 1 - h)[1]
        step(0, places[0])

        def rest():
            for b in range(1, held_rows):
                step(b, places[b])

        pl.when(lax.rem(d, hs) == h)(rest)

    def fix_in():
        def one(d):
            def add_in(b, place_in):
                re, im = x_recv[d, 2 * b : 2 * b + 1, :], x_recv[d, 2 * b + 1 : 2 * b + 2, :]
                recv[0, place_in, 0, 0:1, :] = recv[0, place_in, 0, 0:1, :] - im
                recv[0, place_in, 0, per : per + 1, :] = recv[0, place_in, 0, per : per + 1, :] + re

            foreign(d, add_in)

        x_all(x_recv, 1).wait_recv()
        loop(0, g, one)

    def fix_out():
        def one(d):
            def take_out(b, place_in):
                re = 0.5 * back_send[0, place_in, 0, 0:1, :]
                im = 0.5 * back_send[0, place_in, 0, per : per + 1, :]
                back_send[0, place_in, 0, 0:1, :] = re
                back_send[0, place_in, 0, per : per + 1, :] = im
                xb_send[d, 2 * b : 2 * b + 1, :] = im
                xb_send[d, 2 * b + 1 : 2 * b + 2, :] = -re

            foreign(d, take_out)
            x_home(d).start()

        loop(0, g, one)

    def column_chunk(i):
        either(lambda near: gather_in(i, alien - (held_rows - 1 if near else 0)).wait_recv())
        pl.when(jnp.logical_and(i == 0, lead))(fix_in)

        def spread(m):
            xs = [(recv[i, a, m, :per], recv[i, a, m, per:]) for a in range(half)]
            for k, (re, im) in enumerate(padded_forward(xs)):
                re, im = rotate(re, im, tall_cos[k : k + 1, :], tall_sin[k : k + 1, :])
                cols[k, m, :, :LANES] = re
                cols[k, m, :, LANES:] = im

        loop(0, count, spread)
        block = count * per

        def piece(k):
            spectral = dot_right(cols[pl.ds(k, wide)].reshape(wide * block, 2 * LANES), col_fwd)
            scale = weights[pl.ds(k, wide), pl.ds(pl.multiple_of(i * block, block), block), :]
            scale = scale.reshape(wide * block, LANES)
            spectral = spectral * jnp.concatenate([scale, scale], axis=1)
            got = dot_right(spectral, col_inv)
            for w in range(wide):
                cos_row, sin_row = tall_cos[pl.ds(k + w, 1), :], tall_sin[pl.ds(k + w, 1), :]
                part = got[w * block : (w + 1) * block]
                re, im = rotate(part[:, :LANES], part[:, LANES:], cos_row, -sin_row)
                cols[k + w, :, :, :LANES] = re.reshape(count, per, LANES)
                cols[k + w, :, :, LANES:] = im.reshape(count, per, LANES)

        def filtered(t):
            for one in range(twin):
                piece((t * twin + one) * wide)

        loop(0, low // (wide * twin), filtered)

        def gather(m):
            zs = [(cols[k, m, :, :LANES], cols[k, m, :, LANES:]) for k in range(low)]
            for a, (re, im) in enumerate(cut_inverse(zs)):
                back_send[i, a, m, :per] = re
                back_send[i, a, m, per:] = im

        loop(0, count, gather)
        pl.when(jnp.logical_and(i == 0, lead))(fix_out)
        for b in range(held_rows):
            back_recv[i, b, gi] = back_send[i, slabs[b]]

        def first(p):
            near = lax.rem(p + h, hs) == 1
            pl.when(near)(lambda: home(i, 1, p).start())
            pl.when(jnp.logical_not(near))(lambda: home(i, 0, p).start())

        others(first)

    loop(0, chunks, column_chunk)
    for b in (2, 0):
        loop(0, chunks, lambda i: inner_others(lambda p: home(i, b, p).start()))
    x_all(xb_recv, 3).wait_recv()

    def take_chunk(i, b):
        back_arrival(i, b).wait_recv()

        def columns(t):
            m = t * batch
            parts = []
            for k in range(batch):
                parts.append(jnp.concatenate([back_recv[i, b, d, m + k] for d in range(g)], axis=0).T)
            got = row_dots(jnp.concatenate(parts, axis=0), row_inv, slice(None))
            work[pl.ds(i * count + m, batch)] = got.reshape(batch, LANES, 2 * LANES)

        loop(0, count // batch, columns)

    def take_extras(b):
        parts = [xb_recv[e, 2 * b : 2 * b + 2, :] for e in range(n_row)]
        parts.append(jnp.zeros((LANES - 2 * n_row, LANES), jnp.float32))
        x = jnp.concatenate(parts, axis=0).T
        hi, lo = split(x)
        first, second = row_inv[2 + h, 0], row_inv[2 + h, 1]
        work[0] = work[0] + (dot(hi, first) + (dot(lo, first) + dot(hi, second)))

    def back_strip(t):
        at = pl.ds(pl.multiple_of(t * 8, 8), 8)

        def entry(m):
            re, im = work[m, at, :LANES], work[m, at, LANES:]
            return rotate(re, im, tall_cos[m : m + 1, :], -tall_sin[m : m + 1, :])

        pairs = {}
        for m in real_names(low):
            re, im = entry(m)
            if m in (0, half):
                pairs[m] = (re, None)
            else:
                re_too, im_too = entry(low - m)
                pairs[m] = (re + re_too, im - im_too)
        return at, real_cut(pairs, low)

    def far_back():
        for b in range(1, held_rows):
            loop(0, chunks, lambda i: take_chunk(i, b))
            take_extras(b)

            def img_piece(p):
                def strip(t):
                    at, xs = back_strip(t)
                    for a, x in enumerate(xs):
                        img_send[b - 1, at, a * LANES : (a + 1) * LANES] = x

                loop(p * (step_rows // 8), (p + 1) * (step_rows // 8), strip)
                img_copy(b, p).start()

            loop(0, pieces, img_piece)

    pl.when(inner)(far_back)
    loop(0, chunks, lambda i: take_chunk(i, 0))
    take_extras(0)
    noise = noise_ref[0]

    def tally(c, at, a, applied, totals):
        cs = slice(a * LANES, (a + 1) * LANES)
        d, r = dir_ref[c, at, cs], res_ref[c, at, cs]
        image = applied + noise * d
        image_ref[c, at, cs] = image
        terms = (r * r, d * image, r * image, image * image)
        return [total + term for total, term in zip(totals, terms)]

    def own_strip(t, totals):
        at, xs = back_strip(t)
        for a, x in enumerate(xs):
            totals = tally(h, at, a, x, totals)
        return totals

    def far_strip(t, totals):
        at = pl.ds(pl.multiple_of(t * 8, 8), 8)
        for a in range(half):
            totals = tally(1 - h, at, a, img_in[at, a * LANES : (a + 1) * LANES], totals)
        return totals

    zeros = [jnp.zeros((8, LANES), jnp.float32)] * 4

    lane = lax.broadcasted_iota(jnp.int32, (1, LANES), 1)

    def keep(c, totals):
        for s in range(4):
            one = jnp.sum(jnp.sum(totals[s], axis=0, keepdims=True), axis=1, keepdims=True)
            sums_ref[...] = sums_ref[...] + jnp.where(lane == 4 * c + s, one, 0.0)

    sums_ref[...] = jnp.zeros_like(sums_ref)
    keep(h, lax.fori_loop(0, LANES // 8, own_strip, zeros))

    def far_piece(p, totals):
        img_arrival(p).wait_recv()
        return lax.fori_loop(p * (step_rows // 8), (p + 1) * (step_rows // 8), far_strip, totals)

    keep(1 - h, lax.fori_loop(0, pieces, far_piece, zeros))

    def share(o):
        return remote(sums_ref, held.at[me], sum_sem.at[0], sum_sem.at[1], place(o))

    held[me] = sums_ref[...]
    loop(1, n, lambda o: share(o).start())

    def drain(near):
        def one(i):
            gone(i, held_rows if near else 1).wait_send()
            back_gone(i, alien - (held_rows - 1 if near else 0)).wait_send()

        loop(0, chunks, one)

    either(drain)
    x_all(x_send, 0).wait_send()
    pl.when(lead)(lambda: x_all(xb_send, 2).wait_send())
    remote(img_in, img_in, raw_ssem.at[0], raw_ssem.at[0], across).wait_send()

    pl.when(inner)(lambda: remote(img_send, img_send, img_ssem.at[0], img_ssem.at[0], across).wait_send())
    all_sums = held.at[pl.ds(0, n - 1)]
    remote(all_sums, all_sums, sum_sem.at[0], sum_sem.at[1], across).wait()
    total = jnp.sum(held[...], axis=0)
    for c in range(2):
        old, curve, cross, square = [total[:, 4 * c + s : 4 * c + s + 1] for s in range(4)]
        step = old / curve
        new = jnp.maximum(old - 2.0 * step * cross + step * step * square, 0.0)
        beta = new / (old + TINY)
        coef_ref[c : c + 1, :] = jnp.broadcast_to(step, (1, LANES))
        coef_ref[2 + c : 3 + c, :] = jnp.broadcast_to(beta, (1, LANES))


def finish_kernel(parts, image_ref, dir_ref, res_ref, coef_ref, r_hbm, d_hbm, s_out, r_ref, d_ref, out_sem):
    probes, rows = image_ref.shape[:2]
    strip_rows = rows // parts

    def stores(k):
        at = pl.ds(pl.multiple_of(lax.rem(k, parts) * strip_rows, strip_rows), strip_rows)
        return [
            pltpu.make_async_copy(src.at[k // parts, at, :], dst.at[k // parts, at, :], out_sem.at[s])
            for s, (src, dst) in enumerate(((r_ref, r_hbm), (d_ref, d_hbm)))
        ]

    for c in range(probes):
        s_out[c] = coef_ref[c, 0]

    def work(k):
        c = k // parts
        step, beta = coef_ref[pl.ds(c, 1), 0:1], coef_ref[pl.ds(c + 2, 1), 0:1]

        def strip(t):
            at = pl.ds(pl.multiple_of(lax.rem(k, parts) * strip_rows + t * 16, 16), 16)
            r = res_ref[c, at, :] - step * image_ref[c, at, :]
            r_ref[c, at, :] = r
            d_ref[c, at, :] = r + beta * dir_ref[c, at, :]

        loop(0, strip_rows // 16, strip)
        for one in stores(k):
            one.start()

    loop(0, probes * parts, work)
    pltpu.make_async_copy(r_ref, r_hbm, out_sem.at[0]).wait()
    pltpu.make_async_copy(d_ref, d_hbm, out_sem.at[1]).wait()


def half_tables(embed, n_row, n_sub):
    low, n, hs = embed // LANES, n_row * n_sub, n_sub // 2
    per = LANES // n
    slots = np.arange(LANES)
    scale = 2.0 / (embed * embed)
    fwd_all, inv_all, inv_extra = [], [], []
    for part in range(2):
        own = [r * n_sub + part * hs + s for r in range(n_row) for s in range(hs)]
        freqs = np.stack([per * j + np.arange(per) for j in own])
        extra = np.array([per * (r * n_sub + (1 - part) * hs) for r in range(n_row)])[:, None]

        def forward(q):
            block = complex_block(*unit(slots[:, None] * q.reshape(-1)[None, :], LANES, -1.0))
            block = block.reshape(2, LANES, 2, *q.shape).transpose(0, 1, 3, 2, 4).reshape(2 * LANES, -1)
            return np.pad(block, ((0, 0), (0, LANES - block.shape[1])))

        def inverse(q):
            block = complex_block(*unit(q.reshape(-1)[:, None] * slots[None, :], LANES, 1.0))
            block = block.reshape(2, *q.shape, 2 * LANES).transpose(1, 0, 2, 3).reshape(-1, 2 * LANES)
            return np.pad(block * scale, ((0, LANES - block.shape[0]), (0, 0)))

        fwd_all.append(halves(np.concatenate([forward(freqs), forward(extra)], axis=1)))
        inv_all.append(halves(inverse(freqs)))
        inv_extra.append(halves(inverse(extra)))
    return jnp.stack(fwd_all), jnp.stack(inv_all + inv_extra)


def half_body(n_row, n_sub, residual_in, direction, spectrum, noise_var):
    _, rows, grid_len = direction.shape
    embed = 2 * grid_len
    low = embed // LANES
    n = n_row * n_sub
    g = n // 2
    per = LANES // n
    f32 = jnp.float32
    vmem = pl.BlockSpec(memory_space=pltpu.VMEM)
    away = pl.BlockSpec(memory_space=pl.ANY)
    chunks, pieces = CHUNKS, PIECES
    count = low // chunks
    lanes = spectrum.shape[1]
    row_fwd, row_inv = half_tables(embed, n_row, n_sub)
    _, _, col_fwd, col_inv, _, _, tall_cos, tall_sin = make_tables(embed, n, per)
    col_inv = halves(complex_block(*unit(np.arange(LANES)[:, None] * np.arange(LANES)[None, :], LANES, 1.0)).reshape(2 * LANES, 2 * LANES))
    tile = (count, 2 * per, LANES)
    dma = pltpu.SemaphoreType.DMA
    whole = pltpu.VMEM(direction.shape, f32)
    kept = pltpu.VMEM(direction.shape, f32)
    image, mine, rest, coef = pl.pallas_call(
        functools.partial(half_kernel, low, chunks, pieces, n_row, n_sub),
        out_shape=[kept, kept, kept, pltpu.VMEM((4, LANES), f32)],
        in_specs=[away, away, away, pl.BlockSpec(memory_space=pltpu.SMEM)] + [away] * 4 + [vmem] * 2,
        out_specs=[vmem] * 4,
        scratch_shapes=[
            pltpu.VMEM((lanes // LANES, embed, LANES), f32),
            *[pltpu.VMEM(table.shape, table.dtype) for table in (row_fwd, row_inv, col_fwd, col_inv)],
            pltpu.VMEM((low, lanes, LANES), f32),
            pltpu.VMEM((low, rows, 2 * LANES), f32),
            pltpu.VMEM((low, count, per, 2 * LANES), f32),
            pltpu.VMEM((chunks, 3, g, *tile), f32),
            pltpu.VMEM((chunks, n, *tile), f32),
            pltpu.VMEM((chunks, n, *tile), f32),
            pltpu.VMEM((chunks, 3, g, *tile), f32),
            pltpu.VMEM((2, rows, grid_len), f32),
            pltpu.VMEM((2, rows, grid_len), f32),
            pltpu.VMEM((rows, grid_len), f32),
            pltpu.VMEM((n_row, 8, LANES), f32),
            pltpu.VMEM((g, 8, LANES), f32),
            pltpu.VMEM((g, 8, LANES), f32),
            pltpu.VMEM((n_row, 8, LANES), f32),
            pltpu.VMEM((n, 1, LANES), f32),
            pltpu.VMEM((1, LANES), f32),
            dma((7 + lanes // LANES,)),
            dma((1,)), dma((2, pieces)), dma((1,)), dma((pieces,)),
            dma((chunks,)), dma((chunks,)), dma((chunks,)), dma((chunks, 3)),
            dma((4,)), dma((2,)),
        ],
        compiler_params=pltpu.CompilerParams(
            vmem_limit_bytes=HALF_GRANT, collective_id=1, has_side_effects=True
        ),
        name="cg_step",
    )(direction, residual_in, spectrum, noise_var, row_fwd, row_inv, col_fwd, col_inv, tall_cos, tall_sin)
    parts = PIECES
    residual_out, direction_out, steps = pl.pallas_call(
        functools.partial(finish_kernel, parts),
        out_shape=[
            jax.ShapeDtypeStruct(direction.shape, f32),
            jax.ShapeDtypeStruct(direction.shape, f32),
            jax.ShapeDtypeStruct((2,), f32),
        ],
        in_specs=[vmem] * 4,
        out_specs=[away, away, pl.BlockSpec(memory_space=pltpu.SMEM)],
        scratch_shapes=[whole, whole, dma((2,))],
        compiler_params=pltpu.CompilerParams(vmem_limit_bytes=8 * 1024 * 1024),
        name="finish",
    )(*[pltpu.with_memory_space_constraint(x, pltpu.VMEM) for x in (image, mine, rest, coef)])
    return residual_out, direction_out, steps


def solution(mesh):
    n_row, n_sub = mesh.shape["row"], mesh.shape["sub"]

    def body(residual_in, direction, spectrum, noise_var):
        embed = spectrum.shape[0]
        low = embed // LANES
        per = LANES // (n_row * n_sub)
        whole = direction.shape[1] == LANES and direction.shape[2] == LANES * n_row * n_sub
        if whole and per % 8 == 0 and n_sub == 4:
            return half_body(n_row, n_sub, residual_in, direction, spectrum, noise_var)
        weights = spectrum.reshape(LANES, low, per, low).transpose(1, 3, 2, 0)
        return pair_body(n_row, n_sub, residual_in, direction, weights, noise_var)

    placed = P("grp", ("row", "sub"), None)
    return jax.shard_map(
        body,
        mesh=mesh,
        in_specs=(placed, placed, P("grp", ("row", "sub")), P("grp")),
        out_specs=(placed, placed, P("grp")),
        check_vma=False,
    )
```

```python
import functools
import math

import jax
import jax.numpy as jnp
import numpy as np
from jax import lax
from jax.experimental import pallas as pl
from jax.experimental.pallas import tpu as pltpu
from jax.sharding import PartitionSpec as P

LANES = 128
TINY = 1e-06
CHUNKS = 8
PIECES = 8
HALF_GRANT = 54 * 1024 * 1024
MESH = pl.DeviceIdType.MESH
GRANT = 60 * 1024 * 1024


def unit(turns, modulus, orient):
    angle = orient * 2.0 * np.pi * (np.asarray(turns) % modulus) / modulus
    return np.cos(angle), np.sin(angle)


def halves(table):
    table = np.asarray(table, np.float32)
    hi = table.astype(jnp.bfloat16)
    lo = (table - hi.astype(np.float32)).astype(jnp.bfloat16)
    return jnp.asarray(np.stack([hi, lo]))


def complex_block(cos_part, sin_part):
    return np.stack(
        [np.stack([cos_part, sin_part], 1), np.stack([-sin_part, cos_part], 1)], 0
    )


def split(x):
    hi = x.astype(jnp.bfloat16)
    return hi, (x - hi.astype(jnp.float32)).astype(jnp.bfloat16)


def dot(a, b):
    return jnp.dot(a, b, preferred_element_type=jnp.float32)


def dot_right(x, table_ref):
    hi, lo = split(x)
    return dot(hi, table_ref[0]) + (dot(lo, table_ref[0]) + dot(hi, table_ref[1]))


def dot_left(table_ref, x):
    hi, lo = split(x)
    return dot(table_ref[0], hi) + (dot(table_ref[0], lo) + dot(table_ref[1], hi))


def turn(z, k, n, orient):
    k = k % n
    re, im = z
    if k == 0:
        return z
    if 2 * k == n:
        return -re, -im
    if 4 * k == n or 4 * k == 3 * n:
        sign = orient if 4 * k == n else -orient
        return (-im, re) if sign > 0 else (im, -re)
    c = math.cos(2 * math.pi * k / n)
    s = orient * math.sin(2 * math.pi * k / n)
    return re * c - im * s, re * s + im * c


def add(u, v):
    return u[0] + v[0], u[1] + v[1]


def sub(u, v):
    return u[0] - v[0], u[1] - v[1]


def butterflies(xs, orient):
    n = len(xs)
    if n == 1:
        return xs
    even = butterflies(xs[0::2], orient)
    odd = butterflies(xs[1::2], orient)
    odd = [turn(z, k, n, orient) for k, z in enumerate(odd)]
    return [add(e, o) for e, o in zip(even, odd)] + [sub(e, o) for e, o in zip(even, odd)]


def padded_forward(xs):
    n = len(xs)
    even = butterflies(xs, -1)
    odd = butterflies([turn(z, a, 2 * n, -1) for a, z in enumerate(xs)], -1)
    return [even[i // 2] if i % 2 == 0 else odd[i // 2] for i in range(2 * n)]


def cut_inverse(zs):
    n = len(zs) // 2
    even = butterflies(zs[0::2], 1)
    odd = butterflies(zs[1::2], 1)
    return [add(even[a], turn(odd[a], a, 2 * n, 1)) for a in range(n)]


def rotate(re, im, c, s):
    return re * c - im * s, re * s + im * c


def row_kernel(low, groups, dir_ref, table_ref, cos_ref, sin_ref, *rest):
    outs, work, turned = rest[:-2], rest[-2], rest[-1]
    half = low // 2
    rows = dir_ref.shape[1]
    for c in range(2):
        for a in range(half):
            turned[a, c] = dir_ref[c, :, a * LANES : (a + 1) * LANES].T

    def spread(t, carry):
        at = pl.ds(pl.multiple_of(t * 8, 8), 8)
        xs = [(turned[a, 0, at, :], turned[a, 1, at, :]) for a in range(half)]
        cos_rows, sin_rows = cos_ref[at, :], sin_ref[at, :]
        for m, (re, im) in enumerate(padded_forward(xs)):
            re, im = rotate(re, im, cos_rows[:, m : m + 1], sin_rows[:, m : m + 1])
            work[m, 0, at, :] = re
            work[m, 1, at, :] = im
        return carry

    lax.fori_loop(0, LANES // 8, spread, 0)
    per_chunk = low // len(outs)
    for i, out in enumerate(outs):

        def column(m, carry):
            got = dot_left(table_ref, work[i * per_chunk + m].reshape(2 * LANES, rows))
            size = 2 * LANES // groups
            for j in range(groups):
                out[j, m] = got[j * size : (j + 1) * size]
            return carry

        lax.fori_loop(0, per_chunk, column, 0)


def column_kernel(low, per, x_ref, w_ref, fwd_ref, inv_ref, cos_ref, sin_ref, out_ref, work):
    half = low // 2
    count = x_ref.shape[1]

    def spread(m, carry):
        xs = [(x_ref[a, m, :per], x_ref[a, m, per:]) for a in range(half)]
        for k, (re, im) in enumerate(padded_forward(xs)):
            re, im = rotate(re, im, cos_ref[k : k + 1, :], sin_ref[k : k + 1, :])
            work[k, m, :, :LANES] = re
            work[k, m, :, LANES:] = im
        return carry

    lax.fori_loop(0, count, spread, 0)

    def filtered(k, carry):
        spectral = dot_right(work[k].reshape(count * per, 2 * LANES), fwd_ref)
        weights = w_ref[k].reshape(count * per, LANES)
        spectral = spectral * jnp.concatenate([weights, weights], axis=1)
        got = dot_right(spectral, inv_ref)
        cos_row, sin_row = cos_ref[pl.ds(k, 1), :], sin_ref[pl.ds(k, 1), :]
        re, im = rotate(got[:, :LANES], got[:, LANES:], cos_row, -sin_row)
        work[k, :, :, :LANES] = re.reshape(count, per, LANES)
        work[k, :, :, LANES:] = im.reshape(count, per, LANES)
        return carry

    lax.fori_loop(0, low, filtered, 0)

    def gather(m, carry):
        zs = [(work[k, m, :, :LANES], work[k, m, :, LANES:]) for k in range(low)]
        for a, (re, im) in enumerate(cut_inverse(zs)):
            out_ref[a, m, :per] = re
            out_ref[a, m, per:] = im
        return carry

    lax.fori_loop(0, count, gather, 0)


def image_kernel(low, groups, chunks, *refs):
    ins = refs[:chunks]
    dir_ref, res_ref, noise_ref, table_ref, cos_ref, sin_ref = refs[chunks : chunks + 6]
    image_ref, sums_ref, work, applied = refs[chunks + 6 :]
    half = low // 2
    rows = dir_ref.shape[1]
    per_chunk = low // chunks
    for i, x_ref in enumerate(ins):

        def column(m, carry):
            parts = [x_ref[j, m] for j in range(groups)]
            got = dot_left(table_ref, parts[0] if groups == 1 else jnp.concatenate(parts, axis=0))
            work[i * per_chunk + m] = got.reshape(2, LANES, rows)
            return carry

        lax.fori_loop(0, per_chunk, column, 0)

    def gather(t, carry):
        at = pl.ds(pl.multiple_of(t * 8, 8), 8)
        cos_rows, sin_rows = cos_ref[at, :], sin_ref[at, :]
        zs = []
        for m in range(low):
            zs.append(
                rotate(work[m, 0, at, :], work[m, 1, at, :], cos_rows[:, m : m + 1], -sin_rows[:, m : m + 1])
            )
        for a, (re, im) in enumerate(cut_inverse(zs)):
            applied[a, 0, at, :] = re
            applied[a, 1, at, :] = im
        return carry

    lax.fori_loop(0, LANES // 8, gather, 0)
    noise = noise_ref[0]
    for c in range(2):
        totals = [jnp.zeros((rows, LANES), jnp.float32)] * 4
        for a in range(half):
            cols = slice(a * LANES, (a + 1) * LANES)
            d, r = dir_ref[c, :, cols], res_ref[c, :, cols]
            image = applied[a, c].T + noise * d
            image_ref[c, :, cols] = image
            for s, term in enumerate((r * r, d * image, r * image, image * image)):
                totals[s] = totals[s] + term
        for s in range(4):
            sums_ref[4 * c + s : 4 * c + s + 1, :] = jnp.sum(totals[s], axis=0, keepdims=True)


def update_kernel(n_row, n_sub, sums_ref, image_ref, dir_ref, res_ref, r_out, d_out, s_out, held, send_sem, recv_sem):
    n = n_row * n_sub
    me = lax.axis_index("row") * n_sub + lax.axis_index("sub")

    def place(o):
        peer = lax.rem(me + o, n)
        return {"row": peer // n_sub, "sub": lax.rem(peer, n_sub)}

    barrier = pltpu.get_barrier_semaphore()

    def greet(o, carry):
        pl.semaphore_signal(barrier, inc=1, device_id=place(o), device_id_type=MESH)
        return carry

    lax.fori_loop(1, n, greet, 0)
    pl.semaphore_wait(barrier, n - 1)

    def copy(o):
        return pltpu.make_async_remote_copy(
            src_ref=sums_ref,
            dst_ref=held.at[me],
            send_sem=send_sem.at[o],
            recv_sem=recv_sem.at[o],
            device_id=place(o),
            device_id_type=MESH,
        )

    def start(o, carry):
        copy(o).start()
        return carry

    lax.fori_loop(1, n, start, 0)
    held[me] = sums_ref[...]

    def finish(o, carry):
        copy(o).wait()
        return carry

    lax.fori_loop(1, n, finish, 0)
    total = jnp.sum(jnp.sum(held[...], axis=0), axis=1, keepdims=True)
    for c in range(2):
        old, curve, cross, square = [total[4 * c + s : 4 * c + s + 1] for s in range(4)]
        step = old / curve
        new = jnp.maximum(old - 2.0 * step * cross + step * step * square, 0.0)
        beta = new / (old + TINY)
        s_out[c : c + 1, :] = jnp.broadcast_to(step, (1, LANES))
        rows = min(8, res_ref.shape[1])

        def strip(t, carry):
            at = pl.ds(pl.multiple_of(t * rows, rows), rows)
            r = res_ref[c, at, :] - step * image_ref[c, at, :]
            r_out[c, at, :] = r
            d_out[c, at, :] = r + beta * dir_ref[c, at, :]
            return carry

        lax.fori_loop(0, res_ref.shape[1] // rows, strip, 0)


def params(**more):
    return pltpu.CompilerParams(vmem_limit_bytes=GRANT, **more)


def make_tables(embed, n, per):
    low, f32 = embed // LANES, jnp.float32
    slots, seconds = np.arange(LANES), np.arange(low)
    turn_cos, turn_sin = unit(slots[:, None] * seconds[None, :], embed, -1.0)
    wide_cos, wide_sin = jnp.asarray(turn_cos, f32), jnp.asarray(turn_sin, f32)
    tall_cos, tall_sin = jnp.asarray(turn_cos.T, f32), jnp.asarray(turn_sin.T, f32)
    fwd = complex_block(*unit(slots[:, None] * slots[None, :], LANES, -1.0))
    inv = complex_block(*unit(slots[:, None] * slots[None, :], LANES, 1.0))
    scale = 1.0 / (embed * embed)
    col_fwd = halves(fwd.reshape(2 * LANES, 2 * LANES))
    col_inv = halves(inv.reshape(2 * LANES, 2 * LANES) * scale)
    row_fwd = halves(
        fwd.reshape(2, LANES, 2, n, per).transpose(3, 2, 4, 0, 1).reshape(2 * LANES, 2 * LANES)
    )
    row_inv = halves(
        inv.reshape(2, n, per, 2, LANES).transpose(3, 4, 1, 0, 2).reshape(2 * LANES, 2 * LANES)
    )
    return row_fwd, row_inv, col_fwd, col_inv, wide_cos, wide_sin, tall_cos, tall_sin


def pair_body(n_row, n_sub, residual_in, direction, weights, noise_var):
    _, rows, grid_len = direction.shape
    embed = 2 * grid_len
    low, half = embed // LANES, grid_len // LANES
    n = n_row * n_sub
    per = LANES // n
    f32 = jnp.float32
    vmem = pl.BlockSpec(memory_space=pltpu.VMEM)
    chunks = CHUNKS
    per_chunk = low // chunks
    aligned = (2 * per) % 8 == 0
    groups = n if aligned else 1

    row_fwd, row_inv, col_fwd, col_inv, wide_cos, wide_sin, tall_cos, tall_sin = make_tables(embed, n, per)

    spread = pl.pallas_call(
        functools.partial(row_kernel, low, groups),
        out_shape=[jax.ShapeDtypeStruct((groups, per_chunk, 2 * LANES // groups, rows), f32)] * chunks,
        in_specs=[vmem] * 4,
        out_specs=[vmem] * chunks,
        scratch_shapes=[pltpu.VMEM((low, 2, LANES, rows), f32), pltpu.VMEM((half, 2, LANES, rows), f32)],
        compiler_params=params(),
        name="rows_out",
    )(direction, row_fwd, wide_cos, wide_sin)

    def swap(x):
        return lax.all_to_all(x, ("row", "sub"), split_axis=0, concat_axis=0, tiled=True)

    back = []
    for i, x in enumerate(spread):
        if not aligned:
            x = x.reshape(per_chunk, n, 2 * per, rows).transpose(1, 0, 2, 3)
        x = swap(x)
        if rows != LANES:
            x = x.reshape(half, LANES // rows, per_chunk, 2 * per, rows).transpose(0, 2, 3, 1, 4)
            x = x.reshape(half, per_chunk, 2 * per, LANES)
        x = pl.pallas_call(
            functools.partial(column_kernel, low, per),
            out_shape=jax.ShapeDtypeStruct((half, per_chunk, 2 * per, LANES), f32),
            in_specs=[vmem] * 6,
            out_specs=vmem,
            scratch_shapes=[pltpu.VMEM((low, per_chunk, per, 2 * LANES), f32)],
            compiler_params=params(),
            name=f"columns{i}",
        )(x, weights[:, i * per_chunk : (i + 1) * per_chunk], col_fwd, col_inv, tall_cos, tall_sin)
        if rows != LANES:
            x = x.reshape(half, per_chunk, 2 * per, LANES // rows, rows).transpose(0, 3, 1, 2, 4)
            x = x.reshape(n, per_chunk, 2 * per, rows)
        x = swap(x)
        if not aligned:
            x = x.transpose(1, 0, 2, 3).reshape(1, per_chunk, 2 * LANES, rows)
        back.append(x)

    image, sums = pl.pallas_call(
        functools.partial(image_kernel, low, groups, chunks),
        out_shape=[jax.ShapeDtypeStruct(direction.shape, f32), jax.ShapeDtypeStruct((8, LANES), f32)],
        in_specs=[vmem] * (chunks + 2) + [pl.BlockSpec(memory_space=pltpu.SMEM)] + [vmem] * 3,
        out_specs=[vmem] * 2,
        scratch_shapes=[pltpu.VMEM((low, 2, LANES, rows), f32), pltpu.VMEM((half, 2, LANES, rows), f32)],
        compiler_params=params(),
        name="rows_back",
    )(*back, direction, residual_in, noise_var, row_inv, wide_cos, wide_sin)

    residual_out, direction_out, steps = pl.pallas_call(
        functools.partial(update_kernel, n_row, n_sub),
        out_shape=[
            jax.ShapeDtypeStruct(direction.shape, f32),
            jax.ShapeDtypeStruct(direction.shape, f32),
            jax.ShapeDtypeStruct((2, LANES), f32),
        ],
        in_specs=[vmem] * 4,
        out_specs=[vmem] * 3,
        scratch_shapes=[
            pltpu.VMEM((n, 8, LANES), f32),
            pltpu.SemaphoreType.DMA((n,)),
            pltpu.SemaphoreType.DMA((n,)),
        ],
        compiler_params=params(collective_id=0, has_side_effects=True),
        name="update",
    )(sums, image, direction, residual_in)
    return residual_out, direction_out, steps[:, 0]


def odd_terms(d, n):
    q = n // 4
    zs = butterflies([turn((d[a], -d[a + q]), a, n, -1) for a in range(q)], -1)
    return {4 * j + 1: z for j, z in enumerate(zs)}


def real_forward(xs):
    n = len(xs)
    if n == 1:
        return {0: (xs[0], None)}
    if n == 2:
        return {0: (xs[0] + xs[1], None), 1: (xs[0] - xs[1], None)}
    h = n // 2
    out = {2 * k: z for k, z in real_forward([xs[a] + xs[a + h] for a in range(h)]).items()}
    out.update(odd_terms([xs[a] - xs[a + h] for a in range(h)], n))
    return out


def real_padded(xs):
    n = 2 * len(xs)
    out = {2 * k: z for k, z in real_forward(xs).items()}
    out.update(odd_terms(xs, n))
    return out


def odd_values(pairs, n):
    q = n // 4
    zs = [turn(z, a, n, 1) for a, z in enumerate(butterflies([pairs[4 * j + 1] for j in range(q)], 1))]
    return [z[0] for z in zs] + [-z[1] for z in zs]


def real_inverse(pairs, n):
    if n == 1:
        return [pairs[0][0]]
    if n == 2:
        return [pairs[0][0] + pairs[1][0], pairs[0][0] - pairs[1][0]]
    even = real_inverse({k // 2: z for k, z in pairs.items() if k % 2 == 0}, n // 2)
    odd = odd_values(pairs, n)
    return [e + o for e, o in zip(even, odd)] + [e - o for e, o in zip(even, odd)]


def real_cut(pairs, n):
    even = real_inverse({k // 2: z for k, z in pairs.items() if k % 2 == 0}, n // 2)
    return [e + o for e, o in zip(even, odd_values(pairs, n))]


def real_names(n):
    if n <= 2:
        return list(range(n))
    return [2 * k for k in real_names(n // 2)] + list(range(1, n, 4))


def loop(first, last, step):
    def run(i, carry):
        step(i)
        return carry

    lax.fori_loop(first, last, run, 0)


def half_kernel(
    low, chunks, pieces, n_row, n_sub,
    dir_hbm, res_hbm, spec_hbm, noise_ref, row_fwd_hbm, row_inv_hbm, col_fwd_hbm, col_inv_hbm, tall_cos, tall_sin,
    image_ref, dir_ref, res_ref, coef_ref,
    spec_ref, row_fwd, row_inv, col_fwd, col_inv,
    weights, work, cols, send, recv, back_send, back_recv,
    raw_in, img_send, img_in, x_send, x_recv, xb_send, xb_recv, held, sums_ref,
    load_sem, raw_ssem, raw_rsem, img_ssem, img_rsem, send_sem, recv_sem, back_ssem, back_rsem,
    x_sem, sum_sem,
):
    n = n_row * n_sub
    hs = n_sub // 2
    g = n_row * hs
    held_rows = 3
    half = low // 2
    count = low // chunks
    per = LANES // n
    size = 2 * per
    step_rows = LANES // pieces
    my_r, my_s = lax.axis_index("row"), lax.axis_index("sub")
    h = my_s // hs
    gi = my_r * hs + lax.rem(my_s, hs)
    me = my_r * n_sub + my_s

    def subs(part, own):
        return [own, (n_sub - 1) * (1 - part), hs - part]

    slabs = [my_r * n_sub + one for one in subs(h, my_s)]
    inner = my_s == hs - 1 + h
    tier = lax.rem(my_s + h, 2)
    across = {"row": my_r, "sub": hs - h}
    lead = my_s == h * hs

    def place(o):
        peer = lax.rem(me + o, n)
        return {"row": peer // n_sub, "sub": lax.rem(peer, n_sub)}

    def ally(d, part):
        r, s = d // hs, part * hs + lax.rem(d, hs)
        return {"row": r, "sub": s}, [r * n_sub + one for one in subs(part, s)]

    def ordered(step):
        loop(0, chunks, lambda t: step(t))

    def others(step):
        loop(1, g, lambda o: step(lax.rem(gi + o, g)))

    def inner_others(step):
        def one(r):
            p = r * hs + 1 - h
            pl.when(p != gi)(lambda: step(p))

        loop(0, n_row, one)

    def leader(e):
        return {"row": e, "sub": (1 - h) * hs}

    barrier = pltpu.get_barrier_semaphore()
    loop(
        1, n,
        lambda o: pl.semaphore_signal(barrier, inc=1, device_id=place(o), device_id_type=MESH),
    )

    def load(src, dst, slot):
        return pltpu.make_async_copy(src, dst, load_sem.at[slot])

    load_dir = [load(dir_hbm.at[c], dir_ref.at[c], s) for s, c in enumerate((h, 1 - h))]
    load_fwd = load(row_fwd_hbm, row_fwd, 2)
    load_rest = [
        load(src, dst, 3 + s)
        for s, (src, dst) in enumerate(
            ((row_inv_hbm, row_inv), (col_fwd_hbm, col_fwd), (col_inv_hbm, col_inv), (res_hbm, res_ref))
        )
    ]
    load_spec = [
        load(spec_hbm.at[:, pl.ds(s * LANES, LANES)], spec_ref.at[s], 7 + s) for s in range(spec_ref.shape[0])
    ]
    load_dir[0].start()
    load_fwd.start()
    for one in load_spec:
        one.start()
    for one in load_rest:
        one.start()
    load_dir[1].start()

    def remote(src, dst, s_sem, r_sem, device):
        return pltpu.make_async_remote_copy(
            src_ref=src, dst_ref=dst, send_sem=s_sem, recv_sem=r_sem, device_id=device, device_id_type=MESH
        )

    def strip_of(p):
        return pl.ds(pl.multiple_of(p * step_rows, step_rows), step_rows)

    def raw_copy(p):
        at = strip_of(p)
        return remote(dir_hbm.at[1 - h, at, :], raw_in.at[tier, at, :], raw_ssem.at[0], raw_rsem.at[tier, p], across)

    def raw_arrival(b, p):
        at = strip_of(p)
        return remote(
            dir_hbm.at[1 - h, at, :], raw_in.at[b - 1, at, :], raw_ssem.at[0], raw_rsem.at[b - 1, p], across
        )

    def img_copy(b, p):
        at = strip_of(p)
        device = {"row": my_r, "sub": subs(h, my_s)[b]}
        return remote(img_send.at[b - 1, at, :], img_in.at[at, :], img_ssem.at[0], img_rsem.at[p], device)

    def img_arrival(p):
        at = strip_of(p)
        return remote(img_send.at[0, at, :], img_in.at[at, :], img_ssem.at[0], img_rsem.at[p], across)

    def ahead(i, b, p):
        return remote(
            send.at[i, b, p], recv.at[i, slabs[b]], send_sem.at[i], recv_sem.at[i], ally(p, h)[0]
        )

    def gather_in(i, tiles):
        return remote(recv.at[i, pl.ds(0, tiles)], recv.at[i, pl.ds(0, tiles)], send_sem.at[i], recv_sem.at[i], across)

    def gone(i, held):
        ref = send.at[i, pl.ds(0, held), pl.ds(0, g - 1)]
        return remote(ref, ref, send_sem.at[i], recv_sem.at[i], across)

    def back_gone(i, tiles):
        ref = back_send.at[i, pl.ds(0, tiles)]
        return remote(ref, ref, back_ssem.at[i], back_rsem.at[i, 0], across)

    def home(i, b, p):
        device, places = ally(p, h)
        return remote(
            back_send.at[i, places[b]], back_recv.at[i, b, gi], back_ssem.at[i], back_rsem.at[i, b], device
        )

    def back_arrival(i, b):
        ref = back_recv.at[i, b, pl.ds(0, g - 1)]
        return remote(ref, ref, back_ssem.at[i], back_rsem.at[i, b], across)

    def either(step):
        pl.when(inner)(lambda: step(True))
        pl.when(jnp.logical_not(inner))(lambda: step(False))

    alien = (held_rows - 1) * n_row + g - 1

    def x_ahead(e):
        return remote(x_send.at[e], x_recv.at[gi], x_sem.at[0], x_sem.at[1], leader(e))

    def x_home(d):
        return remote(xb_send.at[d], xb_recv.at[my_r], x_sem.at[2], x_sem.at[3], ally(d, 1 - h)[0])

    def x_all(ref, k):
        return remote(ref, ref, x_sem.at[k], x_sem.at[k], across)

    pl.semaphore_wait(barrier, n - 1)
    loop(0, pieces, lambda p: raw_copy(p).start())

    def row_strip(read, t):
        at = pl.ds(pl.multiple_of(t * 8, 8), 8)
        found = real_padded([read(at, slice(a * LANES, (a + 1) * LANES)) for a in range(half)])
        for m in range(low):
            c, s = tall_cos[m : m + 1, :], tall_sin[m : m + 1, :]
            re, im = found[m] if m in found else found[low - m]
            if im is None:
                re, im = re * c, re * s
            elif m in found:
                re, im = rotate(re, im, c, s)
            else:
                re, im = re * c + im * s, re * s - im * c
            work[m, at, :LANES] = re
            work[m, at, LANES:] = im

    batch = min(4, count)

    def row_dots(x, table, at):
        hi, lo = split(x)
        return dot(hi, table[h, 0, :, at]) + (dot(lo, table[h, 0, :, at]) + dot(hi, table[h, 1, :, at]))

    def row_extras(b):
        got = row_dots(work[0], row_fwd, slice(LANES, 2 * LANES)).T
        for e in range(n_row):
            x_send[e, 2 * b : 2 * b + 2, :] = got[2 * e : 2 * e + 2]

    def send_chunk(i, b):
        def columns(t):
            m = t * batch
            x = work[pl.ds(i * count + m, batch)].reshape(batch * LANES, 2 * LANES)
            got = row_dots(x, row_fwd, slice(0, LANES))
            for k in range(batch):
                part = got[k * LANES : (k + 1) * LANES].T
                for d in range(g):
                    send[i, b, d, m + k] = part[d * size : (d + 1) * size]

        loop(0, count // batch, columns)
        recv[i, slabs[b]] = send[i, b, gi]
        others(lambda p: ahead(i, b, p).start())

    load_dir[0].wait()
    load_fwd.wait()
    loop(0, LANES // 8, lambda t: row_strip(lambda at, cs: dir_ref[h, at, cs], t))
    row_extras(0)
    ordered(lambda i: send_chunk(i, 0))

    def send_extras():
        loop(0, n_row, lambda e: x_ahead(e).start())

    pl.when(jnp.logical_not(inner))(send_extras)

    for one in load_spec:
        one.wait()

    def turn_spectrum(k):
        for s in range(spec_ref.shape[0]):
            part = spec_ref[s, pl.ds(k, LANES, stride=low), :]
            turned = part.T
            for q in range(LANES // low):
                at = pl.ds(s * (LANES // low) + q, low, stride=per)
                weights[k, at, :] = turned[q * low : (q + 1) * low]

    loop(0, low, turn_spectrum)
    for one in load_rest:
        one.wait()
    load_dir[1].wait()

    def far_rows():
        for b in range(1, held_rows):

            def raw_piece(p):
                raw_arrival(b, p).wait_recv()
                loop(
                    p * (step_rows // 8), (p + 1) * (step_rows // 8),
                    lambda t: row_strip(lambda at, cs: raw_in[b - 1, at, cs], t),
                )

            loop(0, pieces, raw_piece)
            row_extras(b)
            if b == held_rows - 1:
                send_extras()
            ordered(lambda i: send_chunk(i, b))

    pl.when(inner)(far_rows)

    wide, twin = 16, 1

    def foreign(d, step):
        places = ally(d, 1 - h)[1]
        step(0, places[0])

        def rest():
            for b in range(1, held_rows):
                step(b, places[b])

        pl.when(lax.rem(d, hs) == h)(rest)

    def fix_in():
        def one(d):
            def add_in(b, place_in):
                re, im = x_recv[d, 2 * b : 2 * b + 1, :], x_recv[d, 2 * b + 1 : 2 * b + 2, :]
                recv[0, place_in, 0, 0:1, :] = recv[0, place_in, 0, 0:1, :] - im
                recv[0, place_in, 0, per : per + 1, :] = recv[0, place_in, 0, per : per + 1, :] + re

            foreign(d, add_in)

        x_all(x_recv, 1).wait_recv()
        loop(0, g, one)

    def fix_out():
        def one(d):
            def take_out(b, place_in):
                re = 0.5 * back_send[0, place_in, 0, 0:1, :]
                im = 0.5 * back_send[0, place_in, 0, per : per + 1, :]
                back_send[0, place_in, 0, 0:1, :] = re
                back_send[0, place_in, 0, per : per + 1, :] = im
                xb_send[d, 2 * b : 2 * b + 1, :] = im
                xb_send[d, 2 * b + 1 : 2 * b + 2, :] = -re

            foreign(d, take_out)
            x_home(d).start()

        loop(0, g, one)

    def column_chunk(i):
        either(lambda near: gather_in(i, alien - (held_rows - 1 if near else 0)).wait_recv())
        pl.when(jnp.logical_and(i == 0, lead))(fix_in)

        def spread(m):
            xs = [(recv[i, a, m, :per], recv[i, a, m, per:]) for a in range(half)]
            for k, (re, im) in enumerate(padded_forward(xs)):
                re, im = rotate(re, im, tall_cos[k : k + 1, :], tall_sin[k : k + 1, :])
                cols[k, m, :, :LANES] = re
                cols[k, m, :, LANES:] = im

        loop(0, count, spread)
        block = count * per

        def piece(k):
            spectral = dot_right(cols[pl.ds(k, wide)].reshape(wide * block, 2 * LANES), col_fwd)
            scale = weights[pl.ds(k, wide), pl.ds(pl.multiple_of(i * block, block), block), :]
            scale = scale.reshape(wide * block, LANES)
            spectral = spectral * jnp.concatenate([scale, scale], axis=1)
            got = dot_right(spectral, col_inv)
            for w in range(wide):
                cos_row, sin_row = tall_cos[pl.ds(k + w, 1), :], tall_sin[pl.ds(k + w, 1), :]
                part = got[w * block : (w + 1) * block]
                re, im = rotate(part[:, :LANES], part[:, LANES:], cos_row, -sin_row)
                cols[k + w, :, :, :LANES] = re.reshape(count, per, LANES)
                cols[k + w, :, :, LANES:] = im.reshape(count, per, LANES)

        def filtered(t):
            for one in range(twin):
                piece((t * twin + one) * wide)

        loop(0, low // (wide * twin), filtered)

        def gather(m):
            zs = [(cols[k, m, :, :LANES], cols[k, m, :, LANES:]) for k in range(low)]
            for a, (re, im) in enumerate(cut_inverse(zs)):
                back_send[i, a, m, :per] = re
                back_send[i, a, m, per:] = im

        loop(0, count, gather)
        pl.when(jnp.logical_and(i == 0, lead))(fix_out)
        for b in range(held_rows):
            back_recv[i, b, gi] = back_send[i, slabs[b]]

        def first(p):
            near = lax.rem(p + h, hs) == 1
            pl.when(near)(lambda: home(i, 1, p).start())
            pl.when(jnp.logical_not(near))(lambda: home(i, 0, p).start())

        others(first)

    ordered(column_chunk)
    for b in (2, 0):
        ordered(lambda i: inner_others(lambda p: home(i, b, p).start()))
    x_all(xb_recv, 3).wait_recv()

    def take_chunk(i, b):
        back_arrival(i, b).wait_recv()

        def columns(t):
            m = t * batch
            parts = []
            for k in range(batch):
                parts.append(jnp.concatenate([back_recv[i, b, d, m + k] for d in range(g)], axis=0).T)
            got = row_dots(jnp.concatenate(parts, axis=0), row_inv, slice(None))
            work[pl.ds(i * count + m, batch)] = got.reshape(batch, LANES, 2 * LANES)

        loop(0, count // batch, columns)

    def take_extras(b):
        parts = [xb_recv[e, 2 * b : 2 * b + 2, :] for e in range(n_row)]
        parts.append(jnp.zeros((LANES - 2 * n_row, LANES), jnp.float32))
        x = jnp.concatenate(parts, axis=0).T
        hi, lo = split(x)
        first, second = row_inv[2 + h, 0], row_inv[2 + h, 1]
        work[0] = work[0] + (dot(hi, first) + (dot(lo, first) + dot(hi, second)))

    def back_strip(t):
        at = pl.ds(pl.multiple_of(t * 8, 8), 8)

        def entry(m):
            re, im = work[m, at, :LANES], work[m, at, LANES:]
            return rotate(re, im, tall_cos[m : m + 1, :], -tall_sin[m : m + 1, :])

        pairs = {}
        for m in real_names(low):
            re, im = entry(m)
            if m in (0, half):
                pairs[m] = (re, None)
            else:
                re_too, im_too = entry(low - m)
                pairs[m] = (re + re_too, im - im_too)
        return at, real_cut(pairs, low)

    def far_back():
        for b in range(1, held_rows):
            ordered(lambda i: take_chunk(i, b))
            take_extras(b)

            def img_piece(p):
                def strip(t):
                    at, xs = back_strip(t)
                    for a, x in enumerate(xs):
                        img_send[b - 1, at, a * LANES : (a + 1) * LANES] = x

                loop(p * (step_rows // 8), (p + 1) * (step_rows // 8), strip)
                img_copy(b, p).start()

            loop(0, pieces, img_piece)

    pl.when(inner)(far_back)
    ordered(lambda i: take_chunk(i, 0))
    take_extras(0)
    noise = noise_ref[0]

    def tally(c, at, a, applied, totals):
        cs = slice(a * LANES, (a + 1) * LANES)
        d, r = dir_ref[c, at, cs], res_ref[c, at, cs]
        image = applied + noise * d
        image_ref[c, at, cs] = image
        terms = (r * r, d * image, r * image, image * image)
        return [total + term for total, term in zip(totals, terms)]

    def own_strip(t, totals):
        at, xs = back_strip(t)
        for a, x in enumerate(xs):
            totals = tally(h, at, a, x, totals)
        return totals

    def far_strip(t, totals):
        at = pl.ds(pl.multiple_of(t * 8, 8), 8)
        for a in range(half):
            totals = tally(1 - h, at, a, img_in[at, a * LANES : (a + 1) * LANES], totals)
        return totals

    zeros = [jnp.zeros((8, LANES), jnp.float32)] * 4

    lane = lax.broadcasted_iota(jnp.int32, (1, LANES), 1)

    def keep(c, totals):
        for s in range(4):
            one = jnp.sum(jnp.sum(totals[s], axis=0, keepdims=True), axis=1, keepdims=True)
            sums_ref[...] = sums_ref[...] + jnp.where(lane == 4 * c + s, one, 0.0)

    sums_ref[...] = jnp.zeros_like(sums_ref)
    keep(h, lax.fori_loop(0, LANES // 8, own_strip, zeros))

    def far_piece(p, totals):
        img_arrival(p).wait_recv()
        return lax.fori_loop(p * (step_rows // 8), (p + 1) * (step_rows // 8), far_strip, totals)

    keep(1 - h, lax.fori_loop(0, pieces, far_piece, zeros))

    def share(o):
        return remote(sums_ref, held.at[me], sum_sem.at[0], sum_sem.at[1], place(o))

    held[me] = sums_ref[...]
    loop(1, n, lambda o: share(o).start())

    def drain(near):
        def one(i):
            gone(i, held_rows if near else 1).wait_send()
            back_gone(i, alien - (held_rows - 1 if near else 0)).wait_send()

        loop(0, chunks, one)

    either(drain)
    x_all(x_send, 0).wait_send()
    pl.when(lead)(lambda: x_all(xb_send, 2).wait_send())
    remote(img_in, img_in, raw_ssem.at[0], raw_ssem.at[0], across).wait_send()

    pl.when(inner)(lambda: remote(img_send, img_send, img_ssem.at[0], img_ssem.at[0], across).wait_send())
    all_sums = held.at[pl.ds(0, n - 1)]
    remote(all_sums, all_sums, sum_sem.at[0], sum_sem.at[1], across).wait()
    total = jnp.sum(held[...], axis=0)
    for c in range(2):
        old, curve, cross, square = [total[:, 4 * c + s : 4 * c + s + 1] for s in range(4)]
        step = old / curve
        new = jnp.maximum(old - 2.0 * step * cross + step * step * square, 0.0)
        beta = new / (old + TINY)
        coef_ref[c : c + 1, :] = jnp.broadcast_to(step, (1, LANES))
        coef_ref[2 + c : 3 + c, :] = jnp.broadcast_to(beta, (1, LANES))


def finish_kernel(parts, image_ref, dir_ref, res_ref, coef_ref, r_hbm, d_hbm, s_out, r_ref, d_ref, out_sem):
    probes, rows = image_ref.shape[:2]
    strip_rows = rows // parts

    def stores(k):
        at = pl.ds(pl.multiple_of(lax.rem(k, parts) * strip_rows, strip_rows), strip_rows)
        return [
            pltpu.make_async_copy(src.at[k // parts, at, :], dst.at[k // parts, at, :], out_sem.at[s])
            for s, (src, dst) in enumerate(((r_ref, r_hbm), (d_ref, d_hbm)))
        ]

    for c in range(probes):
        s_out[c] = coef_ref[c, 0]

    def work(k):
        c = k // parts
        step, beta = coef_ref[pl.ds(c, 1), 0:1], coef_ref[pl.ds(c + 2, 1), 0:1]

        def strip(t):
            at = pl.ds(pl.multiple_of(lax.rem(k, parts) * strip_rows + t * 16, 16), 16)
            r = res_ref[c, at, :] - step * image_ref[c, at, :]
            r_ref[c, at, :] = r
            d_ref[c, at, :] = r + beta * dir_ref[c, at, :]

        loop(0, strip_rows // 16, strip)
        for one in stores(k):
            one.start()

    loop(0, probes * parts, work)
    pltpu.make_async_copy(r_ref, r_hbm, out_sem.at[0]).wait()
    pltpu.make_async_copy(d_ref, d_hbm, out_sem.at[1]).wait()


def half_tables(embed, n_row, n_sub):
    low, n, hs = embed // LANES, n_row * n_sub, n_sub // 2
    per = LANES // n
    slots = np.arange(LANES)
    scale = 2.0 / (embed * embed)
    fwd_all, inv_all, inv_extra = [], [], []
    for part in range(2):
        own = [r * n_sub + part * hs + s for r in range(n_row) for s in range(hs)]
        freqs = np.stack([per * j + np.arange(per) for j in own])
        extra = np.array([per * (r * n_sub + (1 - part) * hs) for r in range(n_row)])[:, None]

        def forward(q):
            block = complex_block(*unit(slots[:, None] * q.reshape(-1)[None, :], LANES, -1.0))
            block = block.reshape(2, LANES, 2, *q.shape).transpose(0, 1, 3, 2, 4).reshape(2 * LANES, -1)
            return np.pad(block, ((0, 0), (0, LANES - block.shape[1])))

        def inverse(q):
            block = complex_block(*unit(q.reshape(-1)[:, None] * slots[None, :], LANES, 1.0))
            block = block.reshape(2, *q.shape, 2 * LANES).transpose(1, 0, 2, 3).reshape(-1, 2 * LANES)
            return np.pad(block * scale, ((0, LANES - block.shape[0]), (0, 0)))

        fwd_all.append(halves(np.concatenate([forward(freqs), forward(extra)], axis=1)))
        inv_all.append(halves(inverse(freqs)))
        inv_extra.append(halves(inverse(extra)))
    return jnp.stack(fwd_all), jnp.stack(inv_all + inv_extra)


def half_body(n_row, n_sub, residual_in, direction, spectrum, noise_var):
    _, rows, grid_len = direction.shape
    embed = 2 * grid_len
    low = embed // LANES
    n = n_row * n_sub
    g = n // 2
    per = LANES // n
    f32 = jnp.float32
    vmem = pl.BlockSpec(memory_space=pltpu.VMEM)
    away = pl.BlockSpec(memory_space=pl.ANY)
    chunks, pieces = CHUNKS, PIECES
    count = low // chunks
    lanes = spectrum.shape[1]
    row_fwd, row_inv = half_tables(embed, n_row, n_sub)
    _, _, col_fwd, col_inv, _, _, tall_cos, tall_sin = make_tables(embed, n, per)
    col_inv = halves(complex_block(*unit(np.arange(LANES)[:, None] * np.arange(LANES)[None, :], LANES, 1.0)).reshape(2 * LANES, 2 * LANES))
    tile = (count, 2 * per, LANES)
    dma = pltpu.SemaphoreType.DMA
    whole = pltpu.VMEM(direction.shape, f32)
    kept = pltpu.VMEM(direction.shape, f32)
    image, mine, rest, coef = pl.pallas_call(
        functools.partial(half_kernel, low, chunks, pieces, n_row, n_sub),
        out_shape=[kept, kept, kept, pltpu.VMEM((4, LANES), f32)],
        in_specs=[away, away, away, pl.BlockSpec(memory_space=pltpu.SMEM)] + [away] * 4 + [vmem] * 2,
        out_specs=[vmem] * 4,
        scratch_shapes=[
            pltpu.VMEM((lanes // LANES, embed, LANES), f32),
            *[pltpu.VMEM(table.shape, table.dtype) for table in (row_fwd, row_inv, col_fwd, col_inv)],
            pltpu.VMEM((low, lanes, LANES), f32),
            pltpu.VMEM((low, rows, 2 * LANES), f32),
            pltpu.VMEM((low, count, per, 2 * LANES), f32),
            pltpu.VMEM((chunks, 3, g, *tile), f32),
            pltpu.VMEM((chunks, n, *tile), f32),
            pltpu.VMEM((chunks, n, *tile), f32),
            pltpu.VMEM((chunks, 3, g, *tile), f32),
            pltpu.VMEM((2, rows, grid_len), f32),
            pltpu.VMEM((2, rows, grid_len), f32),
            pltpu.VMEM((rows, grid_len), f32),
            pltpu.VMEM((n_row, 8, LANES), f32),
            pltpu.VMEM((g, 8, LANES), f32),
            pltpu.VMEM((g, 8, LANES), f32),
            pltpu.VMEM((n_row, 8, LANES), f32),
            pltpu.VMEM((n, 1, LANES), f32),
            pltpu.VMEM((1, LANES), f32),
            dma((7 + lanes // LANES,)),
            dma((1,)), dma((2, pieces)), dma((1,)), dma((pieces,)),
            dma((chunks,)), dma((chunks,)), dma((chunks,)), dma((chunks, 3)),
            dma((4,)), dma((2,)),
        ],
        compiler_params=pltpu.CompilerParams(
            vmem_limit_bytes=HALF_GRANT, collective_id=1, has_side_effects=True
        ),
        name="cg_step",
    )(direction, residual_in, spectrum, noise_var, row_fwd, row_inv, col_fwd, col_inv, tall_cos, tall_sin)
    parts = PIECES
    residual_out, direction_out, steps = pl.pallas_call(
        functools.partial(finish_kernel, parts),
        out_shape=[
            jax.ShapeDtypeStruct(direction.shape, f32),
            jax.ShapeDtypeStruct(direction.shape, f32),
            jax.ShapeDtypeStruct((2,), f32),
        ],
        in_specs=[vmem] * 4,
        out_specs=[away, away, pl.BlockSpec(memory_space=pltpu.SMEM)],
        scratch_shapes=[whole, whole, dma((2,))],
        compiler_params=pltpu.CompilerParams(vmem_limit_bytes=8 * 1024 * 1024),
        name="finish",
    )(*[pltpu.with_memory_space_constraint(x, pltpu.VMEM) for x in (image, mine, rest, coef)])
    return residual_out, direction_out, steps


def solution(mesh):
    n_row, n_sub = mesh.shape["row"], mesh.shape["sub"]

    def body(residual_in, direction, spectrum, noise_var):
        embed = spectrum.shape[0]
        low = embed // LANES
        per = LANES // (n_row * n_sub)
        whole = direction.shape[1] == LANES and direction.shape[2] == LANES * n_row * n_sub
        if whole and per % 8 == 0 and n_sub == 4:
            return half_body(n_row, n_sub, residual_in, direction, spectrum, noise_var)
        weights = spectrum.reshape(LANES, low, per, low).transpose(1, 3, 2, 0)
        return pair_body(n_row, n_sub, residual_in, direction, weights, noise_var)

    placed = P("grp", ("row", "sub"), None)
    return jax.shard_map(
        body,
        mesh=mesh,
        in_specs=(placed, placed, P("grp", ("row", "sub")), P("grp")),
        out_specs=(placed, placed, P("grp")),
        check_vma=False,
    )
```
